512 devices in a mesh: src: 32 (over z, y_hi), tgt: 16 (over y_lo, x, core).
Axes of the slice: x: 4, y: 4 (y_hi: 2, y_lo: 2; y = y_hi * 2 + y_lo), z: 16, core: 2. Of those that a mesh axis runs over, the one named last changes fastest.
Arguments:
- sources: bfloat16 [32768, 512], P('src'), may hold values from -400 to 400
- log_src: float32 [32768], P('src'), may hold values from -1 to 1
- targets: bfloat16 [32768, 512], P(('src', 'tgt')), may hold values from -6 to 6
- potential: float32 [32768], P(('src', 'tgt')), may hold values from -5 to 5
- log_tgt: float32 [32768], P(('src', 'tgt')), may hold values from -1 to 1
Outputs:
- src_pot: float32 [32768], P('src')
- tgt_pot: float32 [32768], P(('src', 'tgt'))
- mapped: bfloat16 [32768, 512], P('src', 'tgt')
The draws below stay inside these ranges and needn't reach their ends.
All inputs are finite; a program needn't handle non-finite values.
Results may differ from the reference program's by a relative error of at most 0.0144.
Values may be sent and summed in bfloat16 or wider, within the bound.
No kernel may reach another device: no remote copies, remote signals or barrier semaphores. Data moves between devices by JAX's collectives and lax.ppermute only.
A program may use at most 64 MiB of HBM per device.

```python
import math
import jax
import jax.numpy as jnp
from jax import lax

F = 512
SRC_DEV = 1024
NS = 32768
NT = 32768
N_SRC = 32


def draw_sources(key, part):
    first = jax.random.fold_in(jax.random.fold_in(key, 17), 0)
    base = jax.random.truncated_normal(first, -6.0, 6.0, (NS, F), jnp.float32)
    return base.astype(jnp.bfloat16)


def block_levels(stream_key, extent, pieces, least, top_value):
    loudness = 1.0
    for dim, parts in pieces:
        steps = jax.random.uniform(jax.random.fold_in(jax.random.fold_in(stream_key, 6), dim), (parts,), jnp.float32, least / len(pieces), top_value / len(pieces))
        loudness = loudness * jnp.repeat(jnp.exp(steps), extent[dim] // parts).reshape((-1,) + (1,) * (len(extent) - 1 - dim))
    return loudness


def centred(own_key, shape, deviation, most, shards=(), held_as=jnp.bfloat16):
    array = deviation * jax.random.normal(own_key, shape, jnp.float32)
    if shards:
        array = array * block_levels(own_key, shape, shards, -0.22, 0.18)
    return jnp.clip(array, -most, most).astype(held_as)


def setup_inputs(seed: int = 0) -> dict:
    key_list = jax.random.split(jax.random.key(seed), 6)
    return {
        "sources": draw_sources(jax.random.fold_in(key_list[5], 71), 0),
        "log_src": jnp.clip(jax.random.uniform(key_list[1], (NS,), jnp.float32, -1.0, 1.0) * block_levels(key_list[1], (NS,), ((0, 32),), -0.4, 0.0), -1.0, 1.0),
        "targets": centred(key_list[2], (NT, F), 1.0, 6.0, ((0, 512),)),
        "potential": centred(key_list[3], (NT,), 1.0, 5.0, ((0, 512),), jnp.float32),
        "log_tgt": jnp.clip(jax.random.uniform(key_list[4], (NT,), jnp.float32, -1.0, 1.0) * block_levels(key_list[4], (NT,), ((0, 512),), -0.4, 0.0), -1.0, 1.0),
    }


def reference(sources, log_src, targets, potential, log_tgt):
    scale = 1.0 / math.sqrt(F)
    points = targets.astype(jnp.float32)
    blocks = sources.astype(jnp.float32).reshape(N_SRC, SRC_DEV, F)
    weights = log_src.reshape(N_SRC, SRC_DEV)

    def scores_of(block):
        return jnp.dot(block, points.T, precision=lax.Precision.HIGHEST) * scale

    def row_pass(items):
        block, logw = items
        shifted = scores_of(block) + potential[None, :]
        top = lax.optimization_barrier(jnp.max(shifted, axis=1))
        total = lax.optimization_barrier(jnp.sum(jnp.exp(shifted - top[:, None]), axis=1))
        return logw - (top + jnp.log(total))
    src_pot = lax.map(row_pass, (blocks, weights))

    def column_pass(items):
        block, pot = items
        lifted = scores_of(block) + pot[:, None]
        top = lax.optimization_barrier(jnp.max(lifted, axis=0))
        return (top, lax.optimization_barrier(jnp.sum(jnp.exp(lifted - top[None, :]), axis=0)))
    tops, totals = lax.map(column_pass, (blocks, src_pot))
    peak = lax.optimization_barrier(jnp.max(tops, axis=0))
    total = lax.optimization_barrier(jnp.sum(totals * jnp.exp(tops - peak[None, :]), axis=0))
    tgt_pot = log_tgt - (peak + jnp.log(total))

    def plan_pass(items):
        block, pot = items
        weight = jnp.exp(scores_of(block) + pot[:, None] + tgt_pot[None, :])
        mass = lax.optimization_barrier(jnp.sum(weight, axis=1))
        plan = weight.astype(jnp.bfloat16).astype(jnp.float32)
        moved = jnp.dot(plan, points, precision=lax.Precision.HIGHEST)
        return (moved / mass[:, None]).astype(jnp.bfloat16)
    mapped = lax.map(plan_pass, (blocks, src_pot)).reshape(NS, F)
    return (src_pot.reshape(NS), tgt_pot, mapped)
```

```python
import math

import jax
import jax.numpy as jnp
from jax import lax
from jax.experimental import pallas as pl
from jax.experimental.pallas import tpu as pltpu
from jax.sharding import Mesh
from jax.sharding import PartitionSpec as P

AXES = ("z", "yh", "yl", "x", "c")
PLANE = ("yh", "yl", "x", "c")
CHIPS = ("yh", "yl", "x")
LOG2E = math.log2(math.e)
LN2 = math.log(2.0)
B = 64
A8 = 8
OFF1 = (0, 4, 11, 2, 6, 9)
OFF2 = (14, 1, 3, 7, 5, 12, 15, 8, 13, 10)
OFF = OFF1 + OFF2


def from_z(array, d):
    n = lax.axis_size("z")
    return lax.ppermute(array, "z", [((i + d) % n, i) for i in range(n)])


def thirds(v):
    hi = lax.reduce_precision(v, 8, 7)
    lo = lax.reduce_precision(v - hi, 8, 7)
    return [hi, lo, v - hi - lo]


def joined(messages):
    ks = [m.shape[0] // (B + A8) for m in messages]
    rows = [m[: k * B] for m, k in zip(messages, ks)]
    extra = [m[k * B :] for m, k in zip(messages, ks)]
    return jnp.concatenate(rows + extra, axis=0)


def eye(n):
    return lax.broadcasted_iota(jnp.int32, (n, n), 0) == lax.broadcasted_iota(jnp.int32, (n, n), 1)


def to_col(row):
    n = row.shape[1]
    return jnp.sum(jnp.where(eye(n), jnp.broadcast_to(row, (n, n)), 0.0), axis=1, keepdims=True)


def to_row(col):
    n = col.shape[0]
    return jnp.sum(jnp.where(eye(n), jnp.broadcast_to(col, (n, n)), 0.0), axis=0, keepdims=True)


CH = 512


def scores_kernel(picks, last, n_msg, scale2, scal, src, *refs):
    msgs = refs[:n_msg]
    rest = refs[n_msg:]
    if last:
        lse_in, s_out, tgt_out, lt_out, lse_out, tg, pot = rest
    else:
        s_out, tgt_out, lt_out, lse_out, tg, pot = rest
    n = pl.program_id(0)

    @pl.when(n == 0)
    def _():
        core = scal[1]
        lt_out[...] = jnp.zeros_like(lt_out)
        for p, (m, k) in enumerate(picks):
            total = msgs[m].shape[0] // (B + A8)
            rows = msgs[m][k * B : (k + 1) * B, :]
            tg[p * B : (p + 1) * B, :] = rows
            ex = msgs[m][total * B + k * A8 : total * B + (k + 1) * A8, 0:128].astype(jnp.float32)
            po = (ex[0:1] + ex[1:2] + ex[2:3]) * LOG2E
            lt_out[p : p + 1, :] = ex[3:4] + ex[4:5] + ex[5:6]
            pot[p * B : (p + 1) * B, :] = jnp.broadcast_to(to_col(po[:, :B]), (B, 128))
        for q in range(tg.shape[0] // 128):
            flipped = tg[q * 128 : (q + 1) * 128, :].astype(jnp.float32).T.astype(jnp.bfloat16)
            for t in range(16):
                at = pl.multiple_of((((t % 2) ^ core) * 8 + t // 2) * 32, 32)
                tgt_out[pl.ds(at, 32), q * 128 : (q + 1) * 128] = flipped[t * 32 : (t + 1) * 32, :]

    s = lax.dot_general(tg[...], src[...], (((1,), (1,)), ((), ())), preferred_element_type=jnp.float32) * scale2
    s_out[...] = s
    shifted = s + jnp.concatenate([pot[...]] * (CH // 128), axis=1)
    top = jnp.max(shifted, axis=0, keepdims=True)
    tot = jnp.sum(jnp.exp2(shifted - top), axis=0, keepdims=True)
    lse = top + jnp.log2(tot)
    if last:
        a = lse_in[...]
        hi = jnp.maximum(a, lse)
        lse = hi + jnp.log2(jnp.exp2(a - hi) + jnp.exp2(lse - hi))
        for i in range(CH // 128):
            piece = lse[:, i * 128 : (i + 1) * 128]
            lse_out[:, pl.ds(n * (CH // 128) + i, 1), :] = jnp.broadcast_to(piece[None], (lse_out.shape[0], 1, 128))
    else:
        lse_out[...] = lse


def scores_call(scal, src, msgs, picks, scale2, lse_in=None):
    t = len(picks) * B
    ns, f = src.shape
    last = lse_in is not None
    whole = lambda m: pl.BlockSpec(m.shape, lambda n, sc: (0,) * m.ndim)
    in_specs = [pl.BlockSpec((CH, f), lambda n, sc: (n, 0))] + [whole(m) for m in msgs]
    if last:
        in_specs.append(pl.BlockSpec((1, CH), lambda n, sc: (0, n)))
        lse_shape = jax.ShapeDtypeStruct((32, ns // 128, 128), jnp.float32)
        lse_spec = pl.BlockSpec((32, ns // 128, 128), lambda n, sc: (0, 0, 0))
    else:
        lse_shape = jax.ShapeDtypeStruct((1, ns), jnp.float32)
        lse_spec = pl.BlockSpec((1, CH), lambda n, sc: (0, n))
    lt_rows = -(-len(picks) // 8) * 8
    args = [scal, src, *msgs] + ([lse_in] if last else [])
    return pl.pallas_call(
        lambda *a: scores_kernel(picks, last, len(msgs), scale2, *a),
        name="scores_last" if last else "scores_first",
        grid_spec=pltpu.PrefetchScalarGridSpec(
            num_scalar_prefetch=1,
            grid=(ns // CH,),
            in_specs=in_specs,
            out_specs=[
                pl.BlockSpec((t, CH), lambda n, sc: (0, n)),
                pl.BlockSpec((f, t), lambda n, sc: (0, 0)),
                pl.BlockSpec((lt_rows, 128), lambda n, sc: (0, 0)),
                lse_spec,
            ],
            scratch_shapes=[pltpu.VMEM((t, f), jnp.bfloat16), pltpu.VMEM((t, 128), jnp.float32)],
        ),
        out_shape=[
            jax.ShapeDtypeStruct((t, ns), jnp.float32),
            jax.ShapeDtypeStruct((f, t), jnp.bfloat16),
            jax.ShapeDtypeStruct((lt_rows, 128), jnp.float32),
            lse_shape,
        ],
        cost_estimate=pl.CostEstimate(flops=2 * t * ns * f, bytes_accessed=4 * t * ns, transcendentals=t * ns),
    )(*args)


def merged_lse(parts):
    top = jnp.max(parts, axis=0)
    return top + jnp.log2(jnp.sum(jnp.exp2(parts - top[None]), axis=0))


def cols_kernel(scal, parts, log_src, s1, s2, pot_out, sp_out, msg_out, held):
    i = pl.program_id(0)

    @pl.when(i == 0)
    def _():
        sp = log_src[...] * LOG2E - merged_lse(parts[...])
        for r in range(sp.shape[0]):
            sp_out[:, r * 128 : (r + 1) * 128] = sp[r : r + 1, :]
        half = sp.shape[0] // 2
        pot_out[...] = jnp.where(scal[0] == 0, sp[:half], sp[half:]) * LN2
        held[...] = jnp.zeros_like(held)

    def step(s_ref):
        lifted = s_ref[...] + sp_out[...]
        top = jnp.max(lifted, axis=1, keepdims=True)
        lse = top + jnp.log2(jnp.sum(jnp.exp2(lifted - top), axis=1, keepdims=True))
        row = to_row(lse)
        row = jnp.concatenate([row, row], axis=1)
        slot = scal[2 + i]
        at = slot // 2
        half = lax.broadcasted_iota(jnp.int32, (1, 128), 1) // B
        held[pl.ds(at, 1), :] = jnp.where(half == slot % 2, row, held[pl.ds(at, 1), :])

    @pl.when(i < len(OFF1))
    def _():
        step(s1)

    @pl.when(i >= len(OFF1))
    def _():
        step(s2)

    @pl.when(i == len(OFF) - 1)
    def _():
        msg_out[...] = jnp.broadcast_to(held[...][None], msg_out.shape)


def cols_call(scal, parts, log_src, s1, s2):
    ns = s1.shape[1]
    n1, n2 = len(OFF1), len(OFF2)
    return pl.pallas_call(
        cols_kernel,
        name="cols",
        grid_spec=pltpu.PrefetchScalarGridSpec(
            num_scalar_prefetch=1,
            grid=(n1 + n2,),
            in_specs=[
                pl.BlockSpec(parts.shape, lambda i, sc: (0, 0, 0)),
                pl.BlockSpec(log_src.shape, lambda i, sc: (0, 0)),
                pl.BlockSpec((B, ns), lambda i, sc: (jnp.minimum(i, n1 - 1), 0)),
                pl.BlockSpec((B, ns), lambda i, sc: (jnp.maximum(i - n1, 0), 0)),
            ],
            out_specs=[
                pl.BlockSpec((8, 128), lambda i, sc: (0, 0)),
                pl.BlockSpec((1, ns), lambda i, sc: (0, 0)),
                pl.BlockSpec((16, 8, 128), lambda i, sc: (0, 0, 0)),
            ],
            scratch_shapes=[pltpu.VMEM((8, 128), jnp.float32)],
        ),
        out_shape=[
            jax.ShapeDtypeStruct((8, 128), jnp.float32),
            jax.ShapeDtypeStruct((1, ns), jnp.float32),
            jax.ShapeDtypeStruct((16, 8, 128), jnp.float32),
        ],
    )(scal, parts, log_src, s1, s2)


def moved_kernel(scal, parts, lt1, lt2, sp, s1, s2, t1, t2, pot_out, mine_out, theirs_out, mass_out, tp1, tp2, lse):
    n = pl.program_id(0)

    @pl.when(n == 0)
    def _():
        lse[...] = merged_lse(parts[...])
        for p in range(len(OFF)):
            slot = scal[2 + p]
            row = lse[pl.ds(slot // 2, 1), :]
            row = jnp.where(slot % 2 == 0, row[:, :B], row[:, B:])
            first = p < len(OFF1)
            lt, tp, q = (lt1, tp1, p) if first else (lt2, tp2, p - len(OFF1))
            tpot = lt[q : q + 1, 0:B] * LOG2E - row
            if p == 0:
                pot_out[...] = tpot * LN2
            tp[q * B : (q + 1) * B, :] = jnp.broadcast_to(to_col(tpot), (B, 128))

    rep = CH // 128
    w1 = jnp.exp2(s1[...] + sp[...] + jnp.concatenate([tp1[...]] * rep, axis=1))
    w2 = jnp.exp2(s2[...] + sp[...] + jnp.concatenate([tp2[...]] * rep, axis=1))
    mass = jnp.sum(w1, axis=0, keepdims=True) + jnp.sum(w2, axis=0, keepdims=True)
    moved = jnp.dot(t1[...], w1.astype(jnp.bfloat16), preferred_element_type=jnp.float32)
    moved = moved + jnp.dot(t2[...], w2.astype(jnp.bfloat16), preferred_element_type=jnp.float32)
    half = moved.shape[0] // 2
    mass_out[...] = mass
    mine_out[...] = moved[:half].astype(jnp.bfloat16)
    theirs_out[0:half, :] = moved[half:].astype(jnp.bfloat16)
    hi = mass.astype(jnp.bfloat16)
    lo = (mass - hi.astype(jnp.float32)).astype(jnp.bfloat16)
    pad = jnp.zeros((6, mass.shape[1]), jnp.float32)
    theirs_out[half : half + 8, :] = jnp.concatenate([hi.astype(jnp.float32), lo.astype(jnp.float32), pad], axis=0).astype(jnp.bfloat16)


def moved_call(scal, parts, lt1, lt2, sp, s1, s2, t1, t2):
    ns = s1.shape[1]
    f = t1.shape[0]
    const2 = lambda a: pl.BlockSpec(a.shape, lambda n, sc: (0, 0))
    return pl.pallas_call(
        moved_kernel,
        name="moved",
        grid_spec=pltpu.PrefetchScalarGridSpec(
            num_scalar_prefetch=1,
            grid=(ns // CH,),
            in_specs=[
                pl.BlockSpec(parts.shape, lambda n, sc: (0, 0, 0)),
                const2(lt1),
                const2(lt2),
                pl.BlockSpec((1, CH), lambda n, sc: (0, n)),
                pl.BlockSpec((s1.shape[0], CH), lambda n, sc: (0, n)),
                pl.BlockSpec((s2.shape[0], CH), lambda n, sc: (0, n)),
                const2(t1),
                const2(t2),
            ],
            out_specs=[
                pl.BlockSpec((1, B), lambda n, sc: (0, 0)),
                pl.BlockSpec((f // 2, CH), lambda n, sc: (0, n)),
                pl.BlockSpec((f // 2 + 8, CH), lambda n, sc: (0, n)),
                pl.BlockSpec((1, CH), lambda n, sc: (0, n)),
            ],
            scratch_shapes=[
                pltpu.VMEM((s1.shape[0], 128), jnp.float32),
                pltpu.VMEM((s2.shape[0], 128), jnp.float32),
                pltpu.VMEM((8, 128), jnp.float32),
            ],
        ),
        out_shape=[
            jax.ShapeDtypeStruct((1, B), jnp.float32),
            jax.ShapeDtypeStruct((f // 2, ns), jnp.bfloat16),
            jax.ShapeDtypeStruct((f // 2 + 8, ns), jnp.bfloat16),
            jax.ShapeDtypeStruct((1, ns), jnp.float32),
        ],
    )(scal, parts, lt1, lt2, sp, s1, s2, t1, t2)


def pack_kernel(mine, theirs, mass, out):
    g = pl.program_id(0)
    f32 = jnp.float32
    both = mine[...].astype(f32) + theirs[pl.ds(pl.multiple_of(g * 32, 32), 32), :].astype(f32)
    extra = theirs[256:264, :].astype(f32)
    total = mass[...] + extra[0:1] + extra[1:2]
    hi = total.astype(jnp.bfloat16).astype(f32)
    lo = total - hi
    for h in range(2):
        for q in range(8):
            at = (h * 8 + q) * 128
            out[h, 0, q * 32 : (q + 1) * 32, :] = both[:, at : at + 128].astype(jnp.bfloat16)
        rows = [v[:, (h * 8 + q) * 128 : (h * 8 + q + 1) * 128] for v in (hi, lo) for q in range(8)]
        out[h, 0, 256:272, :] = jnp.concatenate(rows, axis=0).astype(jnp.bfloat16)


def pack_call(mine, theirs, mass):
    ns = mine.shape[1]
    return pl.pallas_call(
        pack_kernel,
        name="pack",
        grid=(8,),
        in_specs=[
            pl.BlockSpec((32, ns), lambda g: (g, 0)),
            pl.BlockSpec(theirs.shape, lambda g: (0, 0)),
            pl.BlockSpec(mass.shape, lambda g: (0, 0)),
        ],
        out_specs=pl.BlockSpec((2, 1, 272, 128), lambda g: (0, g, 0, 0)),
        out_shape=jax.ShapeDtypeStruct((2, 8, 272, 128), jnp.bfloat16),
    )(mine, theirs, mass)


def finish_kernel(parts, out):
    total = jnp.sum(parts[...].astype(jnp.float32), axis=0)
    for q in range(8):
        mass = total[256 + q : 257 + q, :] + total[264 + q : 265 + q, :]
        image = total[q * 32 : (q + 1) * 32, :] / mass
        out[q * 128 : (q + 1) * 128, :] = image.T.astype(jnp.bfloat16)


def finish_call(parts):
    return pl.pallas_call(
        finish_kernel,
        name="finish",
        out_shape=jax.ShapeDtypeStruct((1024, 32), jnp.bfloat16),
    )(parts)


def body(sources, log_src, targets, potential, log_tgt):
    bf = jnp.bfloat16
    f = sources.shape[1]
    scale2 = LOG2E / math.sqrt(f)
    z, yh, c = lax.axis_index("z"), lax.axis_index("yh"), lax.axis_index("c")
    scal = jnp.concatenate([jnp.stack([yh, c]), (z + jnp.array(OFF, jnp.int32)) % 16]).astype(jnp.int32)

    extra = jnp.stack(thirds(potential) + thirds(log_tgt) + [jnp.zeros_like(potential)] * 2)
    extra = jnp.pad(extra, ((0, 0), (0, f - B))).astype(bf)
    own = jnp.concatenate([targets, extra], axis=0)
    ls = jnp.pad(jnp.stack(thirds(log_src.reshape(2, 512)), axis=1), ((0, 0), (0, 5), (0, 0))).astype(bf)
    halves = jnp.concatenate([sources.reshape(2, 512, f), ls], axis=1)
    sent = lax.dynamic_index_in_dim(halves, c, 0, keepdims=False)
    ra = from_z(own, 4)
    la = from_z(own, -5)
    near = lax.ppermute(sent, ("yh", "yl"), [(0, 3), (3, 0), (1, 2), (2, 1)])
    rb = from_z(joined([own, ra]), 2)
    lb = from_z(joined([la, own]), -2)
    swapped = lax.ppermute(near, "c", [(0, 1), (1, 0)])
    rc = from_z(joined([own, rb, ra, la]), 1)
    lc = from_z(joined([own, lb, la]), -1)
    first = jnp.where(c == 0, near, swapped)
    second = jnp.where(c == 0, swapped, near)
    other = jnp.concatenate([first[:512], second[:512]], axis=0)
    whole = [first[512:].astype(jnp.float32), second[512:].astype(jnp.float32)]
    other_log = jnp.concatenate([w[0] + w[1] + w[2] for w in whole])
    src = jnp.concatenate([jnp.where(yh == 0, sources, other), jnp.where(yh == 0, other, sources)], axis=0)
    log_all = jnp.concatenate([jnp.where(yh == 0, log_src, other_log), jnp.where(yh == 0, other_log, log_src)])
    log_all = log_all.reshape(16, 128)

    s1, t1, lt1, lse1 = scores_call(scal, src, [own, ra, la, rb, lb], [(0, 0), (1, 0), (2, 0), (3, 0), (3, 1), (4, 0)], scale2)
    s2, t2, lt2, rows = scores_call(
        scal, src, [lb, rc, lc], [(0, 1)] + [(1, k) for k in range(5)] + [(2, k) for k in range(4)], scale2, lse1
    )
    row_parts = lax.all_to_all(rows, PLANE, split_axis=0, concat_axis=0, tiled=True)
    src_pot, sp, cols = cols_call(scal, row_parts, log_all, s1, s2)
    col_parts = lax.all_to_all(cols, "z", split_axis=0, concat_axis=0, tiled=True)
    tgt_pot, mine, theirs, mass = moved_call(scal, col_parts, lt1, lt2, sp, s1, s2, t1, t2)
    theirs = lax.ppermute(theirs, "c", [(0, 1), (1, 0)])
    packed = pack_call(mine, theirs, mass).reshape(16, 272, 128)
    parts = lax.all_to_all(packed, CHIPS, split_axis=0, concat_axis=0, tiled=True)
    mapped = finish_call(parts)
    return (src_pot.reshape(-1), tgt_pot.reshape(-1), mapped)


def solution(mesh):
    torus = Mesh(mesh.devices.reshape(16, 2, 2, 4, 2), AXES)
    src, every = ("z", "yh"), ("z", "yh", "yl", "x", "c")
    return jax.shard_map(
        body,
        mesh=torus,
        in_specs=(P(src, None), P(src), P(every, None), P(every), P(every)),
        out_specs=(P(src), P(every), P(src, ("yl", "x", "c"))),
        check_vma=False,
    )
```

```python
import math

import jax
import jax.numpy as jnp
from jax import lax
from jax.experimental import pallas as pl
from jax.experimental.pallas import tpu as pltpu
from jax.sharding import Mesh
from jax.sharding import PartitionSpec as P

AXES = ("z", "yh", "yl", "x", "c")
PLANE = ("yh", "yl", "x", "c")
CHIPS = ("yh", "yl", "x")
LOG2E = math.log2(math.e)
LN2 = math.log(2.0)
B = 64
A8 = 8
OFF1 = (0, 4, 11, 2, 6, 9)
OFF2 = (14, 1, 3, 7, 5, 12, 15, 8, 13, 10)
OFF = OFF1 + OFF2
PICKS = ((0, 0), (1, 0), (2, 0), (3, 0), (3, 1), (4, 0), (4, 1)) + tuple((5, k) for k in range(5)) + tuple((6, k) for k in range(4))
PICKS1 = PICKS[:6]
PICKS2 = tuple((m - 4, k) for m, k in PICKS[6:])


def from_z(array, d):
    n = lax.axis_size("z")
    return lax.ppermute(array, "z", [((i + d) % n, i) for i in range(n)])


def thirds(v):
    hi = lax.reduce_precision(v, 8, 7)
    lo = lax.reduce_precision(v - hi, 8, 7)
    return [hi, lo, v - hi - lo]


def joined(messages):
    ks = [m.shape[0] // (B + A8) for m in messages]
    rows = [m[: k * B] for m, k in zip(messages, ks)]
    extra = [m[k * B :] for m, k in zip(messages, ks)]
    return jnp.concatenate(rows + extra, axis=0)


def eye(n):
    return lax.broadcasted_iota(jnp.int32, (n, n), 0) == lax.broadcasted_iota(jnp.int32, (n, n), 1)


def to_col(row):
    n = row.shape[1]
    return jnp.sum(jnp.where(eye(n), jnp.broadcast_to(row, (n, n)), 0.0), axis=1, keepdims=True)


def to_row(col):
    n = col.shape[0]
    return jnp.sum(jnp.where(eye(n), jnp.broadcast_to(col, (n, n)), 0.0), axis=0, keepdims=True)


CH = 512
MIB = 1 << 20


def params(mib):
    return pltpu.CompilerParams(vmem_limit_bytes=mib * MIB)


SMEM = pl.BlockSpec(memory_space=pltpu.SMEM)
WHOLE = pl.BlockSpec(memory_space=pltpu.VMEM)


def block_of(msgs, m, k):
    total = msgs[m].shape[0] // (B + A8)
    extra = msgs[m][total * B + k * A8 : total * B + (k + 1) * A8, 0:128]
    return msgs[m].at[k * B : (k + 1) * B], extra.astype(jnp.float32)


def scores_kernel(picks, last, n_msg, scale2, src, *refs):
    msgs = refs[:n_msg]
    rest = refs[n_msg:]
    if last:
        lse_in, s_out, lse_out, tg, pot = rest
    else:
        s_out, lse_out, tg, pot = rest
    t = tg.shape[0]
    for p, (m, k) in enumerate(picks):
        rows, ex = block_of(msgs, m, k)
        tg[p * B : (p + 1) * B, :] = rows[...]
        po = (ex[0:1] + ex[1:2] + ex[2:3]) * LOG2E
        pot[p * B : (p + 1) * B, :] = jnp.broadcast_to(to_col(po[:, :B]), (B, 128))

    for n in range(src.shape[0] // CH):
        at = slice(n * CH, (n + 1) * CH)
        s_out[:, at] = (
            lax.dot_general(tg[...], src[at, :], (((1,), (1,)), ((), ())), preferred_element_type=jnp.float32) * scale2
        )

        def shifted(r):
            return s_out[r : r + 32, at] + jnp.concatenate([pot[r : r + 32, :]] * (CH // 128), axis=1)

        top = jnp.full((8, CH), -jnp.inf, jnp.float32)
        for r in range(0, t, 32):
            top = jnp.maximum(top, jnp.max(shifted(r).reshape(4, 8, CH), axis=0))
        top = jnp.max(top, axis=0, keepdims=True)
        tot = jnp.zeros((8, CH), jnp.float32)
        for r in range(0, t, 32):
            tot = tot + jnp.sum(jnp.exp2(shifted(r) - top).reshape(4, 8, CH), axis=0)
        lse = top + jnp.log2(jnp.sum(tot, axis=0, keepdims=True))
        if last:
            a = lse_in[:, at]
            hi = jnp.maximum(a, lse)
            lse = hi + jnp.log2(jnp.exp2(a - hi) + jnp.exp2(lse - hi))
            for i in range(CH // 128):
                piece = lse[:, i * 128 : (i + 1) * 128]
                q = n * (CH // 128) + i
                lse_out[:, q : q + 1, :] = jnp.broadcast_to(piece[None], (lse_out.shape[0], 1, 128))
        else:
            lse_out[:, at] = lse


def scores_call(src, msgs, picks, scale2, lse_in=None):
    t = len(picks) * B
    ns, f = src.shape
    last = lse_in is not None
    lse_shape = (32, ns // 128, 128) if last else (1, ns)
    args = [src, *msgs] + ([lse_in] if last else [])
    return pl.pallas_call(
        lambda *a: scores_kernel(picks, last, len(msgs), scale2, *a),
        name="scores_last" if last else "scores_first",
        in_specs=[WHOLE] * len(args),
        out_specs=[WHOLE] * 2,
        scratch_shapes=[pltpu.VMEM((t, f), jnp.bfloat16), pltpu.VMEM((t, 128), jnp.float32)],
        out_shape=[jax.ShapeDtypeStruct((t, ns), jnp.float32), jax.ShapeDtypeStruct(lse_shape, jnp.float32)],
        compiler_params=params(20),
        cost_estimate=pl.CostEstimate(flops=2 * t * ns * f, bytes_accessed=4 * t * ns, transcendentals=t * ns),
    )(*args)


def prepare_kernel(scal, *refs):
    msgs, (_, tgt_out, lt_out, tg) = refs[:-4], refs[-4:]
    core = scal[1]
    for p, (m, k) in enumerate(PICKS):
        rows, ex = block_of(msgs, m, k)
        tg[p * B : (p + 1) * B, :] = rows[...]
        lt_out[p : p + 1, :] = (ex[3:4] + ex[4:5] + ex[5:6]) * LOG2E
    for q in range(tg.shape[0] // 128):
        flipped = tg[q * 128 : (q + 1) * 128, :].T
        for t in range(16):
            at = pl.multiple_of((((t % 2) ^ core) * 8 + t // 2) * 32, 32)
            tgt_out[pl.ds(at, 32), q * 128 : (q + 1) * 128] = flipped[t * 32 : (t + 1) * 32, :]


def prepare_call(scal, msgs, after):
    t, f = len(OFF) * B, msgs[0].shape[1]
    return pl.pallas_call(
        prepare_kernel,
        name="prepare",
        in_specs=[SMEM] + [WHOLE] * len(msgs) + [pl.BlockSpec(memory_space=pl.ANY)],
        out_specs=[WHOLE] * 2,
        scratch_shapes=[pltpu.VMEM((t, f), jnp.bfloat16)],
        out_shape=[jax.ShapeDtypeStruct((f, t), jnp.bfloat16), jax.ShapeDtypeStruct((len(OFF), 128), jnp.float32)],
        compiler_params=params(16),
        cost_estimate=pl.CostEstimate(flops=2 * t * f * 1024, bytes_accessed=4 * t * f, transcendentals=0),
    )(scal, *msgs, after)


def merged_lse(parts):
    top = jnp.max(parts, axis=0)
    return top + jnp.log2(jnp.sum(jnp.exp2(parts - top[None]), axis=0))


def cols_kernel(scal, parts, log_src, s1, s2, pot_out, sp_out, msg_out, held):
    sp = log_src[...] * LOG2E - merged_lse(parts[...])
    for r in range(sp.shape[0]):
        sp_out[:, r * 128 : (r + 1) * 128] = sp[r : r + 1, :]
    mid = sp.shape[0] // 2
    pot_out[...] = jnp.where(scal[0] == 0, sp[:mid], sp[mid:]) * LN2
    held[...] = jnp.zeros_like(held)

    def step(s_ref, p, i):
        pieces = []
        for r in range(B // 8):
            lifted = s_ref[pl.ds(pl.multiple_of(p * B + r * 8, 8), 8), :] + sp_out[...]
            top = jnp.max(lifted, axis=1, keepdims=True)
            pieces.append(top + jnp.log2(jnp.sum(jnp.exp2(lifted - top), axis=1, keepdims=True)))
        row = to_row(jnp.concatenate(pieces, axis=0))
        row = jnp.concatenate([row, row], axis=1)
        slot = scal[2 + i]
        at = slot // 2
        half = lax.broadcasted_iota(jnp.int32, (1, 128), 1) // B
        held[pl.ds(at, 1), :] = jnp.where(half == slot % 2, row, held[pl.ds(at, 1), :])

    @pl.loop(0, len(OFF1))
    def _(p):
        step(s1, p, p)

    @pl.loop(0, len(OFF2))
    def _(p):
        step(s2, p, p + len(OFF1))

    msg_out[...] = jnp.broadcast_to(held[...][None], msg_out.shape)


def cols_call(scal, parts, log_src, s1, s2):
    ns = s1.shape[1]
    return pl.pallas_call(
        cols_kernel,
        name="cols",
        in_specs=[SMEM] + [WHOLE] * 4,
        out_specs=[WHOLE] * 3,
        scratch_shapes=[pltpu.VMEM((8, 128), jnp.float32)],
        out_shape=[
            jax.ShapeDtypeStruct((8, 128), jnp.float32),
            jax.ShapeDtypeStruct((1, ns), jnp.float32),
            jax.ShapeDtypeStruct((16, 8, 128), jnp.float32),
        ],
        compiler_params=params(16),
    )(scal, parts, log_src, s1, s2)


def moved_kernel(scal, parts, lt, sp, s1, s2, tgt, pot_out, mine_out, theirs_out, mass_out, tp, lse, *wide):
    lse[...] = merged_lse(parts[...])
    for p in range(len(OFF)):
        slot = scal[2 + p]
        row = lse[pl.ds(slot // 2, 1), :]
        row = jnp.where(slot % 2 == 0, row[:, :B], row[:, B:])
        tpot = lt[p : p + 1, 0:B] - row
        if p == 0:
            pot_out[...] = tpot * LN2
        tp[p * B : (p + 1) * B, :] = jnp.broadcast_to(to_col(tpot), (B, 128))

    t1 = s1.shape[0]
    half = tgt.shape[0] // 2
    for n in range(sp.shape[1] // CH):
        at = slice(n * CH, (n + 1) * CH)
        w = wide[n % len(wide)]
        spn = sp[:, at]
        mass = jnp.zeros((8, CH), jnp.float32)
        for r in range(0, tp.shape[0], 32):
            s_ref, q = (s1, r) if r < t1 else (s2, r - t1)
            e = jnp.exp2(s_ref[q : q + 32, at] + spn + jnp.concatenate([tp[r : r + 32, :]] * (CH // 128), axis=1))
            mass = mass + jnp.sum(e.reshape(4, 8, CH), axis=0)
            w[r : r + 32, :] = e.astype(jnp.bfloat16)
        mass = jnp.sum(mass, axis=0, keepdims=True)
        mass_out[:, at] = mass
        theirs_out[0:half, at] = jnp.dot(tgt[half:, :], w[...], preferred_element_type=jnp.float32).astype(jnp.bfloat16)
        mine_out[:, at] = jnp.dot(tgt[:half, :], w[...], preferred_element_type=jnp.float32).astype(jnp.bfloat16)
        hi = mass.astype(jnp.bfloat16).astype(jnp.float32)
        pad = jnp.zeros((6, CH), jnp.float32)
        theirs_out[half : half + 8, at] = jnp.concatenate([hi, mass - hi, pad], axis=0).astype(jnp.bfloat16)


def moved_call(scal, parts, lt, sp, s1, s2, tgt):
    ns = s1.shape[1]
    f, t = tgt.shape
    return pl.pallas_call(
        moved_kernel,
        name="moved",
        in_specs=[SMEM] + [WHOLE] * 6,
        out_specs=[WHOLE] * 4,
        scratch_shapes=[pltpu.VMEM((t, 128), jnp.float32), pltpu.VMEM((8, 128), jnp.float32)]
        + [pltpu.VMEM((t, CH), jnp.bfloat16)] * 2,
        out_shape=[
            jax.ShapeDtypeStruct((1, B), jnp.float32),
            jax.ShapeDtypeStruct((f // 2, ns), jnp.bfloat16),
            jax.ShapeDtypeStruct((f // 2 + 8, ns), jnp.bfloat16),
            jax.ShapeDtypeStruct((1, ns), jnp.float32),
        ],
        compiler_params=params(20),
    )(scal, parts, lt, sp, s1, s2, tgt)


def pack_kernel(mine, theirs, mass, out):
    f32 = jnp.float32
    extra = theirs[256:264, :].astype(f32)
    total = mass[...] + extra[0:1] + extra[1:2]
    hi = total.astype(jnp.bfloat16).astype(f32)
    lo = total - hi
    for h in range(2):
        rows = [v[:, (h * 8 + q) * 128 : (h * 8 + q + 1) * 128] for v in (hi, lo) for q in range(8)]
        rows = jnp.concatenate(rows, axis=0).astype(jnp.bfloat16)
        for g in range(8):
            for q in range(8):
                at = (slice(g * 32, (g + 1) * 32), slice((h * 8 + q) * 128, (h * 8 + q + 1) * 128))
                both = mine[at].astype(f32) + theirs[at].astype(f32)
                out[h * 8 + g, q * 32 : (q + 1) * 32, :] = both.astype(jnp.bfloat16)
            out[h * 8 + g, 256:272, :] = rows


def pack_call(mine, theirs, mass):
    return pl.pallas_call(
        pack_kernel,
        name="pack",
        in_specs=[WHOLE] * 3,
        out_specs=WHOLE,
        out_shape=jax.ShapeDtypeStruct((16, 272, 128), jnp.bfloat16),
        compiler_params=params(8),
    )(mine, theirs, mass)


def finish_kernel(parts, out):
    f32 = jnp.float32

    def added(at):
        total = parts[0, at, :].astype(f32)
        for k in range(1, parts.shape[0]):
            total = total + parts[k, at, :].astype(f32)
        return total

    mass = added(slice(256, 272))
    mass = mass[:8] + mass[8:]
    for q in range(8):
        image = added(slice(q * 32, (q + 1) * 32)) / mass[q : q + 1, :]
        out[:, q * 128 : (q + 1) * 128] = image.astype(jnp.bfloat16)


def finish_call(parts):
    return pl.pallas_call(
        finish_kernel,
        name="finish",
        in_specs=[WHOLE],
        out_specs=WHOLE,
        out_shape=jax.ShapeDtypeStruct((32, 1024), jnp.bfloat16),
        compiler_params=params(8),
    )(parts)


def body(sources, log_src, targets, potential, log_tgt):
    bf = jnp.bfloat16
    f = sources.shape[1]
    scale2 = LOG2E / math.sqrt(f)
    z, yh, c = lax.axis_index("z"), lax.axis_index("yh"), lax.axis_index("c")
    scal = jnp.concatenate([jnp.stack([yh, c]), (z + jnp.array(OFF, jnp.int32)) % 16]).astype(jnp.int32)

    extra = jnp.stack(thirds(potential) + thirds(log_tgt) + [jnp.zeros_like(potential)] * 2)
    extra = jnp.pad(extra, ((0, 0), (0, f - B))).astype(bf)
    own = jnp.concatenate([targets, extra], axis=0)
    ls = jnp.pad(jnp.stack(thirds(log_src.reshape(2, 512)), axis=1), ((0, 0), (0, 5), (0, 0))).astype(bf)
    halves = jnp.concatenate([sources.reshape(2, 512, f), ls], axis=1)
    sent = lax.dynamic_index_in_dim(halves, c, 0, keepdims=False)
    ra = from_z(own, 4)
    la = from_z(own, -5)
    near = lax.ppermute(sent, ("yh", "yl"), [(0, 3), (3, 0), (1, 2), (2, 1)])
    rb = from_z(joined([own, ra]), 2)
    lb = from_z(joined([la, own]), -2)
    swapped = lax.ppermute(near, "c", [(0, 1), (1, 0)])
    rc = from_z(joined([own, rb, ra, la]), 1)
    lc = from_z(joined([own, lb, la]), -1)
    first = jnp.where(c == 0, near, swapped)
    second = jnp.where(c == 0, swapped, near)
    other = jnp.concatenate([first[:512], second[:512]], axis=0)
    whole = [first[512:].astype(jnp.float32), second[512:].astype(jnp.float32)]
    other_log = jnp.concatenate([w[0] + w[1] + w[2] for w in whole])
    src = jnp.concatenate([jnp.where(yh == 0, sources, other), jnp.where(yh == 0, other, sources)], axis=0)
    log_all = jnp.concatenate([jnp.where(yh == 0, log_src, other_log), jnp.where(yh == 0, other_log, log_src)])
    log_all = log_all.reshape(16, 128)

    s1, lse1 = scores_call(src, [own, ra, la, rb, lb], PICKS1, scale2)
    s2, rows = scores_call(src, [lb, rc, lc], PICKS2, scale2, lse1)
    row_parts = lax.all_to_all(rows, PLANE, split_axis=0, concat_axis=0, tiled=True)
    tgt, lt = prepare_call(scal, [own, ra, la, rb, lb, rc, lc], rows)
    src_pot, sp, cols = cols_call(scal, row_parts, log_all, s1, s2)
    col_parts = lax.all_to_all(cols, "z", split_axis=0, concat_axis=0, tiled=True)
    tgt_pot, mine, theirs, mass = moved_call(scal, col_parts, lt, sp, s1, s2, tgt)
    theirs = lax.ppermute(theirs, "c", [(0, 1), (1, 0)])
    packed = pack_call(mine, theirs, mass)
    parts = lax.all_to_all(packed, CHIPS, split_axis=0, concat_axis=0, tiled=True)
    mapped = finish_call(parts).T
    return (src_pot.reshape(-1), tgt_pot.reshape(-1), mapped)


def solution(mesh):
    torus = Mesh(mesh.devices.reshape(16, 2, 2, 4, 2), AXES)
    src, every = ("z", "yh"), ("z", "yh", "yl", "x", "c")
    return jax.shard_map(
        body,
        mesh=torus,
        in_specs=(P(src, None), P(src), P(every, None), P(every), P(every)),
        out_specs=(P(src), P(every), P(src, ("yl", "x", "c"))),
        check_vma=False,
    )
```

```python
import math

import jax
import jax.numpy as jnp
from jax import lax
from jax.experimental import pallas as pl
from jax.experimental.pallas import tpu as pltpu
from jax.sharding import Mesh
from jax.sharding import PartitionSpec as P


AXES = ("z", "yh", "yl", "x", "c")
PLANE = ("yh", "yl", "x", "c")
CHIPS = ("yh", "yl", "x")
LOG2E = math.log2(math.e)
LN2 = math.log(2.0)
B = 64
A8 = 8
OFF1 = (0, 4, 11, 2, 6, 9)
OFF2 = (14, 1, 3, 7, 5, 12, 15, 8, 13, 10)
OFF = OFF1 + OFF2
PICKS = ((0, 0), (1, 0), (2, 0), (3, 0), (3, 1), (4, 0), (4, 1)) + tuple((5, k) for k in range(5)) + tuple((6, k) for k in range(4))
PICKS1 = PICKS[:6]
PICKS2 = PICKS[6:]


def from_z(array, d):
    n = lax.axis_size("z")
    return lax.ppermute(array, "z", [((i + d) % n, i) for i in range(n)])


def thirds(v):
    hi = lax.reduce_precision(v, 8, 7)
    lo = lax.reduce_precision(v - hi, 8, 7)
    return [hi, lo, v - hi - lo]


def own_kernel(targets, potential, log_tgt, out):
    f32, bf = jnp.float32, jnp.bfloat16
    rows = []
    for ref in (potential, log_tgt):
        v = ref[...]
        hi = v.astype(bf).astype(f32)
        lo = (v - hi).astype(bf).astype(f32)
        rows += [hi, lo, v - hi - lo]
    extra = jnp.concatenate(rows + [jnp.zeros((2, B), f32)], axis=0).astype(bf)
    out[0:B, :] = targets[...]
    out[B : B + A8, :] = jnp.concatenate([extra, jnp.zeros((A8, out.shape[1] - B), bf)], axis=1)


def own_call(targets, potential, log_tgt):
    return pl.pallas_call(
        own_kernel,
        name="own",
        in_specs=[WHOLE] * 3,
        out_specs=WHOLE,
        out_shape=jax.ShapeDtypeStruct((B + A8, targets.shape[1]), targets.dtype),
        compiler_params=params(4),
    )(targets, potential.reshape(1, B), log_tgt.reshape(1, B))


def joined(picks, msgs):
    def kernel(*refs):
        out = refs[-1]
        for p, (m, k) in enumerate(picks):
            total = refs[m].shape[0] // (B + A8)
            out[p * B : (p + 1) * B, :] = refs[m][k * B : (k + 1) * B, :]
            at = len(picks) * B + p * A8
            out[at : at + A8, :] = refs[m][total * B + k * A8 : total * B + (k + 1) * A8, :]

    return pl.pallas_call(
        kernel,
        in_specs=[WHOLE] * len(msgs),
        out_specs=WHOLE,
        out_shape=jax.ShapeDtypeStruct((len(picks) * (B + A8), msgs[0].shape[1]), msgs[0].dtype),
        compiler_params=params(4),
    )(*msgs)


def eye(n):
    return lax.broadcasted_iota(jnp.int32, (n, n), 0) == lax.broadcasted_iota(jnp.int32, (n, n), 1)


def to_col(row):
    n = row.shape[1]
    return jnp.sum(jnp.where(eye(n), jnp.broadcast_to(row, (n, n)), 0.0), axis=1, keepdims=True)


def to_row(col):
    n = col.shape[0]
    return jnp.sum(jnp.where(eye(n), jnp.broadcast_to(col, (n, n)), 0.0), axis=0, keepdims=True)


CH = 512
MIB = 1 << 20


def params(mib):
    return pltpu.CompilerParams(vmem_limit_bytes=mib * MIB)


SMEM = pl.BlockSpec(memory_space=pltpu.SMEM)
WHOLE = pl.BlockSpec(memory_space=pltpu.VMEM)


def block_of(msgs, m, k):
    total = msgs[m].shape[0] // (B + A8)
    extra = msgs[m][total * B + k * A8 : total * B + (k + 1) * A8, 0:128]
    return msgs[m].at[k * B : (k + 1) * B], extra.astype(jnp.float32)


def scores_kernel(picks, last, n_msg, scale2, src, *refs):
    msgs = refs[:n_msg]
    rest = refs[n_msg:]
    if last:
        lse_in, scal, s_out, lse_out, tgt_out, lt_out, tg, pot = rest
    else:
        s_out, lse_out, tg, pot = rest
    t = tg.shape[0]
    for p, (m, k) in enumerate(picks):
        rows, ex = block_of(msgs, m, k)
        tg[p * B : (p + 1) * B, :] = rows[...]
        po = (ex[0:1] + ex[1:2] + ex[2:3]) * LOG2E
        pot[p * B : (p + 1) * B, :] = jnp.broadcast_to(to_col(po[:, :B]), (B, 128))

    for n in range(src.shape[0] // CH):
        at = slice(n * CH, (n + 1) * CH)
        s_out[:, at] = (
            lax.dot_general(tg[...], src[at, :], (((1,), (1,)), ((), ())), preferred_element_type=jnp.float32) * scale2
        )

        def shifted(r):
            return s_out[r : r + 32, at] + jnp.concatenate([pot[r : r + 32, :]] * (CH // 128), axis=1)

        top = jnp.full((8, CH), -jnp.inf, jnp.float32)
        for r in range(0, t, 32):
            top = jnp.maximum(top, jnp.max(shifted(r).reshape(4, 8, CH), axis=0))
        top = jnp.max(top, axis=0, keepdims=True)
        tot = jnp.zeros((8, CH), jnp.float32)
        for r in range(0, t, 32):
            tot = tot + jnp.sum(jnp.exp2(shifted(r) - top).reshape(4, 8, CH), axis=0)
        lse = top + jnp.log2(jnp.sum(tot, axis=0, keepdims=True))
        if last:
            a = lse_in[:, at]
            hi = jnp.maximum(a, lse)
            lse = hi + jnp.log2(jnp.exp2(a - hi) + jnp.exp2(lse - hi))
            for i in range(CH // 128):
                piece = lse[:, i * 128 : (i + 1) * 128]
                q = n * (CH // 128) + i
                lse_out[:, q : q + 1, :] = jnp.broadcast_to(piece[None], (lse_out.shape[0], 1, 128))
        else:
            lse_out[:, at] = lse

    if last:
        core = scal[1]
        pieces = []
        for p, (m, k) in enumerate(PICKS):
            rows, ex = block_of(msgs, m, k)
            lt_out[p : p + 1, :] = (ex[3:4] + ex[4:5] + ex[5:6]) * LOG2E
            pieces.append(rows[...])
        for q in range(len(pieces) // 2):
            flipped = jnp.concatenate(pieces[2 * q : 2 * q + 2], axis=0).T
            for f in range(16):
                to = pl.multiple_of((((f % 2) ^ core) * 8 + f // 2) * 32, 32)
                tgt_out[pl.ds(to, 32), q * 128 : (q + 1) * 128] = flipped[f * 32 : (f + 1) * 32, :]


def scores_call(src, msgs, picks, scale2, lse_in=None, scal=None):
    t = len(picks) * B
    ns, f = src.shape
    last = lse_in is not None
    shapes = [jax.ShapeDtypeStruct((t, ns), jnp.float32)]
    if last:
        shapes += [
            jax.ShapeDtypeStruct((32, ns // 128, 128), jnp.float32),
            jax.ShapeDtypeStruct((f, len(OFF) * B), jnp.bfloat16),
            jax.ShapeDtypeStruct((len(OFF), 128), jnp.float32),
        ]
    else:
        shapes.append(jax.ShapeDtypeStruct((1, ns), jnp.float32))
    args = [src, *msgs] + ([lse_in] if last else [])
    return pl.pallas_call(
        lambda *a: scores_kernel(picks, last, len(msgs), scale2, *a),
        name="scores_last" if last else "scores_first",
        in_specs=[WHOLE] * len(args) + ([SMEM] if last else []),
        out_specs=[WHOLE] * len(shapes),
        scratch_shapes=[pltpu.VMEM((t, f), jnp.bfloat16), pltpu.VMEM((t, 128), jnp.float32)],
        out_shape=shapes,
        compiler_params=params(20),
        cost_estimate=pl.CostEstimate(flops=2 * t * ns * f, bytes_accessed=4 * t * ns, transcendentals=t * ns),
    )(*args, *([scal] if last else []))


def merged_lse(parts):
    top = jnp.max(parts, axis=0)
    return top + jnp.log2(jnp.sum(jnp.exp2(parts - top[None]), axis=0))


def cols_kernel(scal, parts, log_src, s1, s2, pot_out, sp_out, msg_out, held):
    sp = log_src[...] * LOG2E - merged_lse(parts[...])
    for r in range(sp.shape[0]):
        sp_out[:, r * 128 : (r + 1) * 128] = sp[r : r + 1, :]
    mid = sp.shape[0] // 2
    pot_out[...] = jnp.where(scal[0] == 0, sp[:mid], sp[mid:]) * LN2
    held[...] = jnp.zeros_like(held)

    def step(s_ref, p, i):
        pieces = []
        for r in range(B // 8):
            lifted = s_ref[p * B + r * 8 : p * B + r * 8 + 8, :] + sp_out[...]
            top = jnp.max(lifted, axis=1, keepdims=True)
            pieces.append(top + jnp.log2(jnp.sum(jnp.exp2(lifted - top), axis=1, keepdims=True)))
        row = to_row(jnp.concatenate(pieces, axis=0))
        row = jnp.concatenate([row, row], axis=1)
        slot = scal[2 + i]
        at = slot // 2
        half = lax.broadcasted_iota(jnp.int32, (1, 128), 1) // B
        held[pl.ds(at, 1), :] = jnp.where(half == slot % 2, row, held[pl.ds(at, 1), :])

    for p in range(len(OFF1)):
        step(s1, p, p)
    for p in range(len(OFF2)):
        step(s2, p, p + len(OFF1))

    msg_out[...] = jnp.broadcast_to(held[...][None], msg_out.shape)


def cols_call(scal, parts, log_src, s1, s2):
    ns = s1.shape[1]
    return pl.pallas_call(
        cols_kernel,
        name="cols",
        in_specs=[SMEM] + [WHOLE] * 4,
        out_specs=[WHOLE] * 3,
        scratch_shapes=[pltpu.VMEM((8, 128), jnp.float32)],
        out_shape=[
            jax.ShapeDtypeStruct((8, 128), jnp.float32),
            jax.ShapeDtypeStruct((1, ns), jnp.float32),
            jax.ShapeDtypeStruct((16, 8, 128), jnp.float32),
        ],
        compiler_params=params(16),
    )(scal, parts, log_src, s1, s2)


def moved_kernel(scal, parts, lt, sp, s1, s2, tgt, pot_out, mine_out, theirs_out, mass_out, tp, lse, *wide):
    lse[...] = merged_lse(parts[...])
    for p in range(len(OFF)):
        slot = scal[2 + p]
        row = lse[pl.ds(slot // 2, 1), :]
        row = jnp.where(slot % 2 == 0, row[:, :B], row[:, B:])
        tpot = lt[p : p + 1, 0:B] - row
        if p == 0:
            pot_out[...] = tpot * LN2
        tp[p * B : (p + 1) * B, :] = jnp.broadcast_to(to_col(tpot), (B, 128))

    t1 = s1.shape[0]
    half = tgt.shape[0] // 2
    for n in range(sp.shape[1] // CH):
        at = slice(n * CH, (n + 1) * CH)
        w = wide[n % len(wide)]
        spn = sp[:, at]
        mass = jnp.zeros((8, CH), jnp.float32)
        for r in range(0, tp.shape[0], 32):
            s_ref, q = (s1, r) if r < t1 else (s2, r - t1)
            e = jnp.exp2(s_ref[q : q + 32, at] + spn + jnp.concatenate([tp[r : r + 32, :]] * (CH // 128), axis=1))
            mass = mass + jnp.sum(e.reshape(4, 8, CH), axis=0)
            w[r : r + 32, :] = e.astype(jnp.bfloat16)
        mass = jnp.sum(mass, axis=0, keepdims=True)
        mass_out[:, at] = mass
        theirs_out[0:half, at] = jnp.dot(tgt[half:, :], w[...], preferred_element_type=jnp.float32).astype(jnp.bfloat16)
        mine_out[:, at] = jnp.dot(tgt[:half, :], w[...], preferred_element_type=jnp.float32).astype(jnp.bfloat16)
        hi = mass.astype(jnp.bfloat16).astype(jnp.float32)
        pad = jnp.zeros((6, CH), jnp.float32)
        theirs_out[half : half + 8, at] = jnp.concatenate([hi, mass - hi, pad], axis=0).astype(jnp.bfloat16)


def moved_call(scal, parts, lt, sp, s1, s2, tgt):
    ns = s1.shape[1]
    f, t = tgt.shape
    return pl.pallas_call(
        moved_kernel,
        name="moved",
        in_specs=[SMEM] + [WHOLE] * 6,
        out_specs=[WHOLE] * 4,
        scratch_shapes=[pltpu.VMEM((t, 128), jnp.float32), pltpu.VMEM((8, 128), jnp.float32)]
        + [pltpu.VMEM((t, CH), jnp.bfloat16)] * 2,
        out_shape=[
            jax.ShapeDtypeStruct((1, B), jnp.float32),
            jax.ShapeDtypeStruct((f // 2, ns), jnp.bfloat16),
            jax.ShapeDtypeStruct((f // 2 + 8, ns), jnp.bfloat16),
            jax.ShapeDtypeStruct((1, ns), jnp.float32),
        ],
        compiler_params=params(20),
    )(scal, parts, lt, sp, s1, s2, tgt)


def pack_kernel(mine, theirs, mass, out):
    f32 = jnp.float32
    extra = theirs[256:264, :].astype(f32)
    total = mass[...] + extra[0:1] + extra[1:2]
    hi = total.astype(jnp.bfloat16).astype(f32)
    lo = total - hi
    for h in range(2):
        rows = [v[:, (h * 8 + q) * 128 : (h * 8 + q + 1) * 128] for v in (hi, lo) for q in range(8)]
        rows = jnp.concatenate(rows, axis=0).astype(jnp.bfloat16)
        for g in range(8):
            for q in range(8):
                at = (slice(g * 32, (g + 1) * 32), slice((h * 8 + q) * 128, (h * 8 + q + 1) * 128))
                both = mine[at].astype(f32) + theirs[at].astype(f32)
                out[h * 8 + g, q * 32 : (q + 1) * 32, :] = both.astype(jnp.bfloat16)
            out[h * 8 + g, 256:272, :] = rows


def pack_call(mine, theirs, mass):
    return pl.pallas_call(
        pack_kernel,
        name="pack",
        in_specs=[WHOLE] * 3,
        out_specs=WHOLE,
        out_shape=jax.ShapeDtypeStruct((16, 272, 128), jnp.bfloat16),
        compiler_params=params(8),
    )(mine, theirs, mass)


def finish_kernel(parts, out):
    f32 = jnp.float32

    def added(at):
        total = parts[0, at, :].astype(f32)
        for k in range(1, parts.shape[0]):
            total = total + parts[k, at, :].astype(f32)
        return total

    mass = added(slice(256, 272))
    mass = mass[:8] + mass[8:]
    for q in range(8):
        image = added(slice(q * 32, (q + 1) * 32)) / mass[q : q + 1, :]
        out[:, q * 128 : (q + 1) * 128] = image.astype(jnp.bfloat16)


def finish_call(parts):
    return pl.pallas_call(
        finish_kernel,
        name="finish",
        in_specs=[WHOLE],
        out_specs=WHOLE,
        out_shape=jax.ShapeDtypeStruct((32, 1024), jnp.bfloat16),
        compiler_params=params(8),
    )(parts)


def body(sources, log_src, targets, potential, log_tgt):
    bf = jnp.bfloat16
    f = sources.shape[1]
    scale2 = LOG2E / math.sqrt(f)
    z, yh, c = lax.axis_index("z"), lax.axis_index("yh"), lax.axis_index("c")
    scal = jnp.concatenate([jnp.stack([yh, c]), (z + jnp.array(OFF, jnp.int32)) % 16]).astype(jnp.int32)

    own = own_call(targets, potential, log_tgt)
    ls = jnp.pad(jnp.stack(thirds(log_src.reshape(2, 512)), axis=1), ((0, 0), (0, 5), (0, 0))).astype(bf)
    halves = jnp.concatenate([sources.reshape(2, 512, f), ls], axis=1)
    mine = lax.dynamic_index_in_dim(halves, c, 0, keepdims=False)
    ra = from_z(own, 4)
    la = from_z(own, -5)
    near = lax.ppermute(mine, ("yh", "yl"), [(0, 3), (3, 0), (1, 2), (2, 1)])
    rb = from_z(joined([(0, 0), (1, 0)], [own, ra]), 2)
    lb = from_z(joined([(1, 0), (0, 0)], [own, la]), -2)
    swapped = lax.ppermute(near, "c", [(0, 1), (1, 0)])
    own_c, swapped = lax.optimization_barrier((own, swapped))
    rc = from_z(joined([(0, 0), (1, 0), (1, 1), (2, 0), (3, 0)], [own_c, rb, ra, la]), 1)
    lc = from_z(joined([(0, 0), (1, 0), (1, 1), (2, 0)], [own_c, lb, la]), -1)
    first = jnp.where(c == 0, near, swapped)
    second = jnp.where(c == 0, swapped, near)
    other = jnp.concatenate([first[:512], second[:512]], axis=0)
    whole = [first[512:].astype(jnp.float32), second[512:].astype(jnp.float32)]
    other_log = jnp.concatenate([w[0] + w[1] + w[2] for w in whole])
    src = jnp.concatenate([jnp.where(yh == 0, sources, other), jnp.where(yh == 0, other, sources)], axis=0)
    log_all = jnp.concatenate([jnp.where(yh == 0, log_src, other_log), jnp.where(yh == 0, other_log, log_src)])
    log_all = log_all.reshape(16, 128)

    msgs = [own, ra, la, rb, lb, rc, lc]
    s1, lse1 = scores_call(src, msgs[:5], PICKS1, scale2)
    s2, rows, tgt, lt = scores_call(src, msgs, PICKS2, scale2, lse1, scal)
    rows, log_all = lax.optimization_barrier((rows, log_all))
    row_parts = lax.all_to_all(rows, PLANE, split_axis=0, concat_axis=0, tiled=True)
    src_pot, sp, cols = cols_call(scal, row_parts, log_all, s1, s2)
    col_parts = lax.all_to_all(cols, "z", split_axis=0, concat_axis=0, tiled=True)
    tgt_pot, mine, theirs, mass = moved_call(scal, col_parts, lt, sp, s1, s2, tgt)
    theirs = lax.ppermute(theirs, "c", [(0, 1), (1, 0)])
    packed = pack_call(mine, theirs, mass)
    parts = lax.all_to_all(packed, CHIPS, split_axis=0, concat_axis=0, tiled=True)
    mapped = finish_call(parts).T
    return (src_pot.reshape(-1), tgt_pot.reshape(-1), mapped)


def solution(mesh):
    torus = Mesh(mesh.devices.reshape(16, 2, 2, 4, 2), AXES)
    src, every = ("z", "yh"), ("z", "yh", "yl", "x", "c")
    return jax.shard_map(
        body,
        mesh=torus,
        in_specs=(P(src, None), P(src), P(every, None), P(every), P(every)),
        out_specs=(P(src), P(every), P(src, ("yl", "x", "c"))),
        check_vma=False,
    )
```

```python
import math

import jax
import jax.numpy as jnp
from jax import lax
from jax.experimental import pallas as pl
from jax.experimental.pallas import tpu as pltpu
from jax.sharding import Mesh
from jax.sharding import PartitionSpec as P


WHOLE = pl.BlockSpec(memory_space=pltpu.VMEM)
FAR = pl.BlockSpec(memory_space=pltpu.HBM)
AXES = ("z", "yh", "yl", "x", "c")
PLANE = ("yh", "yl", "x", "c")
CHIPS = ("yh", "yl", "x")
LOG2E = math.log2(math.e)
LN2 = math.log(2.0)
B = 64
A8 = 8
OFF1 = (0, 4, 11, 2, 6, 9)
OFF2 = (14, 1, 3, 7, 5, 12, 15, 8, 13, 10)
OFF = OFF1 + OFF2
PICKS = ((0, 0), (1, 0), (2, 0), (3, 0), (3, 1), (4, 0), (4, 1)) + tuple((5, k) for k in range(5)) + tuple((6, k) for k in range(4))
PICKS1 = PICKS[:6]
PICKS2 = PICKS[6:]


MIB = 1 << 20


def params(mib):
    return pltpu.CompilerParams(vmem_limit_bytes=mib * MIB)


def from_z(array, d):
    n = lax.axis_size("z")
    return lax.ppermute(array, "z", [((i + d) % n, i) for i in range(n)])


def split(v):
    hi = v.astype(jnp.bfloat16).astype(jnp.float32)
    lo = (v - hi).astype(jnp.bfloat16).astype(jnp.float32)
    return [hi, lo, v - hi - lo]


def far(array):
    return pltpu.with_memory_space_constraint(array, pltpu.HBM)


def own_kernel(targets, potential, log_tgt, out, pot, log, sems):
    f32, bf = jnp.float32, jnp.bfloat16
    copies = [
        pltpu.make_async_copy(targets, out.at[0:B], sems.at[0]),
        pltpu.make_async_copy(potential, pot, sems.at[1]),
        pltpu.make_async_copy(log_tgt, log, sems.at[2]),
    ]
    for copy in copies:
        copy.start()
    for copy in copies:
        copy.wait()
    rows = []
    for ref in (pot, log):
        rows += split(ref[...])
    extra = jnp.concatenate(rows + [jnp.zeros((2, B), f32)], axis=0).astype(bf)
    out[B : B + A8, :] = jnp.concatenate([extra, jnp.zeros((A8, out.shape[1] - B), bf)], axis=1)


def own_call(targets, potential, log_tgt):
    return pl.pallas_call(
        own_kernel,
        name="own",
        in_specs=[FAR] * 3,
        out_specs=WHOLE,
        out_shape=jax.ShapeDtypeStruct((B + A8, targets.shape[1]), targets.dtype),
        scratch_shapes=[pltpu.VMEM((1, B), jnp.float32)] * 2 + [pltpu.SemaphoreType.DMA((3,))],
        compiler_params=params(4),
    )(*[far(a) for a in (targets, potential.reshape(1, B), log_tgt.reshape(1, B))])


def near_kernel(sources, log_src, out, log, sems):
    copies = [
        pltpu.make_async_copy(sources, out.at[0 : sources.shape[0]], sems.at[0]),
        pltpu.make_async_copy(log_src, log, sems.at[1]),
    ]
    for copy in copies:
        copy.start()
    for copy in copies:
        copy.wait()
    f = out.shape[1]
    rows = [part[:, h * f : (h + 1) * f] for part in split(log[...]) for h in range(2)]
    out[sources.shape[0] :, :] = jnp.concatenate(rows + [jnp.zeros((2, f), jnp.float32)], axis=0).astype(out.dtype)


def near_call(sources, log_src):
    n, f = sources.shape
    return pl.pallas_call(
        near_kernel,
        name="near_message",
        in_specs=[FAR] * 2,
        out_specs=WHOLE,
        out_shape=jax.ShapeDtypeStruct((n + A8, f), sources.dtype),
        scratch_shapes=[pltpu.VMEM((1, n), jnp.float32), pltpu.SemaphoreType.DMA((2,))],
        compiler_params=params(4),
    )(far(sources), far(log_src.reshape(1, n)))


def joined(picks, msgs):
    def kernel(*refs):
        out = refs[-1]
        extra = []
        for p, (m, k) in enumerate(picks):
            out[p * B : (p + 1) * B, :] = refs[m][k * B : (k + 1) * B, :]
            extra.append(refs[m][refs[m].shape[0] - A8 :, k * B : (k + 1) * B])
        rest = out.shape[1] - len(picks) * B
        extra.append(jnp.zeros((A8, rest), out.dtype))
        out[len(picks) * B :, :] = jnp.concatenate(extra, axis=1)

    return pl.pallas_call(
        kernel,
        in_specs=[WHOLE] * len(msgs),
        out_specs=WHOLE,
        out_shape=jax.ShapeDtypeStruct((len(picks) * B + A8, msgs[0].shape[1]), msgs[0].dtype),
        compiler_params=params(4),
    )(*msgs)


def eye(n):
    return lax.broadcasted_iota(jnp.int32, (n, n), 0) == lax.broadcasted_iota(jnp.int32, (n, n), 1)


def to_col(row):
    n = row.shape[1]
    return jnp.sum(jnp.where(eye(n), jnp.broadcast_to(row, (n, n)), 0.0), axis=1, keepdims=True)


def to_row(col):
    n = col.shape[0]
    return jnp.sum(jnp.where(eye(n), jnp.broadcast_to(col, (n, n)), 0.0), axis=0, keepdims=True)


CH = 512


def block_of(msgs, m, k):
    extra = msgs[m][msgs[m].shape[0] - A8 :, k * B : (k + 1) * B]
    return msgs[m].at[k * B : (k + 1) * B], extra.astype(jnp.float32)


def scores_kernel(picks, last, n_msg, scale2, src, *refs):
    msgs = refs[:n_msg]
    rest = refs[n_msg:]
    if last:
        lse_in, s_out, lse_out, tgt_out, lt_out, tg, pot = rest
    else:
        near, log_src, s_out, lse_out, log_out, tg, pot = rest
        yh = lax.axis_index("yh")
        logs = near[near.shape[0] - A8 :, :].astype(jnp.float32)
        logs = logs[0:2] + logs[2:4] + logs[4:6]
        for q in range(8):
            mine = log_src[:, q * 128 : (q + 1) * 128]
            other = logs[q // 4 : q // 4 + 1, q % 4 * 128 : (q % 4 + 1) * 128]
            log_out[q : q + 1, :] = jnp.where(yh == 0, mine, other) * LOG2E
            log_out[q + 8 : q + 9, :] = jnp.where(yh == 0, other, mine) * LOG2E
    t = tg.shape[0]
    for p, (m, k) in enumerate(picks):
        rows, ex = block_of(msgs, m, k)
        tg[p * B : (p + 1) * B, :] = rows[...]
        po = (ex[0:1] + ex[1:2] + ex[2:3]) * LOG2E
        pot[p * B : (p + 1) * B, :] = jnp.broadcast_to(to_col(po), (B, 128))

    for n in range(src.shape[0] // CH):
        at = slice(n * CH, (n + 1) * CH)
        s_out[:, at] = (
            lax.dot_general(tg[...], src[at, :], (((1,), (1,)), ((), ())), preferred_element_type=jnp.float32) * scale2
        )

        def shifted(r):
            return s_out[r : r + 32, at] + jnp.concatenate([pot[r : r + 32, :]] * (CH // 128), axis=1)

        top = jnp.full((8, CH), -jnp.inf, jnp.float32)
        for r in range(0, t, 32):
            top = jnp.maximum(top, jnp.max(shifted(r).reshape(4, 8, CH), axis=0))
        top = jnp.max(top, axis=0, keepdims=True)
        tot = jnp.zeros((8, CH), jnp.float32)
        for r in range(0, t, 32):
            tot = tot + jnp.sum(jnp.exp2(shifted(r) - top).reshape(4, 8, CH), axis=0)
        lse = top + jnp.log2(jnp.sum(tot, axis=0, keepdims=True))
        if last:
            a = lse_in[:, at]
            hi = jnp.maximum(a, lse)
            lse = hi + jnp.log2(jnp.exp2(a - hi) + jnp.exp2(lse - hi))
            for i in range(CH // 128):
                piece = lse[:, i * 128 : (i + 1) * 128]
                q = n * (CH // 128) + i
                lse_out[:, q : q + 1, :] = jnp.broadcast_to(piece[None], (lse_out.shape[0], 1, 128))
        else:
            lse_out[:, at] = lse

    if last:
        core = lax.axis_index("c")
        pieces = []
        for p, (m, k) in enumerate(PICKS):
            rows, ex = block_of(msgs, m, k)
            lt_out[p : p + 1, 0:B] = (ex[3:4] + ex[4:5] + ex[5:6]) * LOG2E
            pieces.append(rows[...])
        for q in range(len(pieces) // 2):
            flipped = jnp.concatenate(pieces[2 * q : 2 * q + 2], axis=0).T
            for f in range(16):
                to = pl.multiple_of((((f % 2) ^ core) * 8 + f // 2) * 32, 32)
                tgt_out[pl.ds(to, 32), q * 128 : (q + 1) * 128] = flipped[f * 32 : (f + 1) * 32, :]


def scores_call(src, msgs, picks, scale2, *more, last):
    t = len(picks) * B
    ns, f = src.shape
    shapes = [jax.ShapeDtypeStruct((t, ns), jnp.float32)]
    if last:
        shapes += [
            jax.ShapeDtypeStruct((32, ns // 128, 128), jnp.float32),
            jax.ShapeDtypeStruct((f, len(OFF) * B), jnp.bfloat16),
            jax.ShapeDtypeStruct((len(OFF), 128), jnp.float32),
        ]
    else:
        shapes += [jax.ShapeDtypeStruct((1, ns), jnp.float32), jax.ShapeDtypeStruct((ns // 128, 128), jnp.float32)]
    args = [src, *msgs, *more]
    return pl.pallas_call(
        lambda *a: scores_kernel(picks, last, len(msgs), scale2, *a),
        name="scores_last" if last else "scores_first",
        in_specs=[WHOLE] * len(args),
        out_specs=[WHOLE] * len(shapes),
        scratch_shapes=[pltpu.VMEM((t, f), jnp.bfloat16), pltpu.VMEM((t, 128), jnp.float32)],
        out_shape=shapes,
        compiler_params=params(20),
        cost_estimate=pl.CostEstimate(flops=2 * t * ns * f, bytes_accessed=4 * t * ns, transcendentals=t * ns),
    )(*args)


def merged_lse(parts):
    top = jnp.max(parts, axis=0)
    return top + jnp.log2(jnp.sum(jnp.exp2(parts - top[None]), axis=0))


def slot_of(p):
    return (lax.axis_index("z") + OFF[p]) % 16


def cols_kernel(parts, log_src, s1, s2, sp_out, msg_out, held):
    sp = log_src[...] - merged_lse(parts[...])
    for r in range(sp.shape[0]):
        sp_out[:, r * 128 : (r + 1) * 128] = sp[r : r + 1, :]
    held[...] = jnp.zeros_like(held)

    def step(s_ref, p, i):
        pieces = []
        for r in range(B // 8):
            lifted = s_ref[p * B + r * 8 : p * B + r * 8 + 8, :] + sp_out[...]
            top = jnp.max(lifted, axis=1, keepdims=True)
            pieces.append(top + jnp.log2(jnp.sum(jnp.exp2(lifted - top), axis=1, keepdims=True)))
        row = to_row(jnp.concatenate(pieces, axis=0))
        row = jnp.concatenate([row, row], axis=1)
        slot = slot_of(i)
        at = slot // 2
        half = lax.broadcasted_iota(jnp.int32, (1, 128), 1) // B
        held[pl.ds(at, 1), :] = jnp.where(half == slot % 2, row, held[pl.ds(at, 1), :])

    for p in range(len(OFF1)):
        step(s1, p, p)
    for p in range(len(OFF2)):
        step(s2, p, p + len(OFF1))

    msg_out[...] = jnp.broadcast_to(held[...][None], msg_out.shape)


def cols_call(parts, log_src, s1, s2):
    ns = s1.shape[1]
    return pl.pallas_call(
        cols_kernel,
        name="cols",
        in_specs=[WHOLE] * 4,
        out_specs=[WHOLE] * 2,
        scratch_shapes=[pltpu.VMEM((8, 128), jnp.float32)],
        out_shape=[jax.ShapeDtypeStruct((1, ns), jnp.float32), jax.ShapeDtypeStruct((16, 8, 128), jnp.float32)],
        compiler_params=params(16),
    )(parts, log_src, s1, s2)


def moved_kernel(parts, lt, sp, s1, s2, tgt, pot_out, theirs_out, mass_out, wide, tp, lse):
    lse[...] = merged_lse(parts[...])
    for p in range(len(OFF)):
        slot = slot_of(p)
        row = lse[pl.ds(slot // 2, 1), :]
        row = jnp.where(slot % 2 == 0, row[:, :B], row[:, B:])
        tpot = lt[p : p + 1, 0:B] - row
        if p == 0:
            pot_out[:, 0:B] = tpot * LN2
        tp[p * B : (p + 1) * B, :] = jnp.broadcast_to(to_col(tpot), (B, 128))

    t1 = s1.shape[0]
    half = tgt.shape[0] // 2
    for n in range(sp.shape[1] // CH):
        at = slice(n * CH, (n + 1) * CH)
        spn = sp[:, at]
        mass = jnp.zeros((8, CH), jnp.float32)
        for r in range(0, tp.shape[0], 32):
            s_ref, q = (s1, r) if r < t1 else (s2, r - t1)
            e = jnp.exp2(s_ref[q : q + 32, at] + spn + jnp.concatenate([tp[r : r + 32, :]] * (CH // 128), axis=1))
            mass = mass + jnp.sum(e.reshape(4, 8, CH), axis=0)
            wide[r : r + 32, at] = e.astype(jnp.bfloat16)
        mass = jnp.sum(mass, axis=0, keepdims=True)
        mass_out[:, at] = mass
        part = jnp.dot(tgt[half:, :], wide[:, at], preferred_element_type=jnp.float32)
        theirs_out[0:half, at] = part.astype(jnp.bfloat16)
        hi = mass.astype(jnp.bfloat16).astype(jnp.float32)
        pad = jnp.zeros((6, CH), jnp.float32)
        theirs_out[half : half + 8, at] = jnp.concatenate([hi, mass - hi, pad], axis=0).astype(jnp.bfloat16)


def moved_call(parts, lt, sp, s1, s2, tgt):
    ns = s1.shape[1]
    f, t = tgt.shape
    return pl.pallas_call(
        moved_kernel,
        name="moved",
        in_specs=[WHOLE] * 6,
        out_specs=[WHOLE] * 4,
        scratch_shapes=[pltpu.VMEM((t, 128), jnp.float32), pltpu.VMEM((8, 128), jnp.float32)],
        out_shape=[
            jax.ShapeDtypeStruct((1, 128), jnp.float32),
            jax.ShapeDtypeStruct((f // 2 + 8, ns), jnp.bfloat16),
            jax.ShapeDtypeStruct((1, ns), jnp.float32),
            jax.ShapeDtypeStruct((t, ns), jnp.bfloat16),
        ],
        compiler_params=params(20),
    )(parts, lt, sp, s1, s2, tgt)


def mine_kernel(tgt, wide, out):
    for n in range(out.shape[1] // CH):
        at = slice(n * CH, (n + 1) * CH)
        part = jnp.dot(tgt[: out.shape[0], :], wide[:, at], preferred_element_type=jnp.float32)
        out[:, at] = part.astype(jnp.bfloat16)


def mine_call(tgt, wide):
    f, t = tgt.shape
    ns = wide.shape[1]
    return pl.pallas_call(
        mine_kernel,
        name="mine",
        in_specs=[WHOLE] * 2,
        out_specs=WHOLE,
        out_shape=jax.ShapeDtypeStruct((f // 2, ns), jnp.bfloat16),
        compiler_params=params(12),
        cost_estimate=pl.CostEstimate(flops=f * t * ns, bytes_accessed=2 * t * ns, transcendentals=0),
    )(tgt, wide)


def pack_kernel(mine, theirs, mass, out):
    f32 = jnp.float32
    extra = theirs[256:264, :].astype(f32)
    total = mass[...] + extra[0:1] + extra[1:2]
    hi = total.astype(jnp.bfloat16).astype(f32)
    lo = total - hi
    for h in range(2):
        rows = [v[:, (h * 8 + q) * 128 : (h * 8 + q + 1) * 128] for v in (hi, lo) for q in range(8)]
        rows = jnp.concatenate(rows, axis=0).astype(jnp.bfloat16)
        for g in range(8):
            for q in range(8):
                at = (slice(g * 32, (g + 1) * 32), slice((h * 8 + q) * 128, (h * 8 + q + 1) * 128))
                both = mine[at].astype(f32) + theirs[at].astype(f32)
                out[h * 8 + g, q * 32 : (q + 1) * 32, :] = both.astype(jnp.bfloat16)
            out[h * 8 + g, 256:272, :] = rows


def pack_call(mine, theirs, mass):
    return pl.pallas_call(
        pack_kernel,
        name="pack",
        in_specs=[WHOLE] * 3,
        out_specs=WHOLE,
        out_shape=jax.ShapeDtypeStruct((16, 272, 128), jnp.bfloat16),
        compiler_params=params(8),
    )(mine, theirs, mass)


def finish_kernel(parts, sp, tpot, out, src_pot, tgt_pot):
    f32 = jnp.float32

    def added(at):
        total = parts[0, at, :].astype(f32)
        for k in range(1, parts.shape[0]):
            total = total + parts[k, at, :].astype(f32)
        return total

    first = lax.axis_index("yh") == 0
    for q in range(8):
        rows = [sp[:, (h * 8 + q) * 128 : (h * 8 + q + 1) * 128] for h in range(2)]
        src_pot[q : q + 1, :] = jnp.where(first, rows[0], rows[1]) * LN2
    tgt_pot[...] = tpot[:, 0:B]
    mass = added(slice(256, 272))
    mass = mass[:8] + mass[8:]
    for q in range(8):
        image = added(slice(q * 32, (q + 1) * 32)) / mass[q : q + 1, :]
        out[:, q * 128 : (q + 1) * 128] = image.astype(jnp.bfloat16)


def finish_call(parts, sp, tpot):
    return pl.pallas_call(
        finish_kernel,
        name="finish",
        in_specs=[WHOLE] * 3,
        out_specs=[WHOLE] * 3,
        out_shape=[
            jax.ShapeDtypeStruct((32, 1024), jnp.bfloat16),
            jax.ShapeDtypeStruct((8, 128), jnp.float32),
            jax.ShapeDtypeStruct((1, B), jnp.float32),
        ],
        compiler_params=params(8),
    )(parts, sp, tpot)


def body(sources, log_src, targets, potential, log_tgt):
    f = sources.shape[1]
    scale2 = LOG2E / math.sqrt(f)
    yh = lax.axis_index("yh")

    own = own_call(targets, potential, log_tgt)
    ra = from_z(own, 4)
    la = from_z(own, -5)
    near = lax.ppermute(near_call(sources, log_src), ("yh", "yl"), [(0, 3), (3, 0), (1, 2), (2, 1)])
    rb = from_z(joined([(0, 0), (1, 0)], [own, ra]), 2)
    lb = from_z(joined([(1, 0), (0, 0)], [own, la]), -2)
    rc = from_z(joined([(0, 0), (1, 0), (1, 1), (2, 0), (3, 0)], [own, rb, ra, la]), 1)
    lc = from_z(joined([(0, 0), (1, 0), (1, 1), (2, 0)], [own, lb, la]), -1)
    other = near[: sources.shape[0]]
    src = jnp.concatenate([jnp.where(yh == 0, sources, other), jnp.where(yh == 0, other, sources)], axis=0)
    msgs = [own, ra, la, rb, lb, rc, lc]
    s1, lse1, log_all = scores_call(src, msgs[:5], PICKS1, scale2, near, log_src.reshape(1, -1), last=False)
    s2, rows, tgt, lt = scores_call(src, msgs, PICKS2, scale2, lse1, last=True)
    row_parts = lax.all_to_all(rows, PLANE, split_axis=0, concat_axis=0, tiled=True)
    sp, cols = cols_call(row_parts, log_all, s1, s2)
    col_parts = lax.all_to_all(cols, "z", split_axis=0, concat_axis=0, tiled=True)
    tpot, theirs, mass, wide = moved_call(col_parts, lt, sp, s1, s2, tgt)
    theirs = lax.ppermute(theirs, "c", [(0, 1), (1, 0)])
    packed = pack_call(mine_call(tgt, wide), theirs, mass)
    parts = lax.all_to_all(packed, CHIPS, split_axis=0, concat_axis=0, tiled=True)
    mapped, src_pot, tgt_pot = finish_call(parts, sp, tpot)
    return (src_pot.reshape(-1), tgt_pot.reshape(-1), mapped.T)


def solution(mesh):
    torus = Mesh(mesh.devices.reshape(16, 2, 2, 4, 2), AXES)
    src, every = ("z", "yh"), ("z", "yh", "yl", "x", "c")
    return jax.shard_map(
        body,
        mesh=torus,
        in_specs=(P(src, None), P(src), P(every, None), P(every), P(every)),
        out_specs=(P(src), P(every), P(src, ("yl", "x", "c"))),
        check_vma=False,
    )
```

```python
import math

import jax
import jax.numpy as jnp
from jax import lax
from jax.experimental import pallas as pl
from jax.experimental.pallas import tpu as pltpu
from jax.sharding import Mesh
from jax.sharding import PartitionSpec as P


WHOLE = pl.BlockSpec(memory_space=pltpu.VMEM)
FAR = pl.BlockSpec(memory_space=pltpu.HBM)
AXES = ("z", "yh", "yl", "x", "c")
PLANE = ("c", "x", "yh", "yl")
CHIPS = ("x", "yh", "yl")
LOG2E = math.log2(math.e)
LN2 = math.log(2.0)
B = 64
A8 = 8
OFF1 = (0, 4, 11, 2, 6, 9)
OFF2 = (14, 1, 3, 7, 5, 12, 15, 8, 13, 10)
OFF = OFF1 + OFF2
PICKS = ((0, 0), (1, 0), (2, 0), (3, 0), (3, 1), (4, 0), (4, 1)) + tuple((5, k) for k in range(5)) + tuple((6, k) for k in range(4))
PICKS1 = PICKS[:6]
PICKS2 = PICKS[6:]


MIB = 1 << 20


def params(mib):
    return pltpu.CompilerParams(vmem_limit_bytes=mib * MIB)


def from_z(array, d):
    n = lax.axis_size("z")
    return lax.ppermute(array, "z", [((i + d) % n, i) for i in range(n)])


def split(v):
    hi = v.astype(jnp.bfloat16).astype(jnp.float32)
    lo = (v - hi).astype(jnp.bfloat16).astype(jnp.float32)
    return [hi, lo, v - hi - lo]


def far(array):
    return pltpu.with_memory_space_constraint(array, pltpu.HBM)


def own_kernel(targets, potential, log_tgt, out, pot, log, sems):
    f32, bf = jnp.float32, jnp.bfloat16
    copies = [
        pltpu.make_async_copy(targets, out.at[0:B], sems.at[0]),
        pltpu.make_async_copy(potential, pot, sems.at[1]),
        pltpu.make_async_copy(log_tgt, log, sems.at[2]),
    ]
    for copy in copies:
        copy.start()
    for copy in copies:
        copy.wait()
    rows = []
    for ref in (pot, log):
        rows += split(ref[...])
    extra = jnp.concatenate(rows + [jnp.zeros((2, B), f32)], axis=0).astype(bf)
    out[B : B + A8, :] = jnp.concatenate([extra, jnp.zeros((A8, out.shape[1] - B), bf)], axis=1)


def own_call(targets, potential, log_tgt):
    return pl.pallas_call(
        own_kernel,
        name="own",
        in_specs=[FAR] * 3,
        out_specs=WHOLE,
        out_shape=jax.ShapeDtypeStruct((B + A8, targets.shape[1]), targets.dtype),
        scratch_shapes=[pltpu.VMEM((1, B), jnp.float32)] * 2 + [pltpu.SemaphoreType.DMA((3,))],
        compiler_params=params(4),
    )(*[far(a) for a in (targets, potential.reshape(1, B), log_tgt.reshape(1, B))])


def near_kernel(sources, log_src, out, log, sems):
    copies = [
        pltpu.make_async_copy(sources, out.at[0 : sources.shape[0]], sems.at[0]),
        pltpu.make_async_copy(log_src, log, sems.at[1]),
    ]
    for copy in copies:
        copy.start()
    for copy in copies:
        copy.wait()
    f = out.shape[1]
    rows = [part[:, h * f : (h + 1) * f] for part in split(log[...]) for h in range(2)]
    out[sources.shape[0] :, :] = jnp.concatenate(rows + [jnp.zeros((2, f), jnp.float32)], axis=0).astype(out.dtype)


def near_call(sources, log_src):
    n, f = sources.shape
    return pl.pallas_call(
        near_kernel,
        name="near_message",
        in_specs=[FAR] * 2,
        out_specs=WHOLE,
        out_shape=jax.ShapeDtypeStruct((n + A8, f), sources.dtype),
        scratch_shapes=[pltpu.VMEM((1, n), jnp.float32), pltpu.SemaphoreType.DMA((2,))],
        compiler_params=params(4),
    )(far(sources), far(log_src.reshape(1, n)))


def joined(picks, msgs):
    def kernel(*refs):
        out = refs[-1]
        extra = []
        for p, (m, k) in enumerate(picks):
            out[p * B : (p + 1) * B, :] = refs[m][k * B : (k + 1) * B, :]
            extra.append(refs[m][refs[m].shape[0] - A8 :, k * B : (k + 1) * B])
        rest = out.shape[1] - len(picks) * B
        extra.append(jnp.zeros((A8, rest), out.dtype))
        out[len(picks) * B :, :] = jnp.concatenate(extra, axis=1)

    return pl.pallas_call(
        kernel,
        in_specs=[WHOLE] * len(msgs),
        out_specs=WHOLE,
        out_shape=jax.ShapeDtypeStruct((len(picks) * B + A8, msgs[0].shape[1]), msgs[0].dtype),
        compiler_params=params(4),
    )(*msgs)


def eye(n):
    return lax.broadcasted_iota(jnp.int32, (n, n), 0) == lax.broadcasted_iota(jnp.int32, (n, n), 1)


def to_col(row):
    n = row.shape[1]
    return jnp.sum(jnp.where(eye(n), jnp.broadcast_to(row, (n, n)), 0.0), axis=1, keepdims=True)


def to_row(col):
    n = col.shape[0]
    return jnp.sum(jnp.where(eye(n), jnp.broadcast_to(col, (n, n)), 0.0), axis=0, keepdims=True)


CH = 512


def block_of(msgs, m, k):
    extra = msgs[m][msgs[m].shape[0] - A8 :, k * B : (k + 1) * B]
    return msgs[m].at[k * B : (k + 1) * B], extra.astype(jnp.float32)


def row_lse(s_out, at, pot):
    t = pot.shape[0]

    def shifted(r):
        return s_out[r : r + 32, at] + jnp.concatenate([pot[r : r + 32, :]] * (CH // 128), axis=1)

    top = jnp.full((8, CH), -jnp.inf, jnp.float32)
    for r in range(0, t, 32):
        top = jnp.maximum(top, jnp.max(shifted(r).reshape(4, 8, CH), axis=0))
    top = jnp.max(top, axis=0, keepdims=True)
    tot = jnp.zeros((8, CH), jnp.float32)
    for r in range(0, t, 32):
        tot = tot + jnp.sum(jnp.exp2(shifted(r) - top).reshape(4, 8, CH), axis=0)
    return top + jnp.log2(jnp.sum(tot, axis=0, keepdims=True))


def scores(tg, src, scale2):
    return lax.dot_general(tg, src, (((1,), (1,)), ((), ())), preferred_element_type=jnp.float32) * scale2


def laid_out(msgs, picks, tg, pot):
    for p, (m, k) in enumerate(picks):
        rows, ex = block_of(msgs, m, k)
        tg[p * B : (p + 1) * B, :] = rows[...]
        po = (ex[0:1] + ex[1:2] + ex[2:3]) * LOG2E
        pot[p * B : (p + 1) * B, :] = jnp.broadcast_to(to_col(po), (B, 128))


def own_first_kernel(scale2, src, *refs):
    msgs, (s_out, lse_out, tg, pot) = refs[:-4], refs[-4:]
    laid_out(msgs, PICKS1, tg, pot)
    for n in range(src.shape[0] // CH):
        at = slice(n * CH, (n + 1) * CH)
        s_out[:, at] = scores(tg[...], src[at, :], scale2)
        lse_out[:, at] = row_lse(s_out, at, pot)


def own_last_kernel(scale2, src, lse_in, tg1, pot1, *refs):
    msgs, (s_out, lse_out, tgs, pots, tgt_out, lt_out, tg, pot) = refs[:-8], refs[-8:]
    laid_out(msgs, PICKS2, tg, pot)
    for n in range(src.shape[0] // CH):
        at = slice(n * CH, (n + 1) * CH)
        s_out[:, at] = scores(tg[...], src[at, :], scale2)
        lse_out[:, at] = added_lse(lse_in[:, at], row_lse(s_out, at, pot))
    t1 = tg1.shape[0]
    tgs[:t1, :] = tg1[...]
    tgs[t1:, :] = tg[...]
    pots[:t1, :] = pot1[...]
    pots[t1:, :] = pot[...]
    core = lax.axis_index("c")
    for p, (m, k) in enumerate(PICKS):
        _, ex = block_of(msgs, m, k)
        lt_out[p : p + 1, 0:B] = (ex[3:4] + ex[4:5] + ex[5:6]) * LOG2E
    for q in range(tgs.shape[0] // 128):
        at = slice(q * 128, (q + 1) * 128)
        flipped = (tg1[at, :] if q * 128 < t1 else tg[q * 128 - t1 : (q + 1) * 128 - t1, :]).T
        for f in range(16):
            to = pl.multiple_of((((f % 2) ^ core) * 8 + f // 2) * 32, 32)
            tgt_out[pl.ds(to, 32), at] = flipped[f * 32 : (f + 1) * 32, :]


def near_scores_kernel(scale2, near, log_src, lse_in, tgs, pots, s_out, rows_out, log_out):
    yh = lax.axis_index("yh")
    ns = near.shape[0] - A8
    logs = near[ns:, :].astype(jnp.float32)
    logs = logs[0:2] + logs[2:4] + logs[4:6]
    for q in range(8):
        log_out[0, q : q + 1, :] = log_src[:, q * 128 : (q + 1) * 128] * LOG2E
        log_out[1, q : q + 1, :] = logs[q // 4 : q // 4 + 1, q % 4 * 128 : (q % 4 + 1) * 128] * LOG2E
    for n in range(ns // CH):
        at = slice(n * CH, (n + 1) * CH)
        s_out[:, at] = scores(tgs[...], near[at, :], scale2)
        for block, lse in ((yh, lse_in[:, at]), (1 - yh, row_lse(s_out, at, pots))):
            for i in range(CH // 128):
                piece = jnp.broadcast_to(lse[:, i * 128 : (i + 1) * 128][None], (rows_out.shape[0], 1, 128))
                q = n * (CH // 128) + i
                rows_out[:, block, q : q + 1, :] = piece


def added_lse(a, b):
    top = jnp.maximum(a, b)
    return top + jnp.log2(jnp.exp2(a - top) + jnp.exp2(b - top))


def scores_call(kernel, scale2, args, shapes, scratch, flops):
    return pl.pallas_call(
        lambda *a: kernel(scale2, *a),
        in_specs=[WHOLE] * len(args),
        out_specs=[WHOLE] * len(shapes),
        scratch_shapes=[pltpu.VMEM(s, d) for s, d in scratch],
        out_shape=[jax.ShapeDtypeStruct(s, d) for s, d in shapes],
        compiler_params=params(20),
        cost_estimate=pl.CostEstimate(flops=flops, bytes_accessed=1 << 22, transcendentals=1 << 20),
    )(*args)


def all_scores(sources, log_src, near, msgs, scale2):
    ns, f = sources.shape
    f32, bf = jnp.float32, jnp.bfloat16
    t1, t2 = len(PICKS1) * B, len(PICKS2) * B
    t = t1 + t2
    flops = lambda rows: 2 * rows * ns * f
    s1, lse1, tg1, pot1 = scores_call(
        own_first_kernel, scale2, [sources, *msgs[:5]],
        [((t1, ns), f32), ((1, ns), f32), ((t1, f), bf), ((t1, 128), f32)], [], flops(t1),
    )
    s2, lse2, tgs, pots, tgt, lt = scores_call(
        own_last_kernel, scale2, [sources, lse1, tg1, pot1, *msgs],
        [((t2, ns), f32), ((1, ns), f32), ((t, f), bf), ((t, 128), f32), ((f, t), bf), ((len(OFF), 128), f32)],
        [((t2, f), bf), ((t2, 128), f32)], flops(t2),
    )
    s3, rows, logs = scores_call(
        near_scores_kernel, scale2, [near, log_src.reshape(1, ns), lse2, tgs, pots],
        [((t, ns), f32), ((32, 2, ns // 128, 128), f32), ((2, ns // 128, 128), f32)], [], flops(t),
    )
    return (s1, s2, s3), rows, logs, tgt, lt


def merged_lse(parts):
    top = jnp.max(parts, axis=0)
    return top + jnp.log2(jnp.sum(jnp.exp2(parts - top[None]), axis=0))


def slot_of(p):
    return (lax.axis_index("z") + OFF[p]) % 16


def cols_kernel(parts, logs, s1, s2, s3, sp_out, msg_out, held, lse):
    yh = lax.axis_index("yh")
    for h in range(2):
        lse[h] = merged_lse(parts[:, h])
    for h, block in enumerate((yh, 1 - yh)):
        sp = logs[h] - lse[block]
        for r in range(8):
            sp_out[:, (h * 8 + r) * 128 : (h * 8 + r + 1) * 128] = sp[r : r + 1, :]
    held[...] = jnp.zeros_like(held)
    ns = s1.shape[1]
    n1 = len(OFF1)
    for p in range(len(OFF)):
        s_ref, base = (s1, p * B) if p < n1 else (s2, (p - n1) * B)
        pieces = []
        for r in range(0, B, 8):
            mine = s_ref[base + r : base + r + 8, :] + sp_out[:, :ns]
            other = s3[p * B + r : p * B + r + 8, :] + sp_out[:, ns:]
            top = jnp.max(jnp.maximum(mine, other), axis=1, keepdims=True)
            total = jnp.sum(jnp.exp2(mine - top) + jnp.exp2(other - top), axis=1, keepdims=True)
            pieces.append(top + jnp.log2(total))
        row = to_row(jnp.concatenate(pieces, axis=0))
        row = jnp.concatenate([row, row], axis=1)
        slot = slot_of(p)
        at = slot // 2
        half = lax.broadcasted_iota(jnp.int32, (1, 128), 1) // B
        held[pl.ds(at, 1), :] = jnp.where(half == slot % 2, row, held[pl.ds(at, 1), :])
    msg_out[...] = jnp.broadcast_to(held[...][None], msg_out.shape)


def cols_call(parts, logs, s):
    ns = s[0].shape[1]
    return pl.pallas_call(
        cols_kernel,
        name="cols",
        in_specs=[WHOLE] * 5,
        out_specs=[WHOLE] * 2,
        scratch_shapes=[pltpu.VMEM((8, 128), jnp.float32), pltpu.VMEM((2, 8, 128), jnp.float32)],
        out_shape=[jax.ShapeDtypeStruct((1, 2 * ns), jnp.float32), jax.ShapeDtypeStruct((16, 8, 128), jnp.float32)],
        compiler_params=params(16),
    )(parts, logs, *s)


def moved_kernel(parts, lt, sp, s1, s2, s3, tgt, pot_out, theirs_out, mass_out, wide, tp, lse):
    lse[...] = merged_lse(parts[...])
    for p in range(len(OFF)):
        slot = slot_of(p)
        row = lse[pl.ds(slot // 2, 1), :]
        row = jnp.where(slot % 2 == 0, row[:, :B], row[:, B:])
        tpot = lt[p : p + 1, 0:B] - row
        if p == 0:
            pot_out[:, 0:B] = tpot * LN2
        tp[p * B : (p + 1) * B, :] = jnp.broadcast_to(to_col(tpot), (B, 128))

    t1 = s1.shape[0]
    ns = s1.shape[1]
    half = tgt.shape[0] // 2
    for n in range(sp.shape[1] // CH):
        at = slice(n * CH, (n + 1) * CH)
        spn = sp[:, at]
        mass = jnp.zeros((8, CH), jnp.float32)
        for r in range(0, tp.shape[0], 32):
            if n * CH < ns:
                s = s1[r : r + 32, at] if r < t1 else s2[r - t1 : r - t1 + 32, at]
            else:
                s = s3[r : r + 32, n * CH - ns : (n + 1) * CH - ns]
            e = jnp.exp2(s + spn + jnp.concatenate([tp[r : r + 32, :]] * (CH // 128), axis=1))
            mass = mass + jnp.sum(e.reshape(4, 8, CH), axis=0)
            wide[r : r + 32, at] = e.astype(jnp.bfloat16)
        mass = jnp.sum(mass, axis=0, keepdims=True)
        mass_out[:, at] = mass
        part = jnp.dot(tgt[half:, :], wide[:, at], preferred_element_type=jnp.float32)
        theirs_out[0:half, at] = part.astype(jnp.bfloat16)
        hi = mass.astype(jnp.bfloat16).astype(jnp.float32)
        pad = jnp.zeros((6, CH), jnp.float32)
        theirs_out[half : half + 8, at] = jnp.concatenate([hi, mass - hi, pad], axis=0).astype(jnp.bfloat16)


def moved_call(parts, lt, sp, s, tgt):
    ns = sp.shape[1]
    f, t = tgt.shape
    return pl.pallas_call(
        moved_kernel,
        name="moved",
        in_specs=[WHOLE] * 7,
        out_specs=[WHOLE] * 4,
        scratch_shapes=[pltpu.VMEM((t, 128), jnp.float32), pltpu.VMEM((8, 128), jnp.float32)],
        out_shape=[
            jax.ShapeDtypeStruct((1, 128), jnp.float32),
            jax.ShapeDtypeStruct((f // 2 + 8, ns), jnp.bfloat16),
            jax.ShapeDtypeStruct((1, ns), jnp.float32),
            jax.ShapeDtypeStruct((t, ns), jnp.bfloat16),
        ],
        compiler_params=params(20),
    )(parts, lt, sp, *s, tgt)


def mine_kernel(tgt, wide, out):
    for n in range(out.shape[1] // CH):
        at = slice(n * CH, (n + 1) * CH)
        part = jnp.dot(tgt[: out.shape[0], :], wide[:, at], preferred_element_type=jnp.float32)
        out[:, at] = part.astype(jnp.bfloat16)


def mine_call(tgt, wide):
    f, t = tgt.shape
    ns = wide.shape[1]
    return pl.pallas_call(
        mine_kernel,
        name="mine",
        in_specs=[WHOLE] * 2,
        out_specs=WHOLE,
        out_shape=jax.ShapeDtypeStruct((f // 2, ns), jnp.bfloat16),
        compiler_params=params(12),
        cost_estimate=pl.CostEstimate(flops=f * t * ns, bytes_accessed=2 * t * ns, transcendentals=0),
    )(tgt, wide)


def pack_kernel(mine, theirs, mass, out):
    f32 = jnp.float32
    extra = theirs[256:264, :].astype(f32)
    total = mass[...] + extra[0:1] + extra[1:2]
    hi = total.astype(jnp.bfloat16).astype(f32)
    lo = total - hi
    yh = lax.axis_index("yh")
    for h in range(2):
        to = (h ^ yh) * 2
        rows = [v[:, (h * 8 + q) * 128 : (h * 8 + q + 1) * 128] for v in (hi, lo) for q in range(8)]
        rows = jnp.concatenate(rows, axis=0).astype(jnp.bfloat16)
        for g in range(8):
            at_chip = g % 4 * 4 + g // 4
            for q in range(8):
                at = (slice(g * 32, (g + 1) * 32), slice((h * 8 + q) * 128, (h * 8 + q + 1) * 128))
                both = mine[at].astype(f32) + theirs[at].astype(f32)
                out[to + at_chip, q * 32 : (q + 1) * 32, :] = both.astype(jnp.bfloat16)
            out[to + at_chip, 256:272, :] = rows


def pack_call(mine, theirs, mass):
    return pl.pallas_call(
        pack_kernel,
        name="pack",
        in_specs=[WHOLE] * 3,
        out_specs=WHOLE,
        out_shape=jax.ShapeDtypeStruct((16, 272, 128), jnp.bfloat16),
        compiler_params=params(8),
    )(mine, theirs, mass)


def finish_kernel(parts, sp, tpot, out, src_pot, tgt_pot):
    f32 = jnp.float32

    def added(at):
        total = parts[0, at, :].astype(f32)
        for k in range(1, parts.shape[0]):
            total = total + parts[k, at, :].astype(f32)
        return total

    for q in range(8):
        src_pot[q : q + 1, :] = sp[:, q * 128 : (q + 1) * 128] * LN2
    tgt_pot[...] = tpot[:, 0:B]
    mass = added(slice(256, 272))
    mass = mass[:8] + mass[8:]
    for q in range(8):
        image = added(slice(q * 32, (q + 1) * 32)) / mass[q : q + 1, :]
        out[:, q * 128 : (q + 1) * 128] = image.astype(jnp.bfloat16)


def finish_call(parts, sp, tpot):
    return pl.pallas_call(
        finish_kernel,
        name="finish",
        in_specs=[WHOLE] * 3,
        out_specs=[WHOLE] * 3,
        out_shape=[
            jax.ShapeDtypeStruct((32, 1024), jnp.bfloat16),
            jax.ShapeDtypeStruct((8, 128), jnp.float32),
            jax.ShapeDtypeStruct((1, B), jnp.float32),
        ],
        compiler_params=params(8),
    )(parts, sp, tpot)


def body(sources, log_src, targets, potential, log_tgt):
    f = sources.shape[1]
    scale2 = LOG2E / math.sqrt(f)

    own = own_call(targets, potential, log_tgt)
    ra = from_z(own, 4)
    la = from_z(own, -5)
    near = lax.ppermute(near_call(sources, log_src), ("yh", "yl"), [(0, 3), (3, 0), (1, 2), (2, 1)])
    rb = from_z(joined([(0, 0), (1, 0)], [own, ra]), 2)
    lb = from_z(joined([(1, 0), (0, 0)], [own, la]), -2)
    rc = from_z(joined([(0, 0), (1, 0), (1, 1), (2, 0), (3, 0)], [own, rb, ra, la]), 1)
    lc = from_z(joined([(0, 0), (1, 0), (1, 1), (2, 0)], [own, lb, la]), -1)
    s, rows, logs, tgt, lt = all_scores(sources, log_src, near, [own, ra, la, rb, lb, rc, lc], scale2)
    row_parts = lax.all_to_all(rows, PLANE, split_axis=0, concat_axis=0, tiled=True)
    sp, cols = cols_call(row_parts, logs, s)
    col_parts = lax.all_to_all(cols, "z", split_axis=0, concat_axis=0, tiled=True)
    tpot, theirs, mass, wide = moved_call(col_parts, lt, sp, s, tgt)
    theirs = lax.ppermute(theirs, "c", [(0, 1), (1, 0)])
    packed = pack_call(mine_call(tgt, wide), theirs, mass)
    parts = lax.all_to_all(packed, CHIPS, split_axis=0, concat_axis=0, tiled=True)
    mapped, src_pot, tgt_pot = finish_call(parts, sp, tpot)
    return (src_pot.reshape(-1), tgt_pot.reshape(-1), mapped.T)


def solution(mesh):
    torus = Mesh(mesh.devices.reshape(16, 2, 2, 4, 2), AXES)
    src, every = ("z", "yh"), ("z", "yh", "yl", "x", "c")
    return jax.shard_map(
        body,
        mesh=torus,
        in_specs=(P(src, None), P(src), P(every, None), P(every), P(every)),
        out_specs=(P(src), P(every), P(src, ("yl", "x", "c"))),
        check_vma=False,
    )
```

```python
import math

import jax
import jax.numpy as jnp
from jax import lax
from jax.experimental import pallas as pl
from jax.experimental.pallas import tpu as pltpu
from jax.sharding import Mesh
from jax.sharding import PartitionSpec as P


WHOLE = pl.BlockSpec(memory_space=pltpu.VMEM)
FAR = pl.BlockSpec(memory_space=pltpu.HBM)
AXES = ("z", "yh", "yl", "x", "c")
PLANE = ("c", "x", "yh", "yl")
CHIPS = ("x", "yh", "yl")
LOG2E = math.log2(math.e)
LN2 = math.log(2.0)
B = 64
A8 = 8
OFF1 = (0, 4, 11, 2, 6, 9, 14, 1, 5, 12, 15, 10)
OFF2 = (3, 7, 8, 13)
OFF = OFF1 + OFF2
PICKS = tuple((m, k) for m, count in enumerate((1, 1, 1, 2, 2, 3, 2, 2, 2)) for k in range(count))
PICKS1 = PICKS[: len(OFF1)]
PICKS2 = PICKS[len(OFF1) :]


MIB = 1 << 20


def params(mib):
    return pltpu.CompilerParams(vmem_limit_bytes=mib * MIB)


def from_z(array, d):
    n = lax.axis_size("z")
    return lax.ppermute(array, "z", [((i + d) % n, i) for i in range(n)])


def split(v):
    hi = v.astype(jnp.bfloat16).astype(jnp.float32)
    lo = (v - hi).astype(jnp.bfloat16).astype(jnp.float32)
    return [hi, lo, v - hi - lo]


def far(array):
    return pltpu.with_memory_space_constraint(array, pltpu.HBM)


def own_kernel(targets, potential, log_tgt, out, pot, log, sems):
    f32, bf = jnp.float32, jnp.bfloat16
    copies = [
        pltpu.make_async_copy(targets, out.at[0:B], sems.at[0]),
        pltpu.make_async_copy(potential, pot, sems.at[1]),
        pltpu.make_async_copy(log_tgt, log, sems.at[2]),
    ]
    for copy in copies:
        copy.start()
    for copy in copies:
        copy.wait()
    rows = []
    for ref in (pot, log):
        rows += split(ref[...])
    extra = jnp.concatenate(rows + [jnp.zeros((2, B), f32)], axis=0).astype(bf)
    out[B : B + A8, :] = jnp.concatenate([extra, jnp.zeros((A8, out.shape[1] - B), bf)], axis=1)


def own_call(targets, potential, log_tgt):
    return pl.pallas_call(
        own_kernel,
        name="own",
        in_specs=[FAR] * 3,
        out_specs=WHOLE,
        out_shape=jax.ShapeDtypeStruct((B + A8, targets.shape[1]), targets.dtype),
        scratch_shapes=[pltpu.VMEM((1, B), jnp.float32)] * 2 + [pltpu.SemaphoreType.DMA((3,))],
        compiler_params=params(4),
    )(*[far(a) for a in (targets, potential.reshape(1, B), log_tgt.reshape(1, B))])


def joined(picks, msgs):
    def kernel(*refs):
        out = refs[-1]
        extra = []
        for p, (m, k) in enumerate(picks):
            out[p * B : (p + 1) * B, :] = refs[m][k * B : (k + 1) * B, :]
            extra.append(refs[m][refs[m].shape[0] - A8 :, k * B : (k + 1) * B])
        rest = out.shape[1] - len(picks) * B
        extra.append(jnp.zeros((A8, rest), out.dtype))
        out[len(picks) * B :, :] = jnp.concatenate(extra, axis=1)

    return pl.pallas_call(
        kernel,
        in_specs=[WHOLE] * len(msgs),
        out_specs=WHOLE,
        out_shape=jax.ShapeDtypeStruct((len(picks) * B + A8, msgs[0].shape[1]), msgs[0].dtype),
        compiler_params=params(4),
    )(*msgs)


def eye(n):
    return lax.broadcasted_iota(jnp.int32, (n, n), 0) == lax.broadcasted_iota(jnp.int32, (n, n), 1)


def to_col(row):
    n = row.shape[1]
    return jnp.sum(jnp.where(eye(n), jnp.broadcast_to(row, (n, n)), 0.0), axis=1, keepdims=True)


def to_row(col):
    n = col.shape[0]
    return jnp.sum(jnp.where(eye(n), jnp.broadcast_to(col, (n, n)), 0.0), axis=0, keepdims=True)


CH = 512


def block_of(msgs, m, k):
    extra = msgs[m][msgs[m].shape[0] - A8 :, k * B : (k + 1) * B]
    return msgs[m].at[k * B : (k + 1) * B], extra.astype(jnp.float32)


def row_lse(s_out, at, pot):
    t = pot.shape[0]

    def shifted(r):
        return s_out[r : r + 32, at] + jnp.concatenate([pot[r : r + 32, :]] * (CH // 128), axis=1)

    top = jnp.full((8, CH), -jnp.inf, jnp.float32)
    for r in range(0, t, 32):
        top = jnp.maximum(top, jnp.max(shifted(r).reshape(4, 8, CH), axis=0))
    top = jnp.max(top, axis=0, keepdims=True)
    tot = jnp.zeros((8, CH), jnp.float32)
    for r in range(0, t, 32):
        tot = tot + jnp.sum(jnp.exp2(shifted(r) - top).reshape(4, 8, CH), axis=0)
    return top + jnp.log2(jnp.sum(tot, axis=0, keepdims=True))


def scores(tg, src, scale2):
    return lax.dot_general(tg, src, (((1,), (1,)), ((), ())), preferred_element_type=jnp.float32) * scale2


def laid_out(msgs, picks, tg, pot):
    for p, (m, k) in enumerate(picks):
        rows, ex = block_of(msgs, m, k)
        tg[p * B : (p + 1) * B, :] = rows[...]
        po = (ex[0:1] + ex[1:2] + ex[2:3]) * LOG2E
        pot[p * B : (p + 1) * B, :] = jnp.broadcast_to(to_col(po), (B, 128))


def turned(tg, out, base):
    core = lax.axis_index("c")
    for q in range(tg.shape[0] // 128):
        flipped = tg[q * 128 : (q + 1) * 128, :].T
        for f in range(16):
            to = pl.multiple_of((((f % 2) ^ core) * 8 + f // 2) * 32, 32)
            out[pl.ds(to, 32), base + q * 128 : base + (q + 1) * 128] = flipped[f * 32 : (f + 1) * 32, :]


def first_kernel(scale2, sources, near, *refs):
    msgs, (s_out, lse_out, tgt_out, tg, pot) = refs[:-5], refs[-5:]
    laid_out(msgs, PICKS1, tg, pot)
    ns = sources.shape[0]
    for n in range(2 * ns // CH):
        at = slice(n * CH, (n + 1) * CH)
        ref, row = (sources, n * CH) if n * CH < ns else (near, n * CH - ns)
        s_out[:, at] = scores(tg[...], ref[row : row + CH, :], scale2)
        lse_out[:, at] = row_lse(s_out, at, pot)
    turned(tg, tgt_out, 0)


def last_kernel(scale2, sources, near, lse_in, tgt_in, *refs):
    msgs, (s_out, rows_out, tgt_out, lt_out, tg, pot) = refs[:-6], refs[-6:]
    laid_out(msgs, PICKS2, tg, pot)
    yh = lax.axis_index("yh")
    ns = sources.shape[0]
    for n in range(2 * ns // CH):
        at = slice(n * CH, (n + 1) * CH)
        ref, row, block = (sources, n * CH, yh) if n * CH < ns else (near, n * CH - ns, 1 - yh)
        s_out[:, at] = scores(tg[...], ref[row : row + CH, :], scale2)
        lse = added_lse(lse_in[:, at], row_lse(s_out, at, pot))
        for i in range(CH // 128):
            piece = jnp.broadcast_to(lse[:, i * 128 : (i + 1) * 128][None], (rows_out.shape[0], 1, 128))
            q = row // 128 + i
            rows_out[:, block, q : q + 1, :] = piece
    for p, (m, k) in enumerate(PICKS):
        _, ex = block_of(msgs, m, k)
        lt_out[p : p + 1, 0:B] = (ex[3:4] + ex[4:5] + ex[5:6]) * LOG2E
    t1 = tgt_in.shape[1]
    tgt_out[:, :t1] = tgt_in[...]
    turned(tg, tgt_out, t1)


def added_lse(a, b):
    top = jnp.maximum(a, b)
    return top + jnp.log2(jnp.exp2(a - top) + jnp.exp2(b - top))


def scores_call(kernel, scale2, args, shapes, scratch, flops):
    return pl.pallas_call(
        lambda *a: kernel(scale2, *a),
        in_specs=[WHOLE] * len(args),
        out_specs=[WHOLE] * len(shapes),
        scratch_shapes=[pltpu.VMEM(s, d) for s, d in scratch],
        out_shape=[jax.ShapeDtypeStruct(s, d) for s, d in shapes],
        compiler_params=params(20),
        cost_estimate=pl.CostEstimate(flops=flops, bytes_accessed=1 << 22, transcendentals=1 << 20),
    )(*args)


def all_scores(sources, near, msgs, scale2):
    ns, f = sources.shape
    f32, bf = jnp.float32, jnp.bfloat16
    t1, t2 = len(PICKS1) * B, len(PICKS2) * B
    s1, lse1, tgt1 = scores_call(
        first_kernel, scale2, [sources, near, *msgs[:7]],
        [((t1, 2 * ns), f32), ((1, 2 * ns), f32), ((f, t1), bf)],
        [((t1, f), bf), ((t1, 128), f32)], 4 * t1 * ns * f,
    )
    s2, rows, tgt, lt = scores_call(
        last_kernel, scale2, [sources, near, lse1, tgt1, *msgs],
        [((t2, 2 * ns), f32), ((32, 2, ns // 128, 128), f32), ((f, t1 + t2), bf), ((len(OFF), 128), f32)],
        [((t2, f), bf), ((t2, 128), f32)], 4 * t2 * ns * f,
    )
    return (s1, s2), rows, tgt, lt


def merged_lse(parts):
    top = jnp.max(parts, axis=0)
    return top + jnp.log2(jnp.sum(jnp.exp2(parts - top[None]), axis=0))


def slot_of(p):
    return (lax.axis_index("z") + OFF[p]) % 16


def cols_kernel(parts, log_own, log_near, s1, s2, sp_out, msg_out, held, lse):
    yh = lax.axis_index("yh")
    for h in range(2):
        lse[h] = merged_lse(parts[:, h])
    for h, block in enumerate((yh, 1 - yh)):
        sp = (log_near if h else log_own)[...] * LOG2E - lse[block]
        for r in range(8):
            sp_out[:, (h * 8 + r) * 128 : (h * 8 + r + 1) * 128] = sp[r : r + 1, :]
    held[...] = jnp.zeros_like(held)
    n1 = len(OFF1)
    for p in range(len(OFF)):
        s_ref, base = (s1, p * B) if p < n1 else (s2, (p - n1) * B)
        pieces = []
        for r in range(0, B, 8):
            lifted = s_ref[base + r : base + r + 8, :] + sp_out[...]
            top = jnp.max(lifted, axis=1, keepdims=True)
            pieces.append(top + jnp.log2(jnp.sum(jnp.exp2(lifted - top), axis=1, keepdims=True)))
        row = to_row(jnp.concatenate(pieces, axis=0))
        row = jnp.concatenate([row, row], axis=1)
        slot = slot_of(p)
        at = slot // 2
        half = lax.broadcasted_iota(jnp.int32, (1, 128), 1) // B
        held[pl.ds(at, 1), :] = jnp.where(half == slot % 2, row, held[pl.ds(at, 1), :])
    msg_out[...] = jnp.broadcast_to(held[...][None], msg_out.shape)


def cols_call(parts, log_own, log_near, s):
    ns = s[0].shape[1]
    return pl.pallas_call(
        cols_kernel,
        name="cols",
        in_specs=[WHOLE] * 5,
        out_specs=[WHOLE] * 2,
        scratch_shapes=[pltpu.VMEM((8, 128), jnp.float32), pltpu.VMEM((2, 8, 128), jnp.float32)],
        out_shape=[jax.ShapeDtypeStruct((1, ns), jnp.float32), jax.ShapeDtypeStruct((16, 8, 128), jnp.float32)],
        compiler_params=params(16),
    )(parts, log_own, log_near, *s)


def moved_kernel(parts, lt, sp, s1, s2, tgt, pot_out, theirs_out, mass_out, wide, tp, lse):
    lse[...] = merged_lse(parts[...])
    for p in range(len(OFF)):
        slot = slot_of(p)
        row = lse[pl.ds(slot // 2, 1), :]
        row = jnp.where(slot % 2 == 0, row[:, :B], row[:, B:])
        tpot = lt[p : p + 1, 0:B] - row
        if p == 0:
            pot_out[:, 0:B] = tpot * LN2
        tp[p * B : (p + 1) * B, :] = jnp.broadcast_to(to_col(tpot), (B, 128))

    t1 = s1.shape[0]
    half = tgt.shape[0] // 2
    for n in range(sp.shape[1] // CH):
        at = slice(n * CH, (n + 1) * CH)
        spn = sp[:, at]
        mass = jnp.zeros((8, CH), jnp.float32)
        for r in range(0, tp.shape[0], 32):
            s = s1[r : r + 32, at] if r < t1 else s2[r - t1 : r - t1 + 32, at]
            e = jnp.exp2(s + spn + jnp.concatenate([tp[r : r + 32, :]] * (CH // 128), axis=1))
            mass = mass + jnp.sum(e.reshape(4, 8, CH), axis=0)
            wide[r : r + 32, at] = e.astype(jnp.bfloat16)
        mass = jnp.sum(mass, axis=0, keepdims=True)
        mass_out[:, at] = mass
        part = jnp.dot(tgt[half:, :], wide[:, at], preferred_element_type=jnp.float32)
        theirs_out[0:half, at] = part.astype(jnp.bfloat16)
        hi = mass.astype(jnp.bfloat16).astype(jnp.float32)
        pad = jnp.zeros((6, CH), jnp.float32)
        theirs_out[half : half + 8, at] = jnp.concatenate([hi, mass - hi, pad], axis=0).astype(jnp.bfloat16)


def moved_call(parts, lt, sp, s, tgt):
    ns = sp.shape[1]
    f, t = tgt.shape
    return pl.pallas_call(
        moved_kernel,
        name="moved",
        in_specs=[WHOLE] * 6,
        out_specs=[WHOLE] * 4,
        scratch_shapes=[pltpu.VMEM((t, 128), jnp.float32), pltpu.VMEM((8, 128), jnp.float32)],
        out_shape=[
            jax.ShapeDtypeStruct((1, 128), jnp.float32),
            jax.ShapeDtypeStruct((f // 2 + 8, ns), jnp.bfloat16),
            jax.ShapeDtypeStruct((1, ns), jnp.float32),
            jax.ShapeDtypeStruct((t, ns), jnp.bfloat16),
        ],
        compiler_params=params(20),
    )(parts, lt, sp, *s, tgt)


def mine_kernel(tgt, wide, out):
    for n in range(out.shape[1] // CH):
        at = slice(n * CH, (n + 1) * CH)
        part = jnp.dot(tgt[: out.shape[0], :], wide[:, at], preferred_element_type=jnp.float32)
        out[:, at] = part.astype(jnp.bfloat16)


def mine_call(tgt, wide):
    f, t = tgt.shape
    ns = wide.shape[1]
    return pl.pallas_call(
        mine_kernel,
        name="mine",
        in_specs=[WHOLE] * 2,
        out_specs=WHOLE,
        out_shape=jax.ShapeDtypeStruct((f // 2, ns), jnp.bfloat16),
        compiler_params=params(12),
        cost_estimate=pl.CostEstimate(flops=f * t * ns, bytes_accessed=2 * t * ns, transcendentals=0),
    )(tgt, wide)


def pack_kernel(mine, theirs, mass, out):
    f32 = jnp.float32
    extra = theirs[256:264, :].astype(f32)
    total = mass[...] + extra[0:1] + extra[1:2]
    hi = total.astype(jnp.bfloat16).astype(f32)
    lo = total - hi
    yh = lax.axis_index("yh")
    for h in range(2):
        to = (h ^ yh) * 2
        rows = [v[:, (h * 8 + q) * 128 : (h * 8 + q + 1) * 128] for v in (hi, lo) for q in range(8)]
        rows = jnp.concatenate(rows, axis=0).astype(jnp.bfloat16)
        for g in range(8):
            at_chip = g % 4 * 4 + g // 4
            for q in range(8):
                at = (slice(g * 32, (g + 1) * 32), slice((h * 8 + q) * 128, (h * 8 + q + 1) * 128))
                both = mine[at].astype(f32) + theirs[at].astype(f32)
                out[to + at_chip, q * 32 : (q + 1) * 32, :] = both.astype(jnp.bfloat16)
            out[to + at_chip, 256:272, :] = rows


def pack_call(mine, theirs, mass):
    return pl.pallas_call(
        pack_kernel,
        name="pack",
        in_specs=[WHOLE] * 3,
        out_specs=WHOLE,
        out_shape=jax.ShapeDtypeStruct((16, 272, 128), jnp.bfloat16),
        compiler_params=params(8),
    )(mine, theirs, mass)


def finish_kernel(parts, sp, tpot, out, src_pot, tgt_pot):
    f32 = jnp.float32

    def added(at):
        total = parts[0, at, :].astype(f32)
        for k in range(1, parts.shape[0]):
            total = total + parts[k, at, :].astype(f32)
        return total

    for q in range(8):
        src_pot[q : q + 1, :] = sp[:, q * 128 : (q + 1) * 128] * LN2
    tgt_pot[...] = tpot[:, 0:B]
    mass = added(slice(256, 272))
    mass = mass[:8] + mass[8:]
    for q in range(8):
        image = added(slice(q * 32, (q + 1) * 32)) / mass[q : q + 1, :]
        out[:, q * 128 : (q + 1) * 128] = image.astype(jnp.bfloat16)


def finish_call(parts, sp, tpot):
    return pl.pallas_call(
        finish_kernel,
        name="finish",
        in_specs=[WHOLE] * 3,
        out_specs=[WHOLE] * 3,
        out_shape=[
            jax.ShapeDtypeStruct((32, 1024), jnp.bfloat16),
            jax.ShapeDtypeStruct((8, 128), jnp.float32),
            jax.ShapeDtypeStruct((1, B), jnp.float32),
        ],
        compiler_params=params(8),
    )(parts, sp, tpot)


def body(sources, log_src, targets, potential, log_tgt):
    f = sources.shape[1]
    scale2 = LOG2E / math.sqrt(f)

    other = [(0, 3), (3, 0), (1, 2), (2, 1)]
    near = lax.ppermute(sources, ("yh", "yl"), other)
    own = own_call(targets, potential, log_tgt)
    ra = from_z(own, 4)
    la = from_z(own, -5)
    rb = from_z(joined([(0, 0), (1, 0)], [own, ra]), 2)
    lb = from_z(joined([(1, 0), (0, 0)], [own, la]), -2)
    rc1 = from_z(joined([(0, 0), (1, 0), (2, 0)], [own, ra, la]), 1)
    lc1 = from_z(joined([(0, 0), (1, 0)], [own, la]), -1)
    rc2 = from_z(rb, 1)
    lc2 = from_z(lb, -1)
    log_own = log_src.reshape(8, 128)
    log_near = lax.ppermute(log_own, ("yh", "yl"), other)
    s, rows, tgt, lt = all_scores(sources, near, [own, ra, la, rb, lb, rc1, lc1, rc2, lc2], scale2)
    rows, log_near = lax.optimization_barrier((rows, log_near))
    row_parts = lax.all_to_all(rows, PLANE, split_axis=0, concat_axis=0, tiled=True)
    sp, cols = cols_call(row_parts, log_own, log_near, s)
    col_parts = lax.all_to_all(cols, "z", split_axis=0, concat_axis=0, tiled=True)
    tpot, theirs, mass, wide = moved_call(col_parts, lt, sp, s, tgt)
    theirs = lax.ppermute(theirs, "c", [(0, 1), (1, 0)])
    packed = pack_call(mine_call(tgt, wide), theirs, mass)
    parts = lax.all_to_all(packed, CHIPS, split_axis=0, concat_axis=0, tiled=True)
    mapped, src_pot, tgt_pot = finish_call(parts, sp, tpot)
    return (src_pot.reshape(-1), tgt_pot.reshape(-1), mapped.T)


def solution(mesh):
    torus = Mesh(mesh.devices.reshape(16, 2, 2, 4, 2), AXES)
    src, every = ("z", "yh"), ("z", "yh", "yl", "x", "c")
    return jax.shard_map(
        body,
        mesh=torus,
        in_specs=(P(src, None), P(src), P(every, None), P(every), P(every)),
        out_specs=(P(src), P(every), P(src, ("yl", "x", "c"))),
        check_vma=False,
    )
```

```python
import math

import jax
import jax.numpy as jnp
from jax import lax
from jax.experimental import pallas as pl
from jax.experimental.pallas import tpu as pltpu
from jax.sharding import Mesh
from jax.sharding import PartitionSpec as P


WHOLE = pl.BlockSpec(memory_space=pltpu.VMEM)
FAR = pl.BlockSpec(memory_space=pltpu.HBM)
AXES = ("z", "yh", "yl", "x", "c")
PLANE = ("c", "x", "yh", "yl")
CHIPS = ("x", "yh", "yl")
LOG2E = math.log2(math.e)
LN2 = math.log(2.0)
B = 64
A8 = 8
OFF1 = (0, 4, 11, 2, 6, 9, 14, 1, 3, 7, 5, 12)
OFF2 = (15, 8, 13, 10)
OFF = OFF1 + OFF2
PICKS = tuple((m, k) for m, count in enumerate((1, 1, 1, 2, 2, 5, 4)) for k in range(count))
PICKS1 = PICKS[: len(OFF1)]
PICKS2 = PICKS[len(OFF1) :]


MIB = 1 << 20


def params(mib):
    return pltpu.CompilerParams(vmem_limit_bytes=mib * MIB)


def from_z(array, d):
    n = lax.axis_size("z")
    return lax.ppermute(array, "z", [((i + d) % n, i) for i in range(n)])


def split(v):
    hi = v.astype(jnp.bfloat16).astype(jnp.float32)
    lo = (v - hi).astype(jnp.bfloat16).astype(jnp.float32)
    return [hi, lo, v - hi - lo]


def far(array):
    return pltpu.with_memory_space_constraint(array, pltpu.HBM)


def own_kernel(targets, potential, log_tgt, out, pot, log, sems):
    f32, bf = jnp.float32, jnp.bfloat16
    copies = [
        pltpu.make_async_copy(targets, out.at[0:B], sems.at[0]),
        pltpu.make_async_copy(potential, pot, sems.at[1]),
        pltpu.make_async_copy(log_tgt, log, sems.at[2]),
    ]
    for copy in copies:
        copy.start()
    for copy in copies:
        copy.wait()
    rows = []
    for ref in (pot, log):
        rows += split(ref[...])
    extra = jnp.concatenate(rows + [jnp.zeros((2, B), f32)], axis=0).astype(bf)
    out[B : B + A8, :] = jnp.concatenate([extra, jnp.zeros((A8, out.shape[1] - B), bf)], axis=1)


def own_call(targets, potential, log_tgt):
    return pl.pallas_call(
        own_kernel,
        name="own",
        in_specs=[FAR] * 3,
        out_specs=WHOLE,
        out_shape=jax.ShapeDtypeStruct((B + A8, targets.shape[1]), targets.dtype),
        scratch_shapes=[pltpu.VMEM((1, B), jnp.float32)] * 2 + [pltpu.SemaphoreType.DMA((3,))],
        compiler_params=params(4),
    )(*[far(a) for a in (targets, potential.reshape(1, B), log_tgt.reshape(1, B))])


def near_kernel(sources, log_src, out, log, sems):
    copies = [
        pltpu.make_async_copy(sources, out.at[0 : sources.shape[0]], sems.at[0]),
        pltpu.make_async_copy(log_src, log, sems.at[1]),
    ]
    for copy in copies:
        copy.start()
    for copy in copies:
        copy.wait()
    f = out.shape[1]
    rows = [part[:, h * f : (h + 1) * f] for part in split(log[...]) for h in range(2)]
    out[sources.shape[0] :, :] = jnp.concatenate(rows + [jnp.zeros((2, f), jnp.float32)], axis=0).astype(out.dtype)


def near_call(sources, log_src):
    n, f = sources.shape
    return pl.pallas_call(
        near_kernel,
        name="near_message",
        in_specs=[FAR] * 2,
        out_specs=WHOLE,
        out_shape=jax.ShapeDtypeStruct((n + A8, f), sources.dtype),
        scratch_shapes=[pltpu.VMEM((1, n), jnp.float32), pltpu.SemaphoreType.DMA((2,))],
        compiler_params=params(4),
    )(far(sources), far(log_src.reshape(1, n)))


def joined(picks, msgs):
    def kernel(*refs):
        out = refs[-1]
        extra = []
        for p, (m, k) in enumerate(picks):
            out[p * B : (p + 1) * B, :] = refs[m][k * B : (k + 1) * B, :]
            extra.append(refs[m][refs[m].shape[0] - A8 :, k * B : (k + 1) * B])
        rest = out.shape[1] - len(picks) * B
        extra.append(jnp.zeros((A8, rest), out.dtype))
        out[len(picks) * B :, :] = jnp.concatenate(extra, axis=1)

    return pl.pallas_call(
        kernel,
        in_specs=[WHOLE] * len(msgs),
        out_specs=WHOLE,
        out_shape=jax.ShapeDtypeStruct((len(picks) * B + A8, msgs[0].shape[1]), msgs[0].dtype),
        compiler_params=params(4),
    )(*msgs)


def eye(n):
    return lax.broadcasted_iota(jnp.int32, (n, n), 0) == lax.broadcasted_iota(jnp.int32, (n, n), 1)


def to_col(row):
    n = row.shape[1]
    return jnp.sum(jnp.where(eye(n), jnp.broadcast_to(row, (n, n)), 0.0), axis=1, keepdims=True)


def to_row(col):
    n = col.shape[0]
    return jnp.sum(jnp.where(eye(n), jnp.broadcast_to(col, (n, n)), 0.0), axis=0, keepdims=True)


CH = 512


def block_of(msgs, m, k):
    extra = msgs[m][msgs[m].shape[0] - A8 :, k * B : (k + 1) * B]
    return msgs[m].at[k * B : (k + 1) * B], extra.astype(jnp.float32)


def row_lse(s_out, at, pot):
    t = pot.shape[0]

    def shifted(r):
        return s_out[r : r + 32, at] + jnp.concatenate([pot[r : r + 32, :]] * (CH // 128), axis=1)

    top = jnp.full((8, CH), -jnp.inf, jnp.float32)
    for r in range(0, t, 32):
        top = jnp.maximum(top, jnp.max(shifted(r).reshape(4, 8, CH), axis=0))
    top = jnp.max(top, axis=0, keepdims=True)
    tot = jnp.zeros((8, CH), jnp.float32)
    for r in range(0, t, 32):
        tot = tot + jnp.sum(jnp.exp2(shifted(r) - top).reshape(4, 8, CH), axis=0)
    return top + jnp.log2(jnp.sum(tot, axis=0, keepdims=True))


def scores(tg, src, scale2):
    return lax.dot_general(tg, src, (((1,), (1,)), ((), ())), preferred_element_type=jnp.float32) * scale2


def laid_out(msgs, picks, tg, pot):
    for p, (m, k) in enumerate(picks):
        rows, ex = block_of(msgs, m, k)
        tg[p * B : (p + 1) * B, :] = rows[...]
        po = (ex[0:1] + ex[1:2] + ex[2:3]) * LOG2E
        pot[p * B : (p + 1) * B, :] = jnp.broadcast_to(to_col(po), (B, 128))


def turned(tg, out, base):
    core = lax.axis_index("c")
    for q in range(tg.shape[0] // 128):
        flipped = tg[q * 128 : (q + 1) * 128, :].T
        for f in range(16):
            to = pl.multiple_of((((f % 2) ^ core) * 8 + f // 2) * 32, 32)
            out[pl.ds(to, 32), base + q * 128 : base + (q + 1) * 128] = flipped[f * 32 : (f + 1) * 32, :]


def own_kernel_first(scale2, sources, *refs):
    msgs, (s_out, lse_out, tgt_out, tg, pot) = refs[:-5], refs[-5:]
    laid_out(msgs, PICKS1, tg, pot)
    for n in range(sources.shape[0] // CH):
        at = slice(n * CH, (n + 1) * CH)
        s_out[:, at] = scores(tg[...], sources[at, :], scale2)
        lse_out[:, at] = row_lse(s_out, at, pot)
    turned(tg, tgt_out, 0)


def near_kernel_first(scale2, near, log_src, tg, pot, s_out, lse_out, log_out):
    ns = near.shape[0] - A8
    logs = near[ns:, :].astype(jnp.float32)
    logs = logs[0:2] + logs[2:4] + logs[4:6]
    for q in range(8):
        log_out[0, q : q + 1, :] = log_src[:, q * 128 : (q + 1) * 128] * LOG2E
        log_out[1, q : q + 1, :] = logs[q // 4 : q // 4 + 1, q % 4 * 128 : (q % 4 + 1) * 128] * LOG2E
    for n in range(ns // CH):
        at = slice(n * CH, (n + 1) * CH)
        s_out[:, at] = scores(tg[...], near[at, :], scale2)
        lse_out[:, at] = row_lse(s_out, at, pot)


def last_kernel(scale2, sources, near, lse_own, lse_near, tgt_in, *refs):
    msgs, (s_out, rows_out, tgt_out, lt_out, tg, pot) = refs[:-6], refs[-6:]
    laid_out(msgs, PICKS2, tg, pot)
    yh = lax.axis_index("yh")
    ns = sources.shape[0]
    for n in range(2 * ns // CH):
        at = slice(n * CH, (n + 1) * CH)
        first = n * CH < ns
        ref, lse_in, row, block = (sources, lse_own, n * CH, yh) if first else (near, lse_near, n * CH - ns, 1 - yh)
        s_out[:, at] = scores(tg[...], ref[row : row + CH, :], scale2)
        lse = added_lse(lse_in[:, row : row + CH], row_lse(s_out, at, pot))
        for i in range(CH // 128):
            piece = jnp.broadcast_to(lse[:, i * 128 : (i + 1) * 128][None], (rows_out.shape[0], 1, 128))
            q = row // 128 + i
            rows_out[:, block, q : q + 1, :] = piece
    for p, (m, k) in enumerate(PICKS):
        _, ex = block_of(msgs, m, k)
        lt_out[p : p + 1, 0:B] = (ex[3:4] + ex[4:5] + ex[5:6]) * LOG2E
    t1 = tgt_in.shape[1]
    tgt_out[:, :t1] = tgt_in[...]
    turned(tg, tgt_out, t1)


def added_lse(a, b):
    top = jnp.maximum(a, b)
    return top + jnp.log2(jnp.exp2(a - top) + jnp.exp2(b - top))


def scores_call(kernel, scale2, args, shapes, scratch, flops):
    return pl.pallas_call(
        lambda *a: kernel(scale2, *a),
        in_specs=[WHOLE] * len(args),
        out_specs=[WHOLE] * len(shapes),
        scratch_shapes=[pltpu.VMEM(s, d) for s, d in scratch],
        out_shape=[jax.ShapeDtypeStruct(s, d) for s, d in shapes],
        compiler_params=params(20),
        cost_estimate=pl.CostEstimate(flops=flops, bytes_accessed=1 << 22, transcendentals=1 << 20),
    )(*args)


def all_scores(sources, log_src, near, msgs, scale2):
    ns, f = sources.shape
    f32, bf = jnp.float32, jnp.bfloat16
    t1, t2 = len(PICKS1) * B, len(PICKS2) * B
    s1, lse1, tgt1, tg, pot = scores_call(
        own_kernel_first, scale2, [sources, *msgs[:6]],
        [((t1, ns), f32), ((1, ns), f32), ((f, t1), bf), ((t1, f), bf), ((t1, 128), f32)], [], 2 * t1 * ns * f,
    )
    s2, lse2, logs = scores_call(
        near_kernel_first, scale2, [near, log_src.reshape(1, ns), tg, pot],
        [((t1, ns), f32), ((1, ns), f32), ((2, ns // 128, 128), f32)], [], 2 * t1 * ns * f,
    )
    s3, rows, tgt, lt = scores_call(
        last_kernel, scale2, [sources, near, lse1, lse2, tgt1, *msgs],
        [((t2, 2 * ns), f32), ((32, 2, ns // 128, 128), f32), ((f, t1 + t2), bf), ((len(OFF), 128), f32)],
        [((t2, f), bf), ((t2, 128), f32)], 4 * t2 * ns * f,
    )
    return (s1, s2, s3), rows, logs, tgt, lt


def merged_lse(parts):
    top = jnp.max(parts, axis=0)
    return top + jnp.log2(jnp.sum(jnp.exp2(parts - top[None]), axis=0))


def slot_of(p):
    return (lax.axis_index("z") + OFF[p]) % 16


def cols_kernel(parts, logs, s1, s2, s3, sp_out, msg_out, held, lse):
    yh = lax.axis_index("yh")
    for h in range(2):
        lse[h] = merged_lse(parts[:, h])
    for h, block in enumerate((yh, 1 - yh)):
        sp = logs[h] - lse[block]
        for r in range(8):
            sp_out[:, (h * 8 + r) * 128 : (h * 8 + r + 1) * 128] = sp[r : r + 1, :]
    held[...] = jnp.zeros_like(held)
    n1 = len(OFF1)
    ns = s1.shape[1]
    for p in range(len(OFF)):
        tops, totals = [], []
        for r in range(0, B, 8):
            lifted = []
            for k in range(2 * ns // 128):
                ref, base, col = (s3, (p - n1) * B, k * 128)
                if p < n1:
                    ref, base, col = (s1, p * B, k * 128) if k * 128 < ns else (s2, p * B, k * 128 - ns)
                lifted.append(ref[base + r : base + r + 8, col : col + 128] + sp_out[:, k * 128 : (k + 1) * 128])
            top = lifted[0]
            for v in lifted[1:]:
                top = jnp.maximum(top, v)
            total = jnp.exp2(lifted[0] - top)
            for v in lifted[1:]:
                total = total + jnp.exp2(v - top)
            tops.append(top)
            totals.append(total)
        tops, totals = jnp.concatenate(tops, axis=0), jnp.concatenate(totals, axis=0)
        top = jnp.max(tops, axis=1, keepdims=True)
        row = to_row(top + jnp.log2(jnp.sum(totals * jnp.exp2(tops - top), axis=1, keepdims=True)))
        row = jnp.concatenate([row, row], axis=1)
        slot = slot_of(p)
        at = slot // 2
        half = lax.broadcasted_iota(jnp.int32, (1, 128), 1) // B
        held[pl.ds(at, 1), :] = jnp.where(half == slot % 2, row, held[pl.ds(at, 1), :])
    msg_out[...] = jnp.broadcast_to(held[...][None], msg_out.shape)


def cols_call(parts, logs, s):
    ns = s[2].shape[1]
    return pl.pallas_call(
        cols_kernel,
        name="cols",
        in_specs=[WHOLE] * 5,
        out_specs=[WHOLE] * 2,
        scratch_shapes=[pltpu.VMEM((8, 128), jnp.float32), pltpu.VMEM((2, 8, 128), jnp.float32)],
        out_shape=[jax.ShapeDtypeStruct((1, ns), jnp.float32), jax.ShapeDtypeStruct((16, 8, 128), jnp.float32)],
        compiler_params=params(16),
    )(parts, logs, *s)


def moved_kernel(parts, lt, sp, s1, s2, s3, tgt, pot_out, theirs_out, mass_out, wide, tp, lse):
    lse[...] = merged_lse(parts[...])
    for p in range(len(OFF)):
        slot = slot_of(p)
        row = lse[pl.ds(slot // 2, 1), :]
        row = jnp.where(slot % 2 == 0, row[:, :B], row[:, B:])
        tpot = lt[p : p + 1, 0:B] - row
        if p == 0:
            pot_out[:, 0:B] = tpot * LN2
        tp[p * B : (p + 1) * B, :] = jnp.broadcast_to(to_col(tpot), (B, 128))

    t1, ns = s1.shape
    half = tgt.shape[0] // 2
    for n in range(sp.shape[1] // CH):
        at = slice(n * CH, (n + 1) * CH)
        spn = sp[:, at]
        mass = jnp.zeros((8, CH), jnp.float32)
        for r in range(0, tp.shape[0], 32):
            if r >= t1:
                s = s3[r - t1 : r - t1 + 32, at]
            elif n * CH < ns:
                s = s1[r : r + 32, at]
            else:
                s = s2[r : r + 32, n * CH - ns : (n + 1) * CH - ns]
            e = jnp.exp2(s + spn + jnp.concatenate([tp[r : r + 32, :]] * (CH // 128), axis=1))
            mass = mass + jnp.sum(e.reshape(4, 8, CH), axis=0)
            wide[r : r + 32, at] = e.astype(jnp.bfloat16)
        mass = jnp.sum(mass, axis=0, keepdims=True)
        mass_out[:, at] = mass
        part = jnp.dot(tgt[half:, :], wide[:, at], preferred_element_type=jnp.float32)
        theirs_out[0:half, at] = part.astype(jnp.bfloat16)
        hi = mass.astype(jnp.bfloat16).astype(jnp.float32)
        pad = jnp.zeros((6, CH), jnp.float32)
        theirs_out[half : half + 8, at] = jnp.concatenate([hi, mass - hi, pad], axis=0).astype(jnp.bfloat16)


def moved_call(parts, lt, sp, s, tgt):
    ns = sp.shape[1]
    f, t = tgt.shape
    return pl.pallas_call(
        moved_kernel,
        name="moved",
        in_specs=[WHOLE] * 7,
        out_specs=[WHOLE] * 4,
        scratch_shapes=[pltpu.VMEM((t, 128), jnp.float32), pltpu.VMEM((8, 128), jnp.float32)],
        out_shape=[
            jax.ShapeDtypeStruct((1, 128), jnp.float32),
            jax.ShapeDtypeStruct((f // 2 + 8, ns), jnp.bfloat16),
            jax.ShapeDtypeStruct((1, ns), jnp.float32),
            jax.ShapeDtypeStruct((t, ns), jnp.bfloat16),
        ],
        compiler_params=params(20),
    )(parts, lt, sp, *s, tgt)


def mine_kernel(tgt, wide, out):
    for n in range(out.shape[1] // CH):
        at = slice(n * CH, (n + 1) * CH)
        part = jnp.dot(tgt[: out.shape[0], :], wide[:, at], preferred_element_type=jnp.float32)
        out[:, at] = part.astype(jnp.bfloat16)


def mine_call(tgt, wide):
    f, t = tgt.shape
    ns = wide.shape[1]
    return pl.pallas_call(
        mine_kernel,
        name="mine",
        in_specs=[WHOLE] * 2,
        out_specs=WHOLE,
        out_shape=jax.ShapeDtypeStruct((f // 2, ns), jnp.bfloat16),
        compiler_params=params(12),
        cost_estimate=pl.CostEstimate(flops=f * t * ns, bytes_accessed=2 * t * ns, transcendentals=0),
    )(tgt, wide)


def pack_kernel(mine, theirs, mass, out):
    f32 = jnp.float32
    extra = theirs[256:264, :].astype(f32)
    total = mass[...] + extra[0:1] + extra[1:2]
    hi = total.astype(jnp.bfloat16).astype(f32)
    lo = total - hi
    yh = lax.axis_index("yh")
    for h in range(2):
        to = (h ^ yh) * 2
        rows = [v[:, (h * 8 + q) * 128 : (h * 8 + q + 1) * 128] for v in (hi, lo) for q in range(8)]
        rows = jnp.concatenate(rows, axis=0).astype(jnp.bfloat16)
        for g in range(8):
            at_chip = g % 4 * 4 + g // 4
            for q in range(8):
                at = (slice(g * 32, (g + 1) * 32), slice((h * 8 + q) * 128, (h * 8 + q + 1) * 128))
                both = mine[at].astype(f32) + theirs[at].astype(f32)
                out[to + at_chip, q * 32 : (q + 1) * 32, :] = both.astype(jnp.bfloat16)
            out[to + at_chip, 256:272, :] = rows


def pack_call(mine, theirs, mass):
    return pl.pallas_call(
        pack_kernel,
        name="pack",
        in_specs=[WHOLE] * 3,
        out_specs=WHOLE,
        out_shape=jax.ShapeDtypeStruct((16, 272, 128), jnp.bfloat16),
        compiler_params=params(8),
    )(mine, theirs, mass)


def finish_kernel(parts, sp, tpot, out, src_pot, tgt_pot):
    f32 = jnp.float32

    def added(at):
        total = parts[0, at, :].astype(f32)
        for k in range(1, parts.shape[0]):
            total = total + parts[k, at, :].astype(f32)
        return total

    for q in range(8):
        src_pot[q : q + 1, :] = sp[:, q * 128 : (q + 1) * 128] * LN2
    tgt_pot[...] = tpot[:, 0:B]
    mass = added(slice(256, 272))
    mass = mass[:8] + mass[8:]
    for q in range(8):
        image = added(slice(q * 32, (q + 1) * 32)) / mass[q : q + 1, :]
        out[:, q * 128 : (q + 1) * 128] = image.astype(jnp.bfloat16)


def finish_call(parts, sp, tpot):
    return pl.pallas_call(
        finish_kernel,
        name="finish",
        in_specs=[WHOLE] * 3,
        out_specs=[WHOLE] * 3,
        out_shape=[
            jax.ShapeDtypeStruct((32, 1024), jnp.bfloat16),
            jax.ShapeDtypeStruct((8, 128), jnp.float32),
            jax.ShapeDtypeStruct((1, B), jnp.float32),
        ],
        compiler_params=params(8),
    )(parts, sp, tpot)


def body(sources, log_src, targets, potential, log_tgt):
    f = sources.shape[1]
    scale2 = LOG2E / math.sqrt(f)

    own = own_call(targets, potential, log_tgt)
    ra = from_z(own, 4)
    la = from_z(own, -5)
    near = lax.ppermute(near_call(sources, log_src), ("yh", "yl"), [(0, 3), (3, 0), (1, 2), (2, 1)])
    rb = from_z(joined([(0, 0), (1, 0)], [own, ra]), 2)
    lb = from_z(joined([(1, 0), (0, 0)], [own, la]), -2)
    rc = from_z(joined([(0, 0), (1, 0), (1, 1), (2, 0), (3, 0)], [own, rb, ra, la]), 1)
    lc = from_z(joined([(0, 0), (1, 0), (1, 1), (2, 0)], [own, lb, la]), -1)
    s, rows, logs, tgt, lt = all_scores(sources, log_src, near, [own, ra, la, rb, lb, rc, lc], scale2)
    row_parts = lax.all_to_all(rows, PLANE, split_axis=0, concat_axis=0, tiled=True)
    sp, cols = cols_call(row_parts, logs, s)
    col_parts = lax.all_to_all(cols, "z", split_axis=0, concat_axis=0, tiled=True)
    tpot, theirs, mass, wide = moved_call(col_parts, lt, sp, s, tgt)
    theirs = lax.ppermute(theirs, "c", [(0, 1), (1, 0)])
    packed = pack_call(mine_call(tgt, wide), theirs, mass)
    parts = lax.all_to_all(packed, CHIPS, split_axis=0, concat_axis=0, tiled=True)
    mapped, src_pot, tgt_pot = finish_call(parts, sp, tpot)
    return (src_pot.reshape(-1), tgt_pot.reshape(-1), mapped.T)


def solution(mesh):
    torus = Mesh(mesh.devices.reshape(16, 2, 2, 4, 2), AXES)
    src, every = ("z", "yh"), ("z", "yh", "yl", "x", "c")
    return jax.shard_map(
        body,
        mesh=torus,
        in_specs=(P(src, None), P(src), P(every, None), P(every), P(every)),
        out_specs=(P(src), P(every), P(src, ("yl", "x", "c"))),
        check_vma=False,
    )
```

```python
import math

import jax
import jax.numpy as jnp
from jax import lax
from jax.experimental import pallas as pl
from jax.experimental.pallas import tpu as pltpu
from jax.sharding import Mesh
from jax.sharding import PartitionSpec as P


WHOLE = pl.BlockSpec(memory_space=pltpu.VMEM)
FAR = pl.BlockSpec(memory_space=pltpu.HBM)
AXES = ("z", "yh", "yl", "x", "c")
PLANE = ("c", "x", "yh", "yl")
CHIPS = ("x", "yh", "yl")
LOG2E = math.log2(math.e)
LN2 = math.log(2.0)
B = 64
A8 = 8
OFF1 = (0, 4, 11, 2, 6, 9, 14, 1, 3, 7, 5, 12)
OFF2 = (15, 8, 13, 10)
OFF = OFF1 + OFF2
PICKS = tuple((m, k) for m, count in enumerate((1, 1, 1, 2, 2, 5, 4)) for k in range(count))
PICKS1 = PICKS[: len(OFF1)]
PICKS2 = PICKS[len(OFF1) :]


MIB = 1 << 20


def params(mib):
    return pltpu.CompilerParams(vmem_limit_bytes=mib * MIB)


def sent(array, axes, pairs):
    return lax.ppermute(array, axes, pairs)


def from_z(array, d):
    n = lax.axis_size("z")
    return sent(array, ("z", "c"), [((i + (d if c == 0 else -d)) % n * 2 + c, i * 2 + c) for i in range(n) for c in (0, 1)])


def split(v):
    hi = v.astype(jnp.bfloat16).astype(jnp.float32)
    lo = (v - hi).astype(jnp.bfloat16).astype(jnp.float32)
    return [hi, lo, v - hi - lo]


def far(array):
    return pltpu.with_memory_space_constraint(array, pltpu.HBM)


def own_kernel(targets, potential, log_tgt, out, pot, log, sems):
    f32, bf = jnp.float32, jnp.bfloat16
    copies = [
        pltpu.make_async_copy(targets, out.at[0:B], sems.at[0]),
        pltpu.make_async_copy(potential, pot, sems.at[1]),
        pltpu.make_async_copy(log_tgt, log, sems.at[2]),
    ]
    for copy in copies:
        copy.start()
    for copy in copies:
        copy.wait()
    rows = []
    for ref in (pot, log):
        rows += split(ref[...])
    extra = jnp.concatenate(rows + [jnp.zeros((2, B), f32)], axis=0).astype(bf)
    out[B : B + A8, :] = jnp.concatenate([extra, jnp.zeros((A8, out.shape[1] - B), bf)], axis=1)


def own_call(targets, potential, log_tgt):
    return pl.pallas_call(
        own_kernel,
        name="own",
        in_specs=[FAR] * 3,
        out_specs=WHOLE,
        out_shape=jax.ShapeDtypeStruct((B + A8, targets.shape[1]), targets.dtype),
        scratch_shapes=[pltpu.VMEM((1, B), jnp.float32)] * 2 + [pltpu.SemaphoreType.DMA((3,))],
        compiler_params=params(4),
    )(*[far(a) for a in (targets, potential.reshape(1, B), log_tgt.reshape(1, B))])


def near_kernel(sources, log_src, out, log, sems):
    copies = [
        pltpu.make_async_copy(sources, out.at[0 : sources.shape[0]], sems.at[0]),
        pltpu.make_async_copy(log_src, log, sems.at[1]),
    ]
    for copy in copies:
        copy.start()
    for copy in copies:
        copy.wait()
    f = out.shape[1]
    rows = [part[:, h * f : (h + 1) * f] for part in split(log[...]) for h in range(2)]
    out[sources.shape[0] :, :] = jnp.concatenate(rows + [jnp.zeros((2, f), jnp.float32)], axis=0).astype(out.dtype)


def near_call(sources, log_src):
    n, f = sources.shape
    return pl.pallas_call(
        near_kernel,
        name="near_message",
        in_specs=[FAR] * 2,
        out_specs=WHOLE,
        out_shape=jax.ShapeDtypeStruct((n + A8, f), sources.dtype),
        scratch_shapes=[pltpu.VMEM((1, n), jnp.float32), pltpu.SemaphoreType.DMA((2,))],
        compiler_params=params(4),
    )(far(sources), far(log_src.reshape(1, n)))


def joined(picks, msgs):
    def kernel(*refs):
        out = refs[-1]
        extra = []
        for p, (m, k) in enumerate(picks):
            out[p * B : (p + 1) * B, :] = refs[m][k * B : (k + 1) * B, :]
            extra.append(refs[m][refs[m].shape[0] - A8 :, k * B : (k + 1) * B])
        rest = out.shape[1] - len(picks) * B
        extra.append(jnp.zeros((A8, rest), out.dtype))
        out[len(picks) * B :, :] = jnp.concatenate(extra, axis=1)

    return pl.pallas_call(
        kernel,
        in_specs=[WHOLE] * len(msgs),
        out_specs=WHOLE,
        out_shape=jax.ShapeDtypeStruct((len(picks) * B + A8, msgs[0].shape[1]), msgs[0].dtype),
        compiler_params=params(4),
    )(*msgs)


def eye(n):
    return lax.broadcasted_iota(jnp.int32, (n, n), 0) == lax.broadcasted_iota(jnp.int32, (n, n), 1)


def to_col(row):
    n = row.shape[1]
    return jnp.sum(jnp.where(eye(n), jnp.broadcast_to(row, (n, n)), 0.0), axis=1, keepdims=True)


def to_row(col):
    n = col.shape[0]
    return jnp.sum(jnp.where(eye(n), jnp.broadcast_to(col, (n, n)), 0.0), axis=0, keepdims=True)


CH = 512


def block_of(msgs, m, k):
    extra = msgs[m][msgs[m].shape[0] - A8 :, k * B : (k + 1) * B]
    return msgs[m].at[k * B : (k + 1) * B], extra.astype(jnp.float32)


def row_lse(s_out, at, pot):
    t = pot.shape[0]

    def shifted(r):
        return s_out[r : r + 32, at] + jnp.concatenate([pot[r : r + 32, :]] * (CH // 128), axis=1)

    top = jnp.full((8, CH), -jnp.inf, jnp.float32)
    for r in range(0, t, 32):
        top = jnp.maximum(top, jnp.max(shifted(r).reshape(4, 8, CH), axis=0))
    top = jnp.max(top, axis=0, keepdims=True)
    tot = jnp.zeros((8, CH), jnp.float32)
    for r in range(0, t, 32):
        tot = tot + jnp.sum(jnp.exp2(shifted(r) - top).reshape(4, 8, CH), axis=0)
    return top + jnp.log2(jnp.sum(tot, axis=0, keepdims=True))


def scores(tg, src, scale2):
    return lax.dot_general(tg, src, (((1,), (1,)), ((), ())), preferred_element_type=jnp.float32) * scale2


def laid_out(msgs, picks, tg, pot):
    for p, (m, k) in enumerate(picks):
        rows, ex = block_of(msgs, m, k)
        tg[p * B : (p + 1) * B, :] = rows[...]
        po = (ex[0:1] + ex[1:2] + ex[2:3]) * LOG2E
        pot[p * B : (p + 1) * B, :] = jnp.broadcast_to(to_col(po), (B, 128))


def turned(tg, out, base):
    core = lax.axis_index("c")
    for q in range(tg.shape[0] // 128):
        flipped = tg[q * 128 : (q + 1) * 128, :].T
        for f in range(16):
            to = pl.multiple_of((((f % 2) ^ core) * 8 + f // 2) * 32, 32)
            out[pl.ds(to, 32), base + q * 128 : base + (q + 1) * 128] = flipped[f * 32 : (f + 1) * 32, :]


def own_kernel_first(scale2, sources, *refs):
    msgs, (s_out, lse_out, tgt_out, tg, pot) = refs[:-5], refs[-5:]
    laid_out(msgs, PICKS1, tg, pot)
    for n in range(sources.shape[0] // CH):
        at = slice(n * CH, (n + 1) * CH)
        s_out[:, at] = scores(tg[...], sources[at, :], scale2)
        lse_out[:, at] = row_lse(s_out, at, pot)
    turned(tg, tgt_out, 0)


def near_kernel_first(scale2, near, log_src, tg, pot, s_out, lse_out, log_out):
    ns = near.shape[0] - A8
    logs = near[ns:, :].astype(jnp.float32)
    logs = logs[0:2] + logs[2:4] + logs[4:6]
    for q in range(8):
        log_out[0, q : q + 1, :] = log_src[:, q * 128 : (q + 1) * 128] * LOG2E
        log_out[1, q : q + 1, :] = logs[q // 4 : q // 4 + 1, q % 4 * 128 : (q % 4 + 1) * 128] * LOG2E
    for n in range(ns // CH):
        at = slice(n * CH, (n + 1) * CH)
        s_out[:, at] = scores(tg[...], near[at, :], scale2)
        lse_out[:, at] = row_lse(s_out, at, pot)


def last_kernel(scale2, sources, near, lse_own, lse_near, tgt_in, *refs):
    msgs, (s_out, rows_out, tgt_out, lt_out, tg, pot) = refs[:-6], refs[-6:]
    laid_out(msgs, PICKS2, tg, pot)
    yh = lax.axis_index("yh")
    ns = sources.shape[0]
    for n in range(2 * ns // CH):
        at = slice(n * CH, (n + 1) * CH)
        first = n * CH < ns
        ref, lse_in, row, block = (sources, lse_own, n * CH, yh) if first else (near, lse_near, n * CH - ns, 1 - yh)
        s_out[:, at] = scores(tg[...], ref[row : row + CH, :], scale2)
        lse = added_lse(lse_in[:, row : row + CH], row_lse(s_out, at, pot))
        for i in range(CH // 128):
            piece = jnp.broadcast_to(lse[:, i * 128 : (i + 1) * 128][None], (rows_out.shape[0], 1, 128))
            q = row // 128 + i
            rows_out[:, block, q : q + 1, :] = piece
    for p, (m, k) in enumerate(PICKS):
        _, ex = block_of(msgs, m, k)
        lt_out[p : p + 1, 0:B] = (ex[3:4] + ex[4:5] + ex[5:6]) * LOG2E
    t1 = tgt_in.shape[1]
    tgt_out[:, :t1] = tgt_in[...]
    turned(tg, tgt_out, t1)


def added_lse(a, b):
    top = jnp.maximum(a, b)
    return top + jnp.log2(jnp.exp2(a - top) + jnp.exp2(b - top))


def scores_call(kernel, scale2, args, shapes, scratch, flops):
    return pl.pallas_call(
        lambda *a: kernel(scale2, *a),
        in_specs=[WHOLE] * len(args),
        out_specs=[WHOLE] * len(shapes),
        scratch_shapes=[pltpu.VMEM(s, d) for s, d in scratch],
        out_shape=[jax.ShapeDtypeStruct(s, d) for s, d in shapes],
        compiler_params=params(20),
        cost_estimate=pl.CostEstimate(flops=flops, bytes_accessed=1 << 22, transcendentals=1 << 20),
    )(*args)


def all_scores(sources, log_src, near, msgs, scale2):
    ns, f = sources.shape
    f32, bf = jnp.float32, jnp.bfloat16
    t1, t2 = len(PICKS1) * B, len(PICKS2) * B
    s1, lse1, tgt1, tg, pot = scores_call(
        own_kernel_first, scale2, [sources, *msgs[:6]],
        [((t1, ns), f32), ((1, ns), f32), ((f, t1), bf), ((t1, f), bf), ((t1, 128), f32)], [], 2 * t1 * ns * f,
    )
    s2, lse2, logs = scores_call(
        near_kernel_first, scale2, [near, log_src.reshape(1, ns), tg, pot],
        [((t1, ns), f32), ((1, ns), f32), ((2, ns // 128, 128), f32)], [], 2 * t1 * ns * f,
    )
    s3, rows, tgt, lt = scores_call(
        last_kernel, scale2, [sources, near, lse1, lse2, tgt1, *msgs],
        [((t2, 2 * ns), f32), ((32, 2, ns // 128, 128), f32), ((f, t1 + t2), bf), ((len(OFF), 128), f32)],
        [((t2, f), bf), ((t2, 128), f32)], 4 * t2 * ns * f,
    )
    return (s1, s2, s3), rows, logs, tgt, lt


def merged_lse(parts):
    top = jnp.max(parts, axis=0)
    return top + jnp.log2(jnp.sum(jnp.exp2(parts - top[None]), axis=0))


def slot_of(p):
    off = jnp.where(lax.axis_index("c") == 0, OFF[p], 16 - OFF[p])
    return (lax.axis_index("z") + off) % 16


def cols_kernel(parts, logs, s1, s2, s3, sp_out, msg_out, held, lse):
    yh = lax.axis_index("yh")
    for h in range(2):
        lse[h] = merged_lse(parts[:, h])
    for h, block in enumerate((yh, 1 - yh)):
        sp = logs[h] - lse[block]
        for r in range(8):
            sp_out[:, (h * 8 + r) * 128 : (h * 8 + r + 1) * 128] = sp[r : r + 1, :]
    held[...] = jnp.zeros_like(held)
    n1 = len(OFF1)
    ns = s1.shape[1]
    for p in range(len(OFF)):
        tops, totals = [], []
        for r in range(0, B, 8):
            lifted = []
            for k in range(2 * ns // 128):
                ref, base, col = (s3, (p - n1) * B, k * 128)
                if p < n1:
                    ref, base, col = (s1, p * B, k * 128) if k * 128 < ns else (s2, p * B, k * 128 - ns)
                lifted.append(ref[base + r : base + r + 8, col : col + 128] + sp_out[:, k * 128 : (k + 1) * 128])
            top = lifted[0]
            for v in lifted[1:]:
                top = jnp.maximum(top, v)
            total = jnp.exp2(lifted[0] - top)
            for v in lifted[1:]:
                total = total + jnp.exp2(v - top)
            tops.append(top)
            totals.append(total)
        tops, totals = jnp.concatenate(tops, axis=0), jnp.concatenate(totals, axis=0)
        top = jnp.max(tops, axis=1, keepdims=True)
        row = to_row(top + jnp.log2(jnp.sum(totals * jnp.exp2(tops - top), axis=1, keepdims=True)))
        row = jnp.concatenate([row, row], axis=1)
        slot = slot_of(p)
        at = slot // 2
        half = lax.broadcasted_iota(jnp.int32, (1, 128), 1) // B
        held[pl.ds(at, 1), :] = jnp.where(half == slot % 2, row, held[pl.ds(at, 1), :])
    msg_out[...] = jnp.broadcast_to(held[...][None], msg_out.shape)


def cols_call(parts, logs, s):
    ns = s[2].shape[1]
    return pl.pallas_call(
        cols_kernel,
        name="cols",
        in_specs=[WHOLE] * 5,
        out_specs=[WHOLE] * 2,
        scratch_shapes=[pltpu.VMEM((8, 128), jnp.float32), pltpu.VMEM((2, 8, 128), jnp.float32)],
        out_shape=[jax.ShapeDtypeStruct((1, ns), jnp.float32), jax.ShapeDtypeStruct((16, 8, 128), jnp.float32)],
        compiler_params=params(16),
    )(parts, logs, *s)


def moved_kernel(parts, lt, sp, s1, s2, s3, tgt, pot_out, theirs_out, mass_out, wide, tp, lse):
    lse[...] = merged_lse(parts[...])
    for p in range(len(OFF)):
        slot = slot_of(p)
        row = lse[pl.ds(slot // 2, 1), :]
        row = jnp.where(slot % 2 == 0, row[:, :B], row[:, B:])
        tpot = lt[p : p + 1, 0:B] - row
        if p == 0:
            pot_out[:, 0:B] = tpot * LN2
        tp[p * B : (p + 1) * B, :] = jnp.broadcast_to(to_col(tpot), (B, 128))

    t1, ns = s1.shape
    half = tgt.shape[0] // 2
    for n in range(sp.shape[1] // CH):
        at = slice(n * CH, (n + 1) * CH)
        spn = sp[:, at]
        mass = jnp.zeros((8, CH), jnp.float32)
        for r in range(0, tp.shape[0], 32):
            if r >= t1:
                s = s3[r - t1 : r - t1 + 32, at]
            elif n * CH < ns:
                s = s1[r : r + 32, at]
            else:
                s = s2[r : r + 32, n * CH - ns : (n + 1) * CH - ns]
            e = jnp.exp2(s + spn + jnp.concatenate([tp[r : r + 32, :]] * (CH // 128), axis=1))
            mass = mass + jnp.sum(e.reshape(4, 8, CH), axis=0)
            wide[r : r + 32, at] = e.astype(jnp.bfloat16)
        mass = jnp.sum(mass, axis=0, keepdims=True)
        mass_out[:, at] = mass
        part = jnp.dot(tgt[half:, :], wide[:, at], preferred_element_type=jnp.float32)
        theirs_out[0:half, at] = part.astype(jnp.bfloat16)
        hi = mass.astype(jnp.bfloat16).astype(jnp.float32)
        pad = jnp.zeros((6, CH), jnp.float32)
        theirs_out[half : half + 8, at] = jnp.concatenate([hi, mass - hi, pad], axis=0).astype(jnp.bfloat16)


def moved_call(parts, lt, sp, s, tgt):
    ns = sp.shape[1]
    f, t = tgt.shape
    return pl.pallas_call(
        moved_kernel,
        name="moved",
        in_specs=[WHOLE] * 7,
        out_specs=[WHOLE] * 4,
        scratch_shapes=[pltpu.VMEM((t, 128), jnp.float32), pltpu.VMEM((8, 128), jnp.float32)],
        out_shape=[
            jax.ShapeDtypeStruct((1, 128), jnp.float32),
            jax.ShapeDtypeStruct((f // 2 + 8, ns), jnp.bfloat16),
            jax.ShapeDtypeStruct((1, ns), jnp.float32),
            jax.ShapeDtypeStruct((t, ns), jnp.bfloat16),
        ],
        compiler_params=params(20),
    )(parts, lt, sp, *s, tgt)


def mine_kernel(tgt, wide, out):
    for n in range(out.shape[1] // CH):
        at = slice(n * CH, (n + 1) * CH)
        part = jnp.dot(tgt[: out.shape[0], :], wide[:, at], preferred_element_type=jnp.float32)
        out[:, at] = part.astype(jnp.bfloat16)


def mine_call(tgt, wide):
    f, t = tgt.shape
    ns = wide.shape[1]
    return pl.pallas_call(
        mine_kernel,
        name="mine",
        in_specs=[WHOLE] * 2,
        out_specs=WHOLE,
        out_shape=jax.ShapeDtypeStruct((f // 2, ns), jnp.bfloat16),
        compiler_params=params(12),
        cost_estimate=pl.CostEstimate(flops=f * t * ns, bytes_accessed=2 * t * ns, transcendentals=0),
    )(tgt, wide)


def pack_kernel(mine, theirs, mass, out):
    f32 = jnp.float32
    extra = theirs[256:264, :].astype(f32)
    total = mass[...] + extra[0:1] + extra[1:2]
    hi = total.astype(jnp.bfloat16).astype(f32)
    lo = total - hi
    yh = lax.axis_index("yh")
    for h in range(2):
        to = (h ^ yh) * 2
        rows = [v[:, (h * 8 + q) * 128 : (h * 8 + q + 1) * 128] for v in (hi, lo) for q in range(8)]
        rows = jnp.concatenate(rows, axis=0).astype(jnp.bfloat16)
        for g in range(8):
            at_chip = g % 4 * 4 + g // 4
            for q in range(8):
                at = (slice(g * 32, (g + 1) * 32), slice((h * 8 + q) * 128, (h * 8 + q + 1) * 128))
                both = mine[at].astype(f32) + theirs[at].astype(f32)
                out[to + at_chip, q * 32 : (q + 1) * 32, :] = both.astype(jnp.bfloat16)
            out[to + at_chip, 256:272, :] = rows


def pack_call(mine, theirs, mass):
    return pl.pallas_call(
        pack_kernel,
        name="pack",
        in_specs=[WHOLE] * 3,
        out_specs=WHOLE,
        out_shape=jax.ShapeDtypeStruct((16, 272, 128), jnp.bfloat16),
        compiler_params=params(8),
    )(mine, theirs, mass)


def finish_kernel(parts, sp, tpot, out, src_pot, tgt_pot):
    f32 = jnp.float32

    def added(at):
        total = parts[0, at, :].astype(f32)
        for k in range(1, parts.shape[0]):
            total = total + parts[k, at, :].astype(f32)
        return total

    for q in range(8):
        src_pot[q : q + 1, :] = sp[:, q * 128 : (q + 1) * 128] * LN2
    tgt_pot[...] = tpot[:, 0:B]
    mass = added(slice(256, 272))
    mass = mass[:8] + mass[8:]
    for q in range(8):
        image = added(slice(q * 32, (q + 1) * 32)) / mass[q : q + 1, :]
        out[:, q * 128 : (q + 1) * 128] = image.astype(jnp.bfloat16)


def finish_call(parts, sp, tpot):
    return pl.pallas_call(
        finish_kernel,
        name="finish",
        in_specs=[WHOLE] * 3,
        out_specs=[WHOLE] * 3,
        out_shape=[
            jax.ShapeDtypeStruct((32, 1024), jnp.bfloat16),
            jax.ShapeDtypeStruct((8, 128), jnp.float32),
            jax.ShapeDtypeStruct((1, B), jnp.float32),
        ],
        compiler_params=params(8),
    )(parts, sp, tpot)


def body(sources, log_src, targets, potential, log_tgt):
    f = sources.shape[1]
    scale2 = LOG2E / math.sqrt(f)

    own = own_call(targets, potential, log_tgt)
    ra = from_z(own, 4)
    la = from_z(own, -5)
    near = sent(near_call(sources, log_src), ("yh", "yl"), [(0, 3), (3, 0), (1, 2), (2, 1)])
    rb = from_z(joined([(0, 0), (1, 0)], [own, ra]), 2)
    lb = from_z(joined([(1, 0), (0, 0)], [own, la]), -2)
    rc = from_z(joined([(0, 0), (1, 0), (1, 1), (2, 0), (3, 0)], [own, rb, ra, la]), 1)
    lc = from_z(joined([(0, 0), (1, 0), (1, 1), (2, 0)], [own, lb, la]), -1)
    s, rows, logs, tgt, lt = all_scores(sources, log_src, near, [own, ra, la, rb, lb, rc, lc], scale2)
    row_parts = lax.all_to_all(rows, PLANE, split_axis=0, concat_axis=0, tiled=True)
    sp, cols = cols_call(row_parts, logs, s)
    col_parts = lax.all_to_all(cols, "z", split_axis=0, concat_axis=0, tiled=True)
    tpot, theirs, mass, wide = moved_call(col_parts, lt, sp, s, tgt)
    theirs = lax.ppermute(theirs, "c", [(0, 1), (1, 0)])
    packed = pack_call(mine_call(tgt, wide), theirs, mass)
    parts = lax.all_to_all(packed, CHIPS, split_axis=0, concat_axis=0, tiled=True)
    mapped, src_pot, tgt_pot = finish_call(parts, sp, tpot)
    return (src_pot.reshape(-1), tgt_pot.reshape(-1), mapped.T)


def solution(mesh):
    torus = Mesh(mesh.devices.reshape(16, 2, 2, 4, 2), AXES)
    src, every = ("z", "yh"), ("z", "yh", "yl", "x", "c")
    return jax.shard_map(
        body,
        mesh=torus,
        in_specs=(P(src, None), P(src), P(every, None), P(every), P(every)),
        out_specs=(P(src), P(every), P(src, ("yl", "x", "c"))),
        check_vma=False,
    )
```

```python
import math

import jax
import jax.numpy as jnp
from jax import lax
from jax.experimental import pallas as pl
from jax.experimental.pallas import tpu as pltpu
from jax.sharding import Mesh
from jax.sharding import PartitionSpec as P


WHOLE = pl.BlockSpec(memory_space=pltpu.VMEM)
FAR = pl.BlockSpec(memory_space=pltpu.HBM)
AXES = ("z", "yh", "yl", "x", "c")
PLANE = ("c", "x", "yh", "yl")
CHIPS = ("x", "yh", "yl")
LOG2E = math.log2(math.e)
LN2 = math.log(2.0)
B = 64
A8 = 8
OFF1 = (0, 4, 11, 2, 6, 9, 14, 1, 3, 7, 5, 12)
OFF2 = (15, 8, 13, 10)
OFF = OFF1 + OFF2
PICKS = tuple((m, k) for m, count in enumerate((1, 1, 1, 2, 2, 5, 4)) for k in range(count))
PICKS1 = PICKS[: len(OFF1)]
PICKS2 = PICKS[len(OFF1) :]


MIB = 1 << 20


def params(mib):
    return pltpu.CompilerParams(vmem_limit_bytes=mib * MIB)


def sent(array, axes, pairs):
    return lax.ppermute(array, axes, pairs)


def from_z(array, d):
    n = lax.axis_size("z")
    return sent(array, ("z", "c"), [((i + (d if c == 0 else -d)) % n * 2 + c, i * 2 + c) for i in range(n) for c in (0, 1)])


def split(v):
    hi = v.astype(jnp.bfloat16).astype(jnp.float32)
    lo = (v - hi).astype(jnp.bfloat16).astype(jnp.float32)
    return [hi, lo, v - hi - lo]


def far(array):
    return pltpu.with_memory_space_constraint(array, pltpu.HBM)


def own_kernel(targets, potential, log_tgt, out, pot, log, sems):
    f32, bf = jnp.float32, jnp.bfloat16
    copies = [
        pltpu.make_async_copy(targets, out.at[0:B], sems.at[0]),
        pltpu.make_async_copy(potential, pot, sems.at[1]),
        pltpu.make_async_copy(log_tgt, log, sems.at[2]),
    ]
    for copy in copies:
        copy.start()
    for copy in copies:
        copy.wait()
    rows = []
    for ref in (pot, log):
        rows += split(ref[...])
    extra = jnp.concatenate(rows + [jnp.zeros((2, B), f32)], axis=0).astype(bf)
    out[B : B + A8, :] = jnp.concatenate([extra, jnp.zeros((A8, out.shape[1] - B), bf)], axis=1)


def own_call(targets, potential, log_tgt):
    return pl.pallas_call(
        own_kernel,
        name="own",
        in_specs=[FAR] * 3,
        out_specs=WHOLE,
        out_shape=jax.ShapeDtypeStruct((B + A8, targets.shape[1]), targets.dtype),
        scratch_shapes=[pltpu.VMEM((1, B), jnp.float32)] * 2 + [pltpu.SemaphoreType.DMA((3,))],
        compiler_params=params(4),
    )(*[far(a) for a in (targets, potential.reshape(1, B), log_tgt.reshape(1, B))])


def near_kernel(sources, log_src, out, log, sems):
    n = out.shape[0] - A8
    core = lax.axis_index("c")
    copies = [
        pltpu.make_async_copy(sources.at[pl.ds(pl.multiple_of(core * n, n), n)], out.at[0:n], sems.at[0]),
        pltpu.make_async_copy(log_src, log, sems.at[1]),
    ]
    for copy in copies:
        copy.start()
    for copy in copies:
        copy.wait()
    rows = split(jnp.where(core == 0, log[:, :n], log[:, n:]))
    out[n:, :] = jnp.concatenate(rows + [jnp.zeros((A8 - 3, n), jnp.float32)], axis=0).astype(out.dtype)


def near_call(sources, log_src):
    n, f = sources.shape
    return pl.pallas_call(
        near_kernel,
        name="near_message",
        in_specs=[FAR] * 2,
        out_specs=WHOLE,
        out_shape=jax.ShapeDtypeStruct((n // 2 + A8, f), sources.dtype),
        scratch_shapes=[pltpu.VMEM((1, n), jnp.float32), pltpu.SemaphoreType.DMA((2,))],
        compiler_params=params(4),
    )(far(sources), far(log_src.reshape(1, n)))


def joined(picks, msgs):
    def kernel(*refs):
        out = refs[-1]
        extra = []
        for p, (m, k) in enumerate(picks):
            out[p * B : (p + 1) * B, :] = refs[m][k * B : (k + 1) * B, :]
            extra.append(refs[m][refs[m].shape[0] - A8 :, k * B : (k + 1) * B])
        rest = out.shape[1] - len(picks) * B
        extra.append(jnp.zeros((A8, rest), out.dtype))
        out[len(picks) * B :, :] = jnp.concatenate(extra, axis=1)

    return pl.pallas_call(
        kernel,
        in_specs=[WHOLE] * len(msgs),
        out_specs=WHOLE,
        out_shape=jax.ShapeDtypeStruct((len(picks) * B + A8, msgs[0].shape[1]), msgs[0].dtype),
        compiler_params=params(4),
    )(*msgs)


def eye(n):
    return lax.broadcasted_iota(jnp.int32, (n, n), 0) == lax.broadcasted_iota(jnp.int32, (n, n), 1)


def to_col(row):
    n = row.shape[1]
    return jnp.sum(jnp.where(eye(n), jnp.broadcast_to(row, (n, n)), 0.0), axis=1, keepdims=True)


def to_row(col):
    n = col.shape[0]
    return jnp.sum(jnp.where(eye(n), jnp.broadcast_to(col, (n, n)), 0.0), axis=0, keepdims=True)


CH = 512


def block_of(msgs, m, k):
    extra = msgs[m][msgs[m].shape[0] - A8 :, k * B : (k + 1) * B]
    return msgs[m].at[k * B : (k + 1) * B], extra.astype(jnp.float32)


def row_lse(s_out, at, pot):
    t = pot.shape[0]

    def shifted(r):
        return s_out[r : r + 32, at] + jnp.concatenate([pot[r : r + 32, :]] * (CH // 128), axis=1)

    top = jnp.full((8, CH), -jnp.inf, jnp.float32)
    for r in range(0, t, 32):
        top = jnp.maximum(top, jnp.max(shifted(r).reshape(4, 8, CH), axis=0))
    top = jnp.max(top, axis=0, keepdims=True)
    tot = jnp.zeros((8, CH), jnp.float32)
    for r in range(0, t, 32):
        tot = tot + jnp.sum(jnp.exp2(shifted(r) - top).reshape(4, 8, CH), axis=0)
    return top + jnp.log2(jnp.sum(tot, axis=0, keepdims=True))


def scores(tg, src, scale2):
    return lax.dot_general(tg, src, (((1,), (1,)), ((), ())), preferred_element_type=jnp.float32) * scale2


def laid_out(msgs, picks, tg, pot):
    for p, (m, k) in enumerate(picks):
        rows, ex = block_of(msgs, m, k)
        tg[p * B : (p + 1) * B, :] = rows[...]
        po = (ex[0:1] + ex[1:2] + ex[2:3]) * LOG2E
        pot[p * B : (p + 1) * B, :] = jnp.broadcast_to(to_col(po), (B, 128))


def turned(tg, out, base):
    core = lax.axis_index("c")
    for q in range(tg.shape[0] // 128):
        flipped = tg[q * 128 : (q + 1) * 128, :].T
        for f in range(16):
            to = pl.multiple_of((((f % 2) ^ core) * 8 + f // 2) * 32, 32)
            out[pl.ds(to, 32), base + q * 128 : base + (q + 1) * 128] = flipped[f * 32 : (f + 1) * 32, :]


def own_kernel_first(scale2, sources, *refs):
    msgs, (s_out, lse_out, tgt_out, tg, pot) = refs[:-5], refs[-5:]
    laid_out(msgs, PICKS1, tg, pot)
    for n in range(sources.shape[0] // CH):
        at = slice(n * CH, (n + 1) * CH)
        s_out[:, at] = scores(tg[...], sources[at, :], scale2)
        lse_out[:, at] = row_lse(s_out, at, pot)
    turned(tg, tgt_out, 0)


def near_kernel_first(scale2, near, swapped, log_src, tg, pot, s_out, lse_out, log_out):
    core = lax.axis_index("c")
    halves = []
    for ref in (near, swapped):
        parts = ref[CH:, :].astype(jnp.float32)
        halves.append(parts[0:1] + parts[1:2] + parts[2:3])
    for q in range(8):
        at = slice(q % 4 * 128, (q % 4 + 1) * 128)
        log_out[0, q : q + 1, :] = log_src[:, q * 128 : (q + 1) * 128] * LOG2E
        log_out[1, q : q + 1, :] = jnp.where(core == q // 4, halves[0][:, at], halves[1][:, at]) * LOG2E
    for ref, half in ((near, core), (swapped, 1 - core)):
        at = pl.ds(pl.multiple_of(half * CH, CH), CH)
        s_out[:, at] = scores(tg[...], ref[0:CH, :], scale2)
        lse_out[:, at] = row_lse(s_out, at, pot)


def last_kernel(scale2, sources, near, swapped, lse_own, lse_near, tgt_in, *refs):
    msgs, (s_out, rows_out, tgt_out, lt_out, tg, pot) = refs[:-6], refs[-6:]
    laid_out(msgs, PICKS2, tg, pot)
    yh, core = lax.axis_index("yh"), lax.axis_index("c")
    ns = sources.shape[0]
    for ref, row, lse_in, half, base, block in (
        (sources, 0, lse_own, 0, 0, yh),
        (sources, CH, lse_own, 1, 0, yh),
        (near, 0, lse_near, core, ns, 1 - yh),
        (swapped, 0, lse_near, 1 - core, ns, 1 - yh),
    ):
        begin = half * CH if isinstance(half, int) else pl.multiple_of(half * CH, CH)
        at = pl.ds(base + begin, CH)
        s_out[:, at] = scores(tg[...], ref[row : row + CH, :], scale2)
        lse = added_lse(lse_in[:, pl.ds(begin, CH)], row_lse(s_out, at, pot))
        for i in range(CH // 128):
            piece = jnp.broadcast_to(lse[:, i * 128 : (i + 1) * 128][None], (rows_out.shape[0], 1, 128))
            rows_out[:, block, pl.ds(half * (CH // 128) + i, 1), :] = piece
    for p, (m, k) in enumerate(PICKS):
        _, ex = block_of(msgs, m, k)
        lt_out[p : p + 1, 0:B] = (ex[3:4] + ex[4:5] + ex[5:6]) * LOG2E
    t1 = tgt_in.shape[1]
    tgt_out[:, :t1] = tgt_in[...]
    turned(tg, tgt_out, t1)


def added_lse(a, b):
    top = jnp.maximum(a, b)
    return top + jnp.log2(jnp.exp2(a - top) + jnp.exp2(b - top))


def scores_call(kernel, scale2, args, shapes, scratch, flops):
    return pl.pallas_call(
        lambda *a: kernel(scale2, *a),
        in_specs=[WHOLE] * len(args),
        out_specs=[WHOLE] * len(shapes),
        scratch_shapes=[pltpu.VMEM(s, d) for s, d in scratch],
        out_shape=[jax.ShapeDtypeStruct(s, d) for s, d in shapes],
        compiler_params=params(20),
        cost_estimate=pl.CostEstimate(flops=flops, bytes_accessed=1 << 22, transcendentals=1 << 20),
    )(*args)


def all_scores(sources, log_src, near, swapped, msgs, scale2):
    ns, f = sources.shape
    f32, bf = jnp.float32, jnp.bfloat16
    t1, t2 = len(PICKS1) * B, len(PICKS2) * B
    s1, lse1, tgt1, tg, pot = scores_call(
        own_kernel_first, scale2, [sources, *msgs[:6]],
        [((t1, ns), f32), ((1, ns), f32), ((f, t1), bf), ((t1, f), bf), ((t1, 128), f32)], [], 2 * t1 * ns * f,
    )
    s2, lse2, logs = scores_call(
        near_kernel_first, scale2, [near, swapped, log_src.reshape(1, ns), tg, pot],
        [((t1, ns), f32), ((1, ns), f32), ((2, ns // 128, 128), f32)], [], 2 * t1 * ns * f,
    )
    s3, rows, tgt, lt = scores_call(
        last_kernel, scale2, [sources, near, swapped, lse1, lse2, tgt1, *msgs],
        [((t2, 2 * ns), f32), ((32, 2, ns // 128, 128), f32), ((f, t1 + t2), bf), ((len(OFF), 128), f32)],
        [((t2, f), bf), ((t2, 128), f32)], 4 * t2 * ns * f,
    )
    return (s1, s2, s3), rows, logs, tgt, lt


def merged_lse(parts):
    top = jnp.max(parts, axis=0)
    return top + jnp.log2(jnp.sum(jnp.exp2(parts - top[None]), axis=0))


def slot_of(p):
    off = jnp.where(lax.axis_index("c") == 0, OFF[p], 16 - OFF[p])
    return (lax.axis_index("z") + off) % 16


def cols_kernel(parts, logs, s1, s2, s3, sp_out, msg_out, held, lse):
    yh = lax.axis_index("yh")
    for h in range(2):
        lse[h] = merged_lse(parts[:, h])
    for h, block in enumerate((yh, 1 - yh)):
        sp = logs[h] - lse[block]
        for r in range(8):
            sp_out[:, (h * 8 + r) * 128 : (h * 8 + r + 1) * 128] = sp[r : r + 1, :]
    held[...] = jnp.zeros_like(held)
    n1 = len(OFF1)
    ns = s1.shape[1]
    for p in range(len(OFF)):
        tops, totals = [], []
        for r in range(0, B, 8):
            lifted = []
            for k in range(2 * ns // 128):
                ref, base, col = (s3, (p - n1) * B, k * 128)
                if p < n1:
                    ref, base, col = (s1, p * B, k * 128) if k * 128 < ns else (s2, p * B, k * 128 - ns)
                lifted.append(ref[base + r : base + r + 8, col : col + 128] + sp_out[:, k * 128 : (k + 1) * 128])
            top = lifted[0]
            for v in lifted[1:]:
                top = jnp.maximum(top, v)
            total = jnp.exp2(lifted[0] - top)
            for v in lifted[1:]:
                total = total + jnp.exp2(v - top)
            tops.append(top)
            totals.append(total)
        tops, totals = jnp.concatenate(tops, axis=0), jnp.concatenate(totals, axis=0)
        top = jnp.max(tops, axis=1, keepdims=True)
        row = to_row(top + jnp.log2(jnp.sum(totals * jnp.exp2(tops - top), axis=1, keepdims=True)))
        row = jnp.concatenate([row, row], axis=1)
        slot = slot_of(p)
        at = slot // 2
        half = lax.broadcasted_iota(jnp.int32, (1, 128), 1) // B
        held[pl.ds(at, 1), :] = jnp.where(half == slot % 2, row, held[pl.ds(at, 1), :])
    msg_out[...] = jnp.broadcast_to(held[...][None], msg_out.shape)


def cols_call(parts, logs, s):
    ns = s[2].shape[1]
    return pl.pallas_call(
        cols_kernel,
        name="cols",
        in_specs=[WHOLE] * 5,
        out_specs=[WHOLE] * 2,
        scratch_shapes=[pltpu.VMEM((8, 128), jnp.float32), pltpu.VMEM((2, 8, 128), jnp.float32)],
        out_shape=[jax.ShapeDtypeStruct((1, ns), jnp.float32), jax.ShapeDtypeStruct((16, 8, 128), jnp.float32)],
        compiler_params=params(16),
    )(parts, logs, *s)


def moved_kernel(parts, lt, sp, s1, s2, s3, tgt, pot_out, theirs_out, mass_out, wide, tp, lse):
    lse[...] = merged_lse(parts[...])
    for p in range(len(OFF)):
        slot = slot_of(p)
        row = lse[pl.ds(slot // 2, 1), :]
        row = jnp.where(slot % 2 == 0, row[:, :B], row[:, B:])
        tpot = lt[p : p + 1, 0:B] - row
        if p == 0:
            pot_out[:, 0:B] = tpot * LN2
        tp[p * B : (p + 1) * B, :] = jnp.broadcast_to(to_col(tpot), (B, 128))

    t1, ns = s1.shape
    half = tgt.shape[0] // 2
    for n in range(sp.shape[1] // CH):
        at = slice(n * CH, (n + 1) * CH)
        spn = sp[:, at]
        mass = jnp.zeros((8, CH), jnp.float32)
        for r in range(0, tp.shape[0], 32):
            if r >= t1:
                s = s3[r - t1 : r - t1 + 32, at]
            elif n * CH < ns:
                s = s1[r : r + 32, at]
            else:
                s = s2[r : r + 32, n * CH - ns : (n + 1) * CH - ns]
            e = jnp.exp2(s + spn + jnp.concatenate([tp[r : r + 32, :]] * (CH // 128), axis=1))
            mass = mass + jnp.sum(e.reshape(4, 8, CH), axis=0)
            wide[r : r + 32, at] = e.astype(jnp.bfloat16)
        mass = jnp.sum(mass, axis=0, keepdims=True)
        mass_out[:, at] = mass
        part = jnp.dot(tgt[half:, :], wide[:, at], preferred_element_type=jnp.float32)
        theirs_out[0:half, at] = part.astype(jnp.bfloat16)
        hi = mass.astype(jnp.bfloat16).astype(jnp.float32)
        pad = jnp.zeros((6, CH), jnp.float32)
        theirs_out[half : half + 8, at] = jnp.concatenate([hi, mass - hi, pad], axis=0).astype(jnp.bfloat16)


def moved_call(parts, lt, sp, s, tgt):
    ns = sp.shape[1]
    f, t = tgt.shape
    return pl.pallas_call(
        moved_kernel,
        name="moved",
        in_specs=[WHOLE] * 7,
        out_specs=[WHOLE] * 4,
        scratch_shapes=[pltpu.VMEM((t, 128), jnp.float32), pltpu.VMEM((8, 128), jnp.float32)],
        out_shape=[
            jax.ShapeDtypeStruct((1, 128), jnp.float32),
            jax.ShapeDtypeStruct((f // 2 + 8, ns), jnp.bfloat16),
            jax.ShapeDtypeStruct((1, ns), jnp.float32),
            jax.ShapeDtypeStruct((t, ns), jnp.bfloat16),
        ],
        compiler_params=params(20),
    )(parts, lt, sp, *s, tgt)


def mine_kernel(tgt, wide, out):
    for n in range(out.shape[1] // CH):
        at = slice(n * CH, (n + 1) * CH)
        part = jnp.dot(tgt[: out.shape[0], :], wide[:, at], preferred_element_type=jnp.float32)
        out[:, at] = part.astype(jnp.bfloat16)


def mine_call(tgt, wide):
    f, t = tgt.shape
    ns = wide.shape[1]
    return pl.pallas_call(
        mine_kernel,
        name="mine",
        in_specs=[WHOLE] * 2,
        out_specs=WHOLE,
        out_shape=jax.ShapeDtypeStruct((f // 2, ns), jnp.bfloat16),
        compiler_params=params(12),
        cost_estimate=pl.CostEstimate(flops=f * t * ns, bytes_accessed=2 * t * ns, transcendentals=0),
    )(tgt, wide)


def pack_kernel(mine, theirs, mass, out):
    f32 = jnp.float32
    extra = theirs[256:264, :].astype(f32)
    total = mass[...] + extra[0:1] + extra[1:2]
    hi = total.astype(jnp.bfloat16).astype(f32)
    lo = total - hi
    yh = lax.axis_index("yh")
    for h in range(2):
        to = (h ^ yh) * 2
        rows = [v[:, (h * 8 + q) * 128 : (h * 8 + q + 1) * 128] for v in (hi, lo) for q in range(8)]
        rows = jnp.concatenate(rows, axis=0).astype(jnp.bfloat16)
        for g in range(8):
            at_chip = g % 4 * 4 + g // 4
            for q in range(8):
                at = (slice(g * 32, (g + 1) * 32), slice((h * 8 + q) * 128, (h * 8 + q + 1) * 128))
                both = mine[at].astype(f32) + theirs[at].astype(f32)
                out[to + at_chip, q * 32 : (q + 1) * 32, :] = both.astype(jnp.bfloat16)
            out[to + at_chip, 256:272, :] = rows


def pack_call(mine, theirs, mass):
    return pl.pallas_call(
        pack_kernel,
        name="pack",
        in_specs=[WHOLE] * 3,
        out_specs=WHOLE,
        out_shape=jax.ShapeDtypeStruct((16, 272, 128), jnp.bfloat16),
        compiler_params=params(8),
    )(mine, theirs, mass)


def finish_kernel(parts, sp, tpot, out, src_pot, tgt_pot):
    f32 = jnp.float32

    def added(at):
        total = parts[0, at, :].astype(f32)
        for k in range(1, parts.shape[0]):
            total = total + parts[k, at, :].astype(f32)
        return total

    for q in range(8):
        src_pot[q : q + 1, :] = sp[:, q * 128 : (q + 1) * 128] * LN2
    tgt_pot[...] = tpot[:, 0:B]
    mass = added(slice(256, 272))
    mass = mass[:8] + mass[8:]
    for q in range(8):
        image = added(slice(q * 32, (q + 1) * 32)) / mass[q : q + 1, :]
        out[:, q * 128 : (q + 1) * 128] = image.astype(jnp.bfloat16)


def finish_call(parts, sp, tpot):
    return pl.pallas_call(
        finish_kernel,
        name="finish",
        in_specs=[WHOLE] * 3,
        out_specs=[WHOLE] * 3,
        out_shape=[
            jax.ShapeDtypeStruct((32, 1024), jnp.bfloat16),
            jax.ShapeDtypeStruct((8, 128), jnp.float32),
            jax.ShapeDtypeStruct((1, B), jnp.float32),
        ],
        compiler_params=params(8),
    )(parts, sp, tpot)


def body(sources, log_src, targets, potential, log_tgt):
    f = sources.shape[1]
    scale2 = LOG2E / math.sqrt(f)

    own = own_call(targets, potential, log_tgt)
    ra = from_z(own, 4)
    la = from_z(own, -5)
    near = sent(near_call(sources, log_src), ("yh", "yl"), [(0, 3), (3, 0), (1, 2), (2, 1)])
    rb = from_z(joined([(0, 0), (1, 0)], [own, ra]), 2)
    lb = from_z(joined([(1, 0), (0, 0)], [own, la]), -2)
    rc = from_z(joined([(0, 0), (1, 0), (1, 1), (2, 0), (3, 0)], [own, rb, ra, la]), 1)
    lc = from_z(joined([(0, 0), (1, 0), (1, 1), (2, 0)], [own, lb, la]), -1)
    swapped = sent(near, "c", [(0, 1), (1, 0)])
    s, rows, logs, tgt, lt = all_scores(sources, log_src, near, swapped, [own, ra, la, rb, lb, rc, lc], scale2)
    row_parts = lax.all_to_all(rows, PLANE, split_axis=0, concat_axis=0, tiled=True)
    sp, cols = cols_call(row_parts, logs, s)
    col_parts = lax.all_to_all(cols, "z", split_axis=0, concat_axis=0, tiled=True)
    tpot, theirs, mass, wide = moved_call(col_parts, lt, sp, s, tgt)
    theirs = lax.ppermute(theirs, "c", [(0, 1), (1, 0)])
    packed = pack_call(mine_call(tgt, wide), theirs, mass)
    parts = lax.all_to_all(packed, CHIPS, split_axis=0, concat_axis=0, tiled=True)
    mapped, src_pot, tgt_pot = finish_call(parts, sp, tpot)
    return (src_pot.reshape(-1), tgt_pot.reshape(-1), mapped.T)


def solution(mesh):
    torus = Mesh(mesh.devices.reshape(16, 2, 2, 4, 2), AXES)
    src, every = ("z", "yh"), ("z", "yh", "yl", "x", "c")
    return jax.shard_map(
        body,
        mesh=torus,
        in_specs=(P(src, None), P(src), P(every, None), P(every), P(every)),
        out_specs=(P(src), P(every), P(src, ("yl", "x", "c"))),
        check_vma=False,
    )
```

```python
import math

import jax
import jax.numpy as jnp
from jax import lax
from jax.experimental import pallas as pl
from jax.experimental.pallas import tpu as pltpu
from jax.sharding import Mesh
from jax.sharding import PartitionSpec as P


WHOLE = pl.BlockSpec(memory_space=pltpu.VMEM)
FAR = pl.BlockSpec(memory_space=pltpu.HBM)
AXES = ("z", "yh", "yl", "x", "c")
PLANE = ("c", "x", "yh", "yl")
CHIPS = ("yl", "yh", "x")
LOG2E = math.log2(math.e)
LN2 = math.log(2.0)
B = 64
A8 = 8
OFF1 = (0, 4, 11, 2, 6, 9, 14, 1, 3, 7, 5, 12)
OFF2 = (15, 8, 13, 10)
OFF = OFF1 + OFF2
PICKS = tuple((m, k) for m, count in enumerate((1, 1, 1, 2, 2, 5, 4)) for k in range(count))
PICKS1 = PICKS[: len(OFF1)]
PICKS2 = PICKS[len(OFF1) :]


MIB = 1 << 20


def params(mib):
    return pltpu.CompilerParams(vmem_limit_bytes=mib * MIB)


def sent(array, axes, pairs):
    return lax.ppermute(array, axes, pairs)


def from_z(array, d):
    n = lax.axis_size("z")
    return sent(array, ("z", "c"), [((i + (d if c == 0 else -d)) % n * 2 + c, i * 2 + c) for i in range(n) for c in (0, 1)])


def split(v):
    hi = v.astype(jnp.bfloat16).astype(jnp.float32)
    lo = (v - hi).astype(jnp.bfloat16).astype(jnp.float32)
    return [hi, lo, v - hi - lo]


def far(array):
    return pltpu.with_memory_space_constraint(array, pltpu.HBM)


def own_kernel(targets, potential, log_tgt, out, pot, log, sems):
    f32, bf = jnp.float32, jnp.bfloat16
    copies = [
        pltpu.make_async_copy(targets, out.at[0:B], sems.at[0]),
        pltpu.make_async_copy(potential, pot, sems.at[1]),
        pltpu.make_async_copy(log_tgt, log, sems.at[2]),
    ]
    for copy in copies:
        copy.start()
    for copy in copies:
        copy.wait()
    rows = []
    for ref in (pot, log):
        rows += split(ref[...])
    extra = jnp.concatenate(rows + [jnp.zeros((2, B), f32)], axis=0).astype(bf)
    out[B : B + A8, :] = jnp.concatenate([extra, jnp.zeros((A8, out.shape[1] - B), bf)], axis=1)


def own_call(targets, potential, log_tgt):
    return pl.pallas_call(
        own_kernel,
        name="own",
        in_specs=[FAR] * 3,
        out_specs=WHOLE,
        out_shape=jax.ShapeDtypeStruct((B + A8, targets.shape[1]), targets.dtype),
        scratch_shapes=[pltpu.VMEM((1, B), jnp.float32)] * 2 + [pltpu.SemaphoreType.DMA((3,))],
        compiler_params=params(4),
    )(*[far(a) for a in (targets, potential.reshape(1, B), log_tgt.reshape(1, B))])


def near_kernel(sources, log_src, out, log, sems):
    n = out.shape[0] - A8
    core = lax.axis_index("c")
    copies = [
        pltpu.make_async_copy(sources.at[pl.ds(pl.multiple_of(core * n, n), n)], out.at[0:n], sems.at[0]),
        pltpu.make_async_copy(log_src, log, sems.at[1]),
    ]
    for copy in copies:
        copy.start()
    for copy in copies:
        copy.wait()
    rows = split(jnp.where(core == 0, log[:, :n], log[:, n:]))
    out[n:, :] = jnp.concatenate(rows + [jnp.zeros((A8 - 3, n), jnp.float32)], axis=0).astype(out.dtype)


def near_call(sources, log_src):
    n, f = sources.shape
    return pl.pallas_call(
        near_kernel,
        name="near_message",
        in_specs=[FAR] * 2,
        out_specs=WHOLE,
        out_shape=jax.ShapeDtypeStruct((n // 2 + A8, f), sources.dtype),
        scratch_shapes=[pltpu.VMEM((1, n), jnp.float32), pltpu.SemaphoreType.DMA((2,))],
        compiler_params=params(4),
    )(far(sources), far(log_src.reshape(1, n)))


def joined(picks, msgs):
    def kernel(*refs):
        out = refs[-1]
        extra = []
        for p, (m, k) in enumerate(picks):
            out[p * B : (p + 1) * B, :] = refs[m][k * B : (k + 1) * B, :]
            extra.append(refs[m][refs[m].shape[0] - A8 :, k * B : (k + 1) * B])
        rest = out.shape[1] - len(picks) * B
        extra.append(jnp.zeros((A8, rest), out.dtype))
        out[len(picks) * B :, :] = jnp.concatenate(extra, axis=1)

    return pl.pallas_call(
        kernel,
        in_specs=[WHOLE] * len(msgs),
        out_specs=WHOLE,
        out_shape=jax.ShapeDtypeStruct((len(picks) * B + A8, msgs[0].shape[1]), msgs[0].dtype),
        compiler_params=params(4),
    )(*msgs)


def eye(n):
    return lax.broadcasted_iota(jnp.int32, (n, n), 0) == lax.broadcasted_iota(jnp.int32, (n, n), 1)


def to_col(row):
    n = row.shape[1]
    return jnp.sum(jnp.where(eye(n), jnp.broadcast_to(row, (n, n)), 0.0), axis=1, keepdims=True)


def to_row(col):
    n = col.shape[0]
    return jnp.sum(jnp.where(eye(n), jnp.broadcast_to(col, (n, n)), 0.0), axis=0, keepdims=True)


CH = 512


def block_of(msgs, m, k):
    extra = msgs[m][msgs[m].shape[0] - A8 :, k * B : (k + 1) * B]
    return msgs[m].at[k * B : (k + 1) * B], extra.astype(jnp.float32)


def row_lse(s_out, at, pot):
    t = pot.shape[0]

    def shifted(r):
        return s_out[r : r + 32, at] + jnp.concatenate([pot[r : r + 32, :]] * (CH // 128), axis=1)

    top = jnp.full((8, CH), -jnp.inf, jnp.float32)
    for r in range(0, t, 32):
        top = jnp.maximum(top, jnp.max(shifted(r).reshape(4, 8, CH), axis=0))
    top = jnp.max(top, axis=0, keepdims=True)
    tot = jnp.zeros((8, CH), jnp.float32)
    for r in range(0, t, 32):
        tot = tot + jnp.sum(jnp.exp2(shifted(r) - top).reshape(4, 8, CH), axis=0)
    return top + jnp.log2(jnp.sum(tot, axis=0, keepdims=True))


def scores(tg, src, scale2):
    return lax.dot_general(tg, src, (((1,), (1,)), ((), ())), preferred_element_type=jnp.float32) * scale2


def laid_out(msgs, picks, tg, pot):
    for p, (m, k) in enumerate(picks):
        rows, ex = block_of(msgs, m, k)
        tg[p * B : (p + 1) * B, :] = rows[...]
        po = (ex[0:1] + ex[1:2] + ex[2:3]) * LOG2E
        pot[p * B : (p + 1) * B, :] = jnp.broadcast_to(to_col(po), (B, 128))


def turned(tg, out, base):
    core = lax.axis_index("c")
    for q in range(tg.shape[0] // 128):
        flipped = tg[q * 128 : (q + 1) * 128, :].T
        for f in range(16):
            to = pl.multiple_of((((f % 2) ^ core) * 8 + f // 2) * 32, 32)
            out[pl.ds(to, 32), base + q * 128 : base + (q + 1) * 128] = flipped[f * 32 : (f + 1) * 32, :]


def own_kernel_first(scale2, sources, *refs):
    msgs, (s_out, lse_out, tgt_out, tg, pot) = refs[:-5], refs[-5:]
    laid_out(msgs, PICKS1, tg, pot)
    for n in range(sources.shape[0] // CH):
        at = slice(n * CH, (n + 1) * CH)
        s_out[:, at] = scores(tg[...], sources[at, :], scale2)
        lse_out[:, at] = row_lse(s_out, at, pot)
    turned(tg, tgt_out, 0)


def near_kernel_first(scale2, near, swapped, log_src, tg, pot, s_out, lse_out, log_out):
    core = lax.axis_index("c")
    halves = []
    for ref in (near, swapped):
        parts = ref[CH:, :].astype(jnp.float32)
        halves.append(parts[0:1] + parts[1:2] + parts[2:3])
    for q in range(8):
        at = slice(q % 4 * 128, (q % 4 + 1) * 128)
        log_out[0, q : q + 1, :] = log_src[:, q * 128 : (q + 1) * 128] * LOG2E
        log_out[1, q : q + 1, :] = jnp.where(core == q // 4, halves[0][:, at], halves[1][:, at]) * LOG2E
    for ref, half in ((near, core), (swapped, 1 - core)):
        at = pl.ds(pl.multiple_of(half * CH, CH), CH)
        s_out[:, at] = scores(tg[...], ref[0:CH, :], scale2)
        lse_out[:, at] = row_lse(s_out, at, pot)


def last_kernel(scale2, sources, near, swapped, lse_own, lse_near, tgt_in, *refs):
    msgs, (s_out, rows_out, tgt_out, lt_out, tg, pot) = refs[:-6], refs[-6:]
    laid_out(msgs, PICKS2, tg, pot)
    yh, core = lax.axis_index("yh"), lax.axis_index("c")
    ns = sources.shape[0]
    for ref, row, lse_in, half, base, block in (
        (sources, 0, lse_own, 0, 0, yh),
        (sources, CH, lse_own, 1, 0, yh),
        (near, 0, lse_near, core, ns, 1 - yh),
        (swapped, 0, lse_near, 1 - core, ns, 1 - yh),
    ):
        begin = half * CH if isinstance(half, int) else pl.multiple_of(half * CH, CH)
        at = pl.ds(base + begin, CH)
        s_out[:, at] = scores(tg[...], ref[row : row + CH, :], scale2)
        lse = added_lse(lse_in[:, pl.ds(begin, CH)], row_lse(s_out, at, pot))
        for i in range(CH // 128):
            piece = jnp.broadcast_to(lse[:, i * 128 : (i + 1) * 128][None], (rows_out.shape[0], 1, 128))
            rows_out[:, block, pl.ds(half * (CH // 128) + i, 1), :] = piece
    for p, (m, k) in enumerate(PICKS):
        _, ex = block_of(msgs, m, k)
        lt_out[p : p + 1, 0:B] = (ex[3:4] + ex[4:5] + ex[5:6]) * LOG2E
    t1 = tgt_in.shape[1]
    tgt_out[:, :t1] = tgt_in[...]
    turned(tg, tgt_out, t1)


def added_lse(a, b):
    top = jnp.maximum(a, b)
    return top + jnp.log2(jnp.exp2(a - top) + jnp.exp2(b - top))


def scores_call(kernel, scale2, args, shapes, scratch, flops):
    return pl.pallas_call(
        lambda *a: kernel(scale2, *a),
        in_specs=[WHOLE] * len(args),
        out_specs=[WHOLE] * len(shapes),
        scratch_shapes=[pltpu.VMEM(s, d) for s, d in scratch],
        out_shape=[jax.ShapeDtypeStruct(s, d) for s, d in shapes],
        compiler_params=params(20),
        cost_estimate=pl.CostEstimate(flops=flops, bytes_accessed=1 << 22, transcendentals=1 << 20),
    )(*args)


def all_scores(sources, log_src, near, swapped, msgs, scale2):
    ns, f = sources.shape
    f32, bf = jnp.float32, jnp.bfloat16
    t1, t2 = len(PICKS1) * B, len(PICKS2) * B
    s1, lse1, tgt1, tg, pot = scores_call(
        own_kernel_first, scale2, [sources, *msgs[:6]],
        [((t1, ns), f32), ((1, ns), f32), ((f, t1), bf), ((t1, f), bf), ((t1, 128), f32)], [], 2 * t1 * ns * f,
    )
    s2, lse2, logs = scores_call(
        near_kernel_first, scale2, [near, swapped, log_src.reshape(1, ns), tg, pot],
        [((t1, ns), f32), ((1, ns), f32), ((2, ns // 128, 128), f32)], [], 2 * t1 * ns * f,
    )
    s3, rows, tgt, lt = scores_call(
        last_kernel, scale2, [sources, near, swapped, lse1, lse2, tgt1, *msgs],
        [((t2, 2 * ns), f32), ((32, 2, ns // 128, 128), f32), ((f, t1 + t2), bf), ((len(OFF), 128), f32)],
        [((t2, f), bf), ((t2, 128), f32)], 4 * t2 * ns * f,
    )
    return (s1, s2, s3), rows, logs, tgt, lt


def merged_lse(parts):
    top = jnp.max(parts, axis=0)
    return top + jnp.log2(jnp.sum(jnp.exp2(parts - top[None]), axis=0))


def slot_of(p):
    off = jnp.where(lax.axis_index("c") == 0, OFF[p], 16 - OFF[p])
    return (lax.axis_index("z") + off) % 16


def cols_kernel(parts, logs, s1, s2, s3, sp_out, msg_out, held, lse):
    yh = lax.axis_index("yh")
    for h in range(2):
        lse[h] = merged_lse(parts[:, h])
    for h, block in enumerate((yh, 1 - yh)):
        sp = logs[h] - lse[block]
        for r in range(8):
            sp_out[:, (h * 8 + r) * 128 : (h * 8 + r + 1) * 128] = sp[r : r + 1, :]
    held[...] = jnp.zeros_like(held)
    n1 = len(OFF1)
    ns = s1.shape[1]
    for p in range(len(OFF)):
        tops, totals = [], []
        for r in range(0, B, 8):
            lifted = []
            for k in range(2 * ns // 128):
                ref, base, col = (s3, (p - n1) * B, k * 128)
                if p < n1:
                    ref, base, col = (s1, p * B, k * 128) if k * 128 < ns else (s2, p * B, k * 128 - ns)
                lifted.append(ref[base + r : base + r + 8, col : col + 128] + sp_out[:, k * 128 : (k + 1) * 128])
            top = lifted[0]
            for v in lifted[1:]:
                top = jnp.maximum(top, v)
            total = jnp.exp2(lifted[0] - top)
            for v in lifted[1:]:
                total = total + jnp.exp2(v - top)
            tops.append(top)
            totals.append(total)
        tops, totals = jnp.concatenate(tops, axis=0), jnp.concatenate(totals, axis=0)
        top = jnp.max(tops, axis=1, keepdims=True)
        row = to_row(top + jnp.log2(jnp.sum(totals * jnp.exp2(tops - top), axis=1, keepdims=True)))
        row = jnp.concatenate([row, row], axis=1)
        slot = slot_of(p)
        at = slot // 2
        half = lax.broadcasted_iota(jnp.int32, (1, 128), 1) // B
        held[pl.ds(at, 1), :] = jnp.where(half == slot % 2, row, held[pl.ds(at, 1), :])
    msg_out[...] = jnp.broadcast_to(held[...][None], msg_out.shape)


def cols_call(parts, logs, s):
    ns = s[2].shape[1]
    return pl.pallas_call(
        cols_kernel,
        name="cols",
        in_specs=[WHOLE] * 5,
        out_specs=[WHOLE] * 2,
        scratch_shapes=[pltpu.VMEM((8, 128), jnp.float32), pltpu.VMEM((2, 8, 128), jnp.float32)],
        out_shape=[jax.ShapeDtypeStruct((1, ns), jnp.float32), jax.ShapeDtypeStruct((16, 8, 128), jnp.float32)],
        compiler_params=params(16),
    )(parts, logs, *s)


def moved_kernel(parts, lt, sp, s1, s2, s3, tgt, pot_out, theirs_out, mass_out, wide, tp, lse):
    lse[...] = merged_lse(parts[...])
    for p in range(len(OFF)):
        slot = slot_of(p)
        row = lse[pl.ds(slot // 2, 1), :]
        row = jnp.where(slot % 2 == 0, row[:, :B], row[:, B:])
        tpot = lt[p : p + 1, 0:B] - row
        if p == 0:
            pot_out[:, 0:B] = tpot * LN2
        tp[p * B : (p + 1) * B, :] = jnp.broadcast_to(to_col(tpot), (B, 128))

    t1, ns = s1.shape
    half = tgt.shape[0] // 2
    for n in range(sp.shape[1] // CH):
        at = slice(n * CH, (n + 1) * CH)
        spn = sp[:, at]
        mass = jnp.zeros((8, CH), jnp.float32)
        for r in range(0, tp.shape[0], 32):
            if r >= t1:
                s = s3[r - t1 : r - t1 + 32, at]
            elif n * CH < ns:
                s = s1[r : r + 32, at]
            else:
                s = s2[r : r + 32, n * CH - ns : (n + 1) * CH - ns]
            e = jnp.exp2(s + spn + jnp.concatenate([tp[r : r + 32, :]] * (CH // 128), axis=1))
            mass = mass + jnp.sum(e.reshape(4, 8, CH), axis=0)
            wide[r : r + 32, at] = e.astype(jnp.bfloat16)
        mass = jnp.sum(mass, axis=0, keepdims=True)
        mass_out[:, at] = mass
        part = jnp.dot(tgt[half:, :], wide[:, at], preferred_element_type=jnp.float32)
        theirs_out[0:half, at] = part.astype(jnp.bfloat16)
        hi = mass.astype(jnp.bfloat16).astype(jnp.float32)
        pad = jnp.zeros((6, CH), jnp.float32)
        theirs_out[half : half + 8, at] = jnp.concatenate([hi, mass - hi, pad], axis=0).astype(jnp.bfloat16)


def moved_call(parts, lt, sp, s, tgt):
    ns = sp.shape[1]
    f, t = tgt.shape
    return pl.pallas_call(
        moved_kernel,
        name="moved",
        in_specs=[WHOLE] * 7,
        out_specs=[WHOLE] * 4,
        scratch_shapes=[pltpu.VMEM((t, 128), jnp.float32), pltpu.VMEM((8, 128), jnp.float32)],
        out_shape=[
            jax.ShapeDtypeStruct((1, 128), jnp.float32),
            jax.ShapeDtypeStruct((f // 2 + 8, ns), jnp.bfloat16),
            jax.ShapeDtypeStruct((1, ns), jnp.float32),
            jax.ShapeDtypeStruct((t, ns), jnp.bfloat16),
        ],
        compiler_params=params(20),
    )(parts, lt, sp, *s, tgt)


def mine_kernel(tgt, wide, out):
    for n in range(out.shape[1] // CH):
        at = slice(n * CH, (n + 1) * CH)
        part = jnp.dot(tgt[: out.shape[0], :], wide[:, at], preferred_element_type=jnp.float32)
        out[:, at] = part.astype(jnp.bfloat16)


def mine_call(tgt, wide):
    f, t = tgt.shape
    ns = wide.shape[1]
    return pl.pallas_call(
        mine_kernel,
        name="mine",
        in_specs=[WHOLE] * 2,
        out_specs=WHOLE,
        out_shape=jax.ShapeDtypeStruct((f // 2, ns), jnp.bfloat16),
        compiler_params=params(12),
        cost_estimate=pl.CostEstimate(flops=f * t * ns, bytes_accessed=2 * t * ns, transcendentals=0),
    )(tgt, wide)


def pack_kernel(mine, theirs, mass, out):
    f32 = jnp.float32
    extra = theirs[256:264, :].astype(f32)
    total = mass[...] + extra[0:1] + extra[1:2]
    hi = total.astype(jnp.bfloat16).astype(f32)
    lo = total - hi
    yh = lax.axis_index("yh")
    for h in range(2):
        to = (h ^ yh) * 4
        rows = [v[:, (h * 8 + q) * 128 : (h * 8 + q + 1) * 128] for v in (hi, lo) for q in range(8)]
        rows = jnp.concatenate(rows, axis=0).astype(jnp.bfloat16)
        for g in range(8):
            at_chip = g // 4 * 8 + g % 4
            for q in range(8):
                at = (slice(g * 32, (g + 1) * 32), slice((h * 8 + q) * 128, (h * 8 + q + 1) * 128))
                both = mine[at].astype(f32) + theirs[at].astype(f32)
                out[to + at_chip, q * 32 : (q + 1) * 32, :] = both.astype(jnp.bfloat16)
            out[to + at_chip, 256:272, :] = rows


def pack_call(mine, theirs, mass):
    return pl.pallas_call(
        pack_kernel,
        name="pack",
        in_specs=[WHOLE] * 3,
        out_specs=WHOLE,
        out_shape=jax.ShapeDtypeStruct((16, 272, 128), jnp.bfloat16),
        compiler_params=params(8),
    )(mine, theirs, mass)


def finish_kernel(parts, sp, tpot, out, src_pot, tgt_pot):
    f32 = jnp.float32

    def added(at):
        total = parts[0, at, :].astype(f32)
        for k in range(1, parts.shape[0]):
            total = total + parts[k, at, :].astype(f32)
        return total

    for q in range(8):
        src_pot[q : q + 1, :] = sp[:, q * 128 : (q + 1) * 128] * LN2
    tgt_pot[...] = tpot[:, 0:B]
    mass = added(slice(256, 272))
    mass = mass[:8] + mass[8:]
    for q in range(8):
        image = added(slice(q * 32, (q + 1) * 32)) / mass[q : q + 1, :]
        out[:, q * 128 : (q + 1) * 128] = image.astype(jnp.bfloat16)


def finish_call(parts, sp, tpot):
    return pl.pallas_call(
        finish_kernel,
        name="finish",
        in_specs=[WHOLE] * 3,
        out_specs=[WHOLE] * 3,
        out_shape=[
            jax.ShapeDtypeStruct((32, 1024), jnp.bfloat16),
            jax.ShapeDtypeStruct((8, 128), jnp.float32),
            jax.ShapeDtypeStruct((1, B), jnp.float32),
        ],
        compiler_params=params(8),
    )(parts, sp, tpot)


def body(sources, log_src, targets, potential, log_tgt):
    f = sources.shape[1]
    scale2 = LOG2E / math.sqrt(f)

    own = own_call(targets, potential, log_tgt)
    ra = from_z(own, 4)
    la = from_z(own, -5)
    near = sent(near_call(sources, log_src), ("yh", "yl"), [(0, 3), (3, 0), (1, 2), (2, 1)])
    rb = from_z(joined([(0, 0), (1, 0)], [own, ra]), 2)
    lb = from_z(joined([(1, 0), (0, 0)], [own, la]), -2)
    rc = from_z(joined([(0, 0), (1, 0), (1, 1), (2, 0), (3, 0)], [own, rb, ra, la]), 1)
    lc = from_z(joined([(0, 0), (1, 0), (1, 1), (2, 0)], [own, lb, la]), -1)
    swapped = sent(near, "c", [(0, 1), (1, 0)])
    s, rows, logs, tgt, lt = all_scores(sources, log_src, near, swapped, [own, ra, la, rb, lb, rc, lc], scale2)
    row_parts = lax.all_to_all(rows, PLANE, split_axis=0, concat_axis=0, tiled=True)
    sp, cols = cols_call(row_parts, logs, s)
    col_parts = lax.all_to_all(cols, "z", split_axis=0, concat_axis=0, tiled=True)
    tpot, theirs, mass, wide = moved_call(col_parts, lt, sp, s, tgt)
    theirs = lax.ppermute(theirs, "c", [(0, 1), (1, 0)])
    packed = pack_call(mine_call(tgt, wide), theirs, mass)
    parts = lax.all_to_all(packed, CHIPS, split_axis=0, concat_axis=0, tiled=True)
    mapped, src_pot, tgt_pot = finish_call(parts, sp, tpot)
    return (src_pot.reshape(-1), tgt_pot.reshape(-1), mapped.T)


def solution(mesh):
    torus = Mesh(mesh.devices.reshape(16, 2, 2, 4, 2), AXES)
    src, every = ("z", "yh"), ("z", "yh", "yl", "x", "c")
    return jax.shard_map(
        body,
        mesh=torus,
        in_specs=(P(src, None), P(src), P(every, None), P(every), P(every)),
        out_specs=(P(src), P(every), P(src, ("yl", "x", "c"))),
        check_vma=False,
    )
```
